512 devices in a mesh: seq: 16 (over y, z_hi), mp: 32 (over z_lo, x, core).
Axes of the slice: x: 4, y: 4, z: 16 (z_hi: 4, z_lo: 4; z = z_hi * 4 + z_lo), core: 2. Of those that a mesh axis runs over, the one named last changes fastest.
Arguments:
- incoming: bfloat16 [8192, 4096], P('seq', 'mp'), may hold values from -12 to 12
- queries: bfloat16 [8192, 4096], P('seq', 'mp'), may hold values from -5 to 5
- key_vecs: bfloat16 [8192, 4096], P('seq', 'mp'), may hold values from -5 to 5
- value_vecs: bfloat16 [8192, 4096], P('seq', 'mp'), may hold values from -6 to 6
- w_out: bfloat16 [4096, 4096], P(None, 'mp'), may hold values from -0.09375 to 0.09375
- norm_gain: float32 [4096], P('mp'), may hold values from 0.25 to 1.75
- filters: bfloat16 [4096, 256], P('mp'), may hold values from -0.375 to 0.375
- filter_len: int32 [4096], P('mp'), may hold values from 128 to 256, as said below
- skip_gain: float32 [4096], P('mp'), may hold values from 0.5 to 1.5
- slot_map: int32 [32], replicated, may hold values from 0 to 31, as said below
Outputs:
- layer_out: bfloat16 [8192, 4096], P('seq', 'mp')
The draws below stay inside these ranges and needn't reach their ends.
Inputs may be any that keep to these rules, and one draw needn't show every extreme that they name: `slot_map`: slots 2 * i and 2 * i + 1, the rows of index i of seq, hold blocks i and 31 - i, in either order. `filter_len`: some channel uses all 256 taps.
All inputs are finite; a program needn't handle non-finite values.
Results may differ from the reference program's by a relative error of at most 0.0055.
Values may be sent and summed in bfloat16 or wider, within the bound.
A program may use at most 64 MiB of HBM per device.

```python
import jax
import jax.numpy as jnp
from jax import lax

D = 4096
HD = 128
SPAN = 256
FILT = 256
SPANS = 32
TOKENS = 8192


def draw_slot_map(key, part):
    flips = jax.random.randint(jax.random.fold_in(key, 11), (SPANS // 2,), 0, 2).astype(jnp.int32)
    lower_ids = jnp.arange(SPANS // 2, dtype=jnp.int32)
    upper_ids = SPANS - 1 - lower_ids
    first_ids = jnp.where(flips == 1, upper_ids, lower_ids)
    second_ids = jnp.where(flips == 1, lower_ids, upper_ids)
    return jnp.stack([first_ids, second_ids], axis=1).reshape(SPANS).astype(jnp.int32)


def draw_filter_len(key, part):
    first_key, second_key = jax.random.split(jax.random.fold_in(key, 23))
    lengths = jax.random.randint(first_key, (D,), FILT // 2, FILT + 1)
    chosen = jax.random.randint(second_key, (), 0, D)
    return jnp.where(jnp.arange(D) == chosen, FILT, lengths).astype(jnp.int32)


def draw_incoming(key, part):
    channel = jnp.arange(D, dtype=jnp.float32) / D
    raw_values = jnp.clip(jax.random.normal(jax.random.fold_in(key, 31), (TOKENS, D), jnp.float32), -6.0, 6.0)
    amplitude = 1.0 + channel
    return (raw_values * amplitude[None, :]).astype(jnp.bfloat16)


def query_key_pair(key):
    first_key, second_key = jax.random.split(jax.random.fold_in(key, 47), 2)
    shape = (TOKENS, D)
    query_rows = jnp.clip(1.5 * jax.random.normal(first_key, shape, jnp.float32), -5.0, 5.0)
    key_rows = jnp.clip(1.5 * jax.random.normal(second_key, shape, jnp.float32), -5.0, 5.0)
    return (query_rows, key_rows)


def draw_queries(key, part):
    return query_key_pair(key)[0].astype(jnp.bfloat16)


def draw_key_vecs(key, part):
    return query_key_pair(key)[1].astype(jnp.bfloat16)


def shard_levels(stream_key, extent, cuts, low, high):
    loudness, own = 1.0, jax.random.fold_in(stream_key, 6)
    for dim, shards_of in cuts:
        draws = jnp.exp(jax.random.uniform(jax.random.fold_in(own, dim), (shards_of,), jnp.float32, low / len(cuts), high / len(cuts)))
        loudness = loudness * jnp.repeat(draws, extent[dim] // shards_of).reshape([-1 if axis == dim else 1 for axis in range(len(extent))])
    return loudness


def scatter_about(key, dims, width, limit, cuts=(), kind=jnp.bfloat16):
    drawn = jax.random.normal(key, dims, jnp.float32) * width
    if len(cuts) > 0:
        drawn = shard_levels(key, dims, cuts, -0.22, 0.18) * drawn
    return jnp.clip(drawn, min=-limit, max=limit).astype(kind)


def setup_inputs(seed: int = 0) -> dict:
    key_list = jax.random.split(jax.random.key(seed), 11)
    return {
        "incoming": draw_incoming(jax.random.fold_in(key_list[10], 71), 0),
        "queries": draw_queries(jax.random.fold_in(key_list[10], 71), 0),
        "key_vecs": draw_key_vecs(jax.random.fold_in(key_list[10], 71), 0),
        "value_vecs": scatter_about(key_list[3], (TOKENS, D), 1.0, 6.0, ((0, 16), (1, 32))),
        "w_out": scatter_about(key_list[4], (D, D), D ** -0.5, 0.09375, ((1, 32),)),
        "norm_gain": jnp.clip(1.0 + 0.15 * jax.random.normal(key_list[5], (D,), jnp.float32), 0.25, 1.75),
        "filters": scatter_about(key_list[6], (D, FILT), FILT ** -0.5, 0.375, ((0, 32),)),
        "filter_len": draw_filter_len(jax.random.fold_in(key_list[10], 71), 0),
        "skip_gain": jnp.clip(0.5 + 1.0 * jax.random.uniform(key_list[8], (D,), jnp.float32) ** shard_levels(key_list[8], (D,), ((0, 32),), -0.2, 0.2), 0.5, 1.5),
        "slot_map": draw_slot_map(jax.random.fold_in(key_list[10], 71), 0),
    }


EPS = 1e-05

def toeplitz_table(group_taps, lag_table):
    tap_count = group_taps.shape[1]
    inside = (lag_table >= 0) & (lag_table < tap_count)
    picked = jnp.take(group_taps, jnp.clip(lag_table, 0, tap_count - 1).astype(jnp.int32), axis=1)
    return jnp.where(inside[None, :, :], picked, jnp.zeros((), group_taps.dtype))

def reference(incoming, queries, key_vecs, value_vecs, w_out, norm_gain, filters, filter_len, skip_gain, slot_map):
    row_ids = jnp.arange(TOKENS, dtype=jnp.int32)
    position = (slot_map[row_ids // SPAN] * SPAN + row_ids % SPAN).astype(jnp.int32)
    head_count = D // HD
    block_count = TOKENS // SPAN
    query_split = queries.reshape(TOKENS, head_count, HD).transpose(1, 0, 2)
    key_split = key_vecs.reshape(TOKENS, head_count, HD).transpose(1, 0, 2)
    value_split = value_vecs.reshape(TOKENS, head_count, HD).transpose(1, 0, 2)

    def one_head(operands):
        head_query, head_key, head_value = operands

        def one_block(block):
            block_query, block_pos = block
            scores = jnp.dot(block_query, head_key.T, preferred_element_type=jnp.float32) * HD ** (-0.5)
            allowed = position[None, :] <= block_pos[:, None]
            row_peak = lax.optimization_barrier(jnp.max(jnp.where(allowed, scores, -jnp.inf), axis=1, keepdims=True))
            weights = jnp.where(allowed, jnp.exp(scores - row_peak), 0.0)
            totals = lax.optimization_barrier(jnp.sum(weights, axis=1, keepdims=True))
            numerator = jnp.dot(weights.astype(jnp.bfloat16), head_value, preferred_element_type=jnp.float32)
            return (numerator / totals).astype(jnp.bfloat16)
        blocks_out = lax.map(one_block, (head_query.reshape(block_count, SPAN, HD), position.reshape(block_count, SPAN)))
        return blocks_out.reshape(TOKENS, HD)
    attention = lax.map(one_head, (query_split, key_split, value_split)).transpose(1, 0, 2).reshape(TOKENS, D)
    residual = incoming.astype(jnp.float32) + jnp.dot(attention, w_out, preferred_element_type=jnp.float32)
    mean_square = lax.optimization_barrier(jnp.mean(residual * residual, axis=1, keepdims=True))
    normed = (residual * lax.rsqrt(mean_square + EPS) * norm_gain[None, :]).astype(jnp.bfloat16)
    tap_ids = jnp.arange(FILT, dtype=jnp.int32)
    taps = jnp.where(tap_ids[None, :] < filter_len[:, None], filters, jnp.zeros((), filters.dtype))
    inverse = jnp.zeros((TOKENS,), jnp.int32).at[position].set(row_ids)
    ordered = normed[inverse].reshape(SPANS, SPAN, D)
    before = jnp.concatenate([jnp.zeros((1, SPAN, D), ordered.dtype), ordered[:-1]], axis=0)
    group_count = D // HD
    now_groups = ordered.reshape(SPANS, SPAN, group_count, HD).transpose(2, 0, 1, 3)
    before_groups = before.reshape(SPANS, SPAN, group_count, HD).transpose(2, 0, 1, 3)
    taps_groups = taps.reshape(group_count, HD, FILT)
    lag_now = (jnp.arange(SPAN, dtype=jnp.int32)[:, None] - jnp.arange(SPAN, dtype=jnp.int32)[None, :]).astype(jnp.int32)

    def one_group(operands):
        group_taps, group_now, group_before = operands
        near_matrix = toeplitz_table(group_taps, lag_now).astype(jnp.float32)
        far_matrix = toeplitz_table(group_taps, lag_now + SPAN).astype(jnp.float32)
        near_part = jnp.einsum('cts,nsc->ntc', near_matrix, group_now.astype(jnp.float32), precision=lax.Precision.HIGHEST)
        far_part = jnp.einsum('cts,nsc->ntc', far_matrix, group_before.astype(jnp.float32), precision=lax.Precision.HIGHEST)
        return near_part + far_part
    conv_groups = lax.map(one_group, (taps_groups, now_groups, before_groups))
    conv_natural = conv_groups.transpose(1, 2, 0, 3).reshape(TOKENS, D)
    conv_stored = conv_natural[position]
    layer_out = residual + conv_stored + skip_gain[None, :] * normed.astype(jnp.float32)
    return layer_out.astype(jnp.bfloat16)
```

```python
import functools
import math

import jax
import jax.numpy as jnp
from jax import lax
from jax.experimental import pallas as pl
from jax.experimental.pallas import tpu as pltpu
from jax.sharding import PartitionSpec as P

D = 4096
HD = 128
SPAN = 256
EPS = 1e-05
NEG = -1e30
LOG2 = HD ** (-0.5) * math.log2(math.e)
BF = jnp.bfloat16
F32 = jnp.float32


def remote(src, dst, send_sem, recv_sem, seq):
    return pltpu.make_async_remote_copy(
        src_ref=src,
        dst_ref=dst,
        send_sem=send_sem,
        recv_sem=recv_sem,
        device_id={"seq": seq},
        device_id_type=pl.DeviceIdType.MESH,
    )


def greet(peers):
    barrier = pltpu.get_barrier_semaphore()
    for peer in peers:
        pl.semaphore_signal(
            barrier, inc=1, device_id=peer, device_id_type=pl.DeviceIdType.MESH
        )
    pl.semaphore_wait(barrier, len(peers))


def to_lanes(rep):
    return jnp.concatenate(
        [rep[k : k + 128].T[0:1] for k in range(0, rep.shape[0], 128)], axis=0
    )


def from_lanes(rows):
    return jnp.concatenate(
        [jnp.broadcast_to(rows[k : k + 1], (128, 128)).T for k in range(rows.shape[0])], axis=0
    )


def attention_kernel(
    slot_ref,
    q_ref,
    k_ref,
    v_ref,
    out_ref,
    qb,
    kvb,
    acc,
    peak,
    total,
    osend,
    lsend,
    orecv,
    lrecv,
    q_ssem,
    q_rsem,
    kv_ssem,
    kv_rsem,
    o_ssem,
    o_rsem,
    l_ssem,
    l_rsem,
):
    rank = lax.axis_index("seq")
    y, zh = rank // 4, rank % 4
    along_y = [((y + d) % 4) * 4 + zh for d in range(4)]
    along_z = [y * 4 + (zh + d) % 4 for d in range(4)]
    gap = slot_ref[2 * rank] - slot_ref[2 * rank + 1]
    straight = jnp.full((SPAN, HD), gap, jnp.int32) < 0

    def in_order(ref, half):
        one, two = ref[0:SPAN, :].astype(F32), ref[SPAN : 2 * SPAN, :].astype(F32)
        return jnp.where(straight, (one, two)[half], (two, one)[half]).astype(BF)

    for half in range(2):
        qb[0, half] = in_order(q_ref, half)
        kvb[0, half, 0] = in_order(k_ref, half)
        kvb[0, half, 1] = in_order(v_ref, half)
    greet([{"seq": along_y[d]} for d in (1, 2, 3)] + [{"seq": along_z[d]} for d in (1, 3)])

    def kv_copy(direction, half, sub, relay):
        source = 0 if not relay else (3 if direction == 0 else 1)
        target = 2 if relay else (3 if direction == 0 else 1)
        rows = pl.ds(sub * 128, 128)
        return remote(
            kvb.at[source, half, :, rows],
            kvb.at[target, half, :, rows],
            kv_ssem.at[direction, half, 2 if relay else sub],
            kv_rsem.at[target, half, sub],
            along_z[1 if direction == 0 else 3],
        )

    def kv_arrival(slot, half, sub):
        rows = pl.ds(sub * 128, 128)
        view = kvb.at[slot, half, :, rows]
        return remote(view, view, kv_ssem.at[0, half, sub], kv_rsem.at[slot, half, sub], rank)

    def q_copy(d):
        return remote(qb.at[0], qb.at[4 - d], q_ssem.at[d - 1], q_rsem.at[3 - d], along_y[d])

    def o_copies(d, half):
        return (
            remote(
                osend.at[d - 1, half],
                orecv.at[3 - d, half],
                o_ssem.at[d - 1, half],
                o_rsem.at[3 - d, half],
                along_y[d],
            ),
            remote(
                lsend.at[d - 1, half],
                lrecv.at[3 - d, half],
                l_ssem.at[d - 1, half],
                l_rsem.at[3 - d, half],
                along_y[d],
            ),
        )

    for sub in range(2):
        kv_copy(0, 0, sub, False).start()
        kv_copy(1, 0, 1 - sub, False).start()
    for d in (1, 3, 2):
        q_copy(d).start()

    acc[...] = jnp.zeros_like(acc)
    total[...] = jnp.zeros_like(total)
    peak[...] = jnp.full_like(peak, NEG)
    ones = jnp.ones((SPAN, HD), BF)

    def block(d, qhalf, slot, half, diagonal):
        keys, values = kvb[slot, half, 0], kvb[slot, half, 1]
        scores = lax.dot_general(
            qb[d, qhalf], keys, (((1,), (1,)), ((), ())), preferred_element_type=F32
        )
        if diagonal:
            row = lax.broadcasted_iota(jnp.int32, (SPAN, SPAN), 0)
            col = lax.broadcasted_iota(jnp.int32, (SPAN, SPAN), 1)
            scores = jnp.where(col <= row, scores, NEG)
        old = peak[d, qhalf]
        new = jnp.maximum(old, jnp.max(scores, axis=1, keepdims=True))
        weights = jnp.exp2((scores - jnp.concatenate([new, new], axis=1)) * LOG2)
        factor = jnp.exp2((old - new) * LOG2)
        summed = lax.dot_general(
            weights.astype(BF),
            jnp.concatenate([values, ones], axis=1),
            (((1,), (0,)), ((), ())),
            preferred_element_type=F32,
        )
        acc[d, qhalf] = acc[d, qhalf] * factor + summed[:, :HD]
        total[d, qhalf] = total[d, qhalf] * factor + summed[:, HD:]
        peak[d, qhalf] = new

    def visit(d, slot, half):
        q_low = ((y + d) % 4) * 4 + zh
        k_low = y * 4 + (zh + slot) % 4
        if half == 0:
            block(d, 1, slot, 0, False)

            @pl.when(k_low < q_low)
            def _():
                block(d, 0, slot, 0, False)
        else:

            @pl.when(q_low < k_low)
            def _():
                block(d, 1, slot, 1, False)

    def visit_all(slot, half, start):
        def step(d, carry):
            visit(d, slot, half)
            return carry

        lax.fori_loop(start, 4, step, 0)

    def send_partial(half):
        def step(d, carry):
            norm = jnp.maximum(total[d, half], 1e-30)
            osend[d - 1, half] = (acc[d, half] / norm).astype(BF)
            lsend[d - 1, half, 0:2] = to_lanes(peak[d, half] * LOG2 + jnp.log2(norm))
            return carry

        lax.fori_loop(1, 4, step, 0)
        for d in (2, 1, 3):
            for copy in o_copies(d, half):
                copy.start()

    def combine(half):
        for d in (1, 2, 3):
            for copy in o_copies(d, half):
                copy.wait_recv()
        norm = jnp.maximum(total[0, half], 1e-30)
        logs = [peak[0, half] * LOG2 + jnp.log2(norm)]
        logs += [from_lanes(lrecv[s, half, 0:2]) for s in range(3)]
        top = functools.reduce(jnp.maximum, logs)
        shares = [jnp.exp2(log - top) for log in logs]
        mixed = shares[0] * (acc[0, half] / norm)
        for s in range(3):
            mixed = mixed + shares[s + 1] * orecv[s, half].astype(F32)
        out_ref[half] = (mixed / functools.reduce(jnp.add, shares)).astype(BF)

    block(0, 0, 0, 0, True)
    block(0, 1, 0, 0, False)
    block(0, 1, 0, 1, True)
    for d in (1, 2, 3):
        q_copy(d).wait_recv()
    visit_all(0, 0, 1)
    visit_all(0, 1, 1)
    for half in range(2):
        kv_arrival(3, half, 0).wait_recv()
        kv_copy(0, half, 0, True).start()
        kv_arrival(1, half, 1).wait_recv()
        kv_copy(1, half, 1, True).start()
        if half == 0:
            for sub in range(2):
                kv_copy(0, 1, sub, False).start()
                kv_copy(1, 1, 1 - sub, False).start()
        kv_arrival(3, half, 1).wait_recv()
        visit_all(3, half, 0)
        kv_arrival(1, half, 0).wait_recv()
        visit_all(1, half, 0)
        if half == 1:
            combine(0)
        kv_arrival(2, half, 0).wait_recv()
        kv_arrival(2, half, 1).wait_recv()
        visit_all(2, half, 0)
        send_partial(half)
    combine(1)
    for direction in range(2):
        for half in range(2):
            for sub in range(2):
                kv_copy(direction, half, sub, False).wait_send()
            kv_copy(direction, half, direction, True).wait_send()
    for d in (1, 2, 3):
        q_copy(d).wait_send()
        for half in range(2):
            for copy in o_copies(d, half):
                copy.wait_send()


def attend(slot_map, queries, key_vecs, value_vecs):
    dma = pltpu.SemaphoreType.DMA
    vmem = pl.BlockSpec(memory_space=pltpu.VMEM)
    return pl.pallas_call(
        attention_kernel,
        out_shape=jax.ShapeDtypeStruct((2, SPAN, HD), BF),
        in_specs=[pl.BlockSpec(memory_space=pltpu.SMEM)] + [vmem] * 3,
        out_specs=vmem,
        scratch_shapes=[
            pltpu.VMEM((4, 2, SPAN, HD), BF),
            pltpu.VMEM((4, 2, 2, SPAN, HD), BF),
            pltpu.VMEM((4, 2, SPAN, HD), F32),
            pltpu.VMEM((4, 2, SPAN, HD), F32),
            pltpu.VMEM((4, 2, SPAN, HD), F32),
            pltpu.VMEM((3, 2, SPAN, HD), BF),
            pltpu.VMEM((3, 2, 8, HD), F32),
            pltpu.VMEM((3, 2, SPAN, HD), BF),
            pltpu.VMEM((3, 2, 8, HD), F32),
            dma((3,)),
            dma((3,)),
            dma((2, 2, 3)),
            dma((4, 2, 2)),
            dma((3, 2)),
            dma((3, 2)),
            dma((3, 2)),
            dma((3, 2)),
        ],
        compiler_params=pltpu.CompilerParams(collective_id=0, has_side_effects=True),
        name="attend",
    )(slot_map, queries, key_vecs, value_vecs)


def from_everyone(x, axis):
    size = lax.axis_size(axis)
    return lax.all_to_all(jnp.broadcast_to(x[None], (size, *x.shape)), axis, 0, 0, tiled=True)


def of_everyone(x, axis):
    everything = from_everyone(x, axis)
    return jnp.sum(everything, axis=0)


def shifted(block, axis, distance):
    devices = range(lax.axis_size(axis))
    route = [(i - distance, i) for i in devices if i - distance in devices]
    return lax.ppermute(block, axis, route)


def causal_window(extended, taps_lag):
    pair_count, twice, width = extended.shape
    length = twice // 2
    tap_count = taps_lag.shape[0]
    inner = math.gcd(tap_count, 16)

    def causal_advance(block, accum):
        base = block * inner
        window = lax.dynamic_slice_in_dim(
            extended, length - base - inner + 1, length + inner - 1, 1
        ).astype(jnp.float32)
        tap_block = lax.dynamic_slice_in_dim(taps_lag, base, inner, 0).astype(jnp.float32)
        for lag in range(inner):
            offset = inner - 1 - lag
            accum = accum + tap_block[lag][None, None, :] * window[:, offset : offset + length]
        return accum

    start = jnp.zeros((pair_count, length, width), jnp.float32)
    return lax.fori_loop(0, tap_count // inner, causal_advance, start)


def on_device(
    incoming,
    queries,
    key_vecs,
    value_vecs,
    w_out,
    norm_gain,
    filters,
    filter_len,
    skip_gain,
    slot_map,
):
    tok_rows, local_width = queries.shape
    seq_rank = lax.axis_index("seq")
    seq_size = lax.axis_size("seq")
    pair_ids = lax.dynamic_slice_in_dim(slot_map, 2 * seq_rank, 2)
    low_first = pair_ids[0] < pair_ids[1]
    attention = attend(slot_map, queries, key_vecs, value_vecs).reshape(tok_rows, HD)
    incoming = incoming.reshape(2, SPAN, local_width)
    incoming = jnp.where(low_first, incoming, incoming[::-1]).reshape(tok_rows, local_width)
    projected = jnp.dot(
        lax.all_gather(attention, "mp", axis=1, tiled=True),
        w_out,
        preferred_element_type=jnp.float32,
    )
    residual = incoming.astype(jnp.float32) + projected
    square_total = of_everyone(jnp.sum(residual * residual, axis=1), "mp")
    normed = (residual * lax.rsqrt(square_total / D + EPS)[:, None] * norm_gain[None, :]).astype(
        jnp.bfloat16
    )
    tap_count = filters.shape[1]
    taps = jnp.where(
        jnp.arange(tap_count, dtype=jnp.int32)[None, :] < filter_len[:, None],
        filters,
        jnp.zeros((), filters.dtype),
    )
    taps_lag = taps.T
    own_pair = normed.reshape(2, SPAN, local_width)
    last_rank = seq_rank == seq_size - 1
    low_before = shifted(own_pair[0], "seq", 1)
    high_before = shifted(own_pair[1], "seq", -1)
    high_before = jnp.where(last_rank, own_pair[0], high_before)
    before_pair = jnp.stack([low_before, high_before])
    conv_pair = causal_window(jnp.concatenate([before_pair, own_pair], axis=1), taps_lag)
    conv_rows = conv_pair.reshape(tok_rows, local_width)
    layer_out = residual + conv_rows + skip_gain[None, :] * normed.astype(jnp.float32)
    layer_out = layer_out.astype(jnp.bfloat16).reshape(2, SPAN, local_width)
    return jnp.where(low_first, layer_out, layer_out[::-1]).reshape(tok_rows, local_width)


def solution(mesh):
    placed = (
        P("seq", "mp"),
        P("seq", "mp"),
        P("seq", "mp"),
        P("seq", "mp"),
        P(None, "mp"),
        P("mp"),
        P("mp", None),
        P("mp"),
        P("mp"),
        P(),
    )
    return jax.shard_map(
        on_device, mesh=mesh, in_specs=placed, out_specs=P("seq", "mp"), check_vma=False
    )
```

```python
import functools
import math

import jax
import jax.numpy as jnp
from jax import lax
from jax.experimental import pallas as pl
from jax.experimental.pallas import tpu as pltpu
from jax.sharding import PartitionSpec as P

D = 4096
HD = 128
SPAN = 256
FILT = 256
EPS = 1e-05
NEG = -1e30
LOG2 = HD ** (-0.5) * math.log2(math.e)
BF = jnp.bfloat16
F32 = jnp.float32
TILE = 64


def remote(src, dst, send_sem, recv_sem, **where):
    return pltpu.make_async_remote_copy(
        src_ref=src,
        dst_ref=dst,
        send_sem=send_sem,
        recv_sem=recv_sem,
        device_id=where,
        device_id_type=pl.DeviceIdType.MESH,
    )


def greet(peers):
    barrier = pltpu.get_barrier_semaphore()
    for peer in peers:
        pl.semaphore_signal(
            barrier, inc=1, device_id=peer, device_id_type=pl.DeviceIdType.MESH
        )
    pl.semaphore_wait(barrier, len(peers))


def to_lanes(rep):
    return jnp.concatenate(
        [rep[k : k + 128].T[0:1] for k in range(0, rep.shape[0], 128)], axis=0
    )


def from_lanes(rows):
    return jnp.concatenate(
        [jnp.broadcast_to(rows[k : k + 1], (128, 128)).T for k in range(rows.shape[0])], axis=0
    )


def layer_kernel(
    slot_ref,
    q_ref,
    k_ref,
    v_ref,
    inc_ref,
    w_ref,
    gain_ref,
    filt_ref,
    flen_ref,
    skip_ref,
    out_ref,
    qb,
    kvb,
    acc,
    peak,
    total,
    osend,
    lsend,
    orecv,
    lrecv,
    gath,
    resid,
    taps,
    stat,
    stat_core,
    stat_x,
    stat_z,
    nb,
    hb,
    shift,
    conv,
    final,
    q_ssem,
    q_rsem,
    kv_ssem,
    kv_rsem,
    o_ssem,
    o_rsem,
    l_ssem,
    l_rsem,
    z_ssem,
    z_rsem,
    x_ssem,
    x_rsem,
    p_ssem,
    p_rsem,
    t_ssem,
    tc_rsem,
    tx_rsem,
    tz_rsem,
    h_ssem,
    h_rsem,
):
    rank, head = lax.axis_index("seq"), lax.axis_index("mp")
    y, zh = rank // 4, rank % 4
    along_y = [((y + d) % 4) * 4 + zh for d in range(4)]
    along_z = [y * 4 + (zh + d) % 4 for d in range(4)]
    zl, x, core = head // 8, (head // 2) % 4, head % 2
    near = jnp.where(zl == 0, 1, zl - 1)
    far = jnp.where(zl < 2, 3, 0)
    lines = [zl, near, 6 - zl - near - far, far]
    xs = [(x + d) % 4 for d in range(4)]
    partner = head + 1 - 2 * core

    def mp_of(zl_i, x_i):
        return (zl_i * 4 + x_i) * 2 + core

    gap = slot_ref[2 * rank] - slot_ref[2 * rank + 1]
    straight = jnp.full((SPAN, HD), gap, jnp.int32) < 0

    def in_order(ref, half):
        one, two = ref[0:SPAN, :].astype(F32), ref[SPAN : 2 * SPAN, :].astype(F32)
        return jnp.where(straight, (one, two)[half], (two, one)[half])

    for half in range(2):
        qb[0, half] = in_order(q_ref, half).astype(BF)
        kvb[0, half, 0] = in_order(k_ref, half).astype(BF)
        kvb[0, half, 1] = in_order(v_ref, half).astype(BF)
    greet(
        [{"seq": along_y[d]} for d in (1, 2, 3)]
        + [{"seq": along_z[d]} for d in (1, 3)]
        + [{"seq": (rank + d) % 16} for d in (1, 15)]
        + [{"mp": partner}]
        + [{"mp": mp_of(zl, xs[d])} for d in (1, 2, 3)]
        + [{"mp": mp_of(lines[k], x)} for k in (1, 2, 3)]
    )

    def kv_copy(direction, half, sub, relay):
        source = 0 if not relay else (3 if direction == 0 else 1)
        target = 2 if relay else (3 if direction == 0 else 1)
        rows = pl.ds(sub * 128, 128)
        return remote(
            kvb.at[source, half, :, rows],
            kvb.at[target, half, :, rows],
            kv_ssem.at[direction, half, 2 if relay else sub],
            kv_rsem.at[target, half, sub],
            seq=along_z[1 if direction == 0 else 3],
        )

    def kv_arrival(slot, half, sub):
        view = kvb.at[slot, half, :, pl.ds(sub * 128, 128)]
        return remote(view, view, kv_ssem.at[0, half, sub], kv_rsem.at[slot, half, sub], seq=rank)

    def q_copy(d):
        return remote(qb.at[0], qb.at[4 - d], q_ssem.at[d - 1], q_rsem.at[3 - d], seq=along_y[d])

    def o_copies(d, half):
        return (
            remote(
                osend.at[d - 1, half],
                orecv.at[3 - d, half],
                o_ssem.at[d - 1, half],
                o_rsem.at[3 - d, half],
                seq=along_y[d],
            ),
            remote(
                lsend.at[d - 1, half],
                lrecv.at[3 - d, half],
                l_ssem.at[d - 1, half],
                l_rsem.at[3 - d, half],
                seq=along_y[d],
            ),
        )

    def line_copy(half, k):
        view = gath.at[half, zl, x, core]
        return remote(
            view, view, z_ssem.at[half, k - 1], z_rsem.at[half, zl], mp=mp_of(lines[k], x)
        )

    def line_arrival(half, k):
        view = gath.at[half, lines[k], x, core]
        return remote(view, view, z_ssem.at[half, k - 1], z_rsem.at[half, lines[k]], mp=head)

    def x_copy(half, k, direction, sub, relay):
        source = xs[(3 if direction == 0 else 1) if relay else 0]
        view = gath.at[half, lines[k], source, core, pl.ds(sub * 128, 128)]
        return remote(
            view,
            view,
            x_ssem.at[half, k, direction, 2 if relay else sub],
            x_rsem.at[half, k, source, sub],
            mp=mp_of(zl, xs[1 if direction == 0 else 3]),
        )

    def x_arrival(half, k, d, sub):
        view = gath.at[half, lines[k], xs[d], core, pl.ds(sub * 128, 128)]
        return remote(view, view, x_ssem.at[half, k, 0, sub], x_rsem.at[half, k, xs[d], sub], mp=head)

    def p_copy(half, k, d):
        view = gath.at[half, lines[k], xs[d], core]
        return remote(view, view, p_ssem.at[half, k, d], p_rsem.at[half, k, d], mp=partner)

    def p_arrival(half, k, d):
        view = gath.at[half, lines[k], xs[d], 1 - core]
        return remote(view, view, p_ssem.at[half, k, d], p_rsem.at[half, k, d], mp=head)

    def core_copy(half):
        return remote(
            stat.at[half, 0], stat_core.at[half], t_ssem.at[half, 0], tc_rsem.at[half], mp=partner
        )

    def sx_copy(half, d):
        return remote(
            stat.at[half, 1],
            stat_x.at[half, 3 - d],
            t_ssem.at[half, d],
            tx_rsem.at[half, 3 - d],
            mp=mp_of(zl, xs[d]),
        )

    def sz_copy(half, k):
        return remote(
            stat.at[half, 2],
            stat_z.at[half, zl],
            t_ssem.at[half, 3 + k],
            tz_rsem.at[half, zl],
            mp=mp_of(lines[k], x),
        )

    def sz_arrival(half, k):
        view = stat_z.at[half, lines[k]]
        return remote(view, view, t_ssem.at[half, 3 + k], tz_rsem.at[half, lines[k]], mp=head)

    def h_copy(half):
        return remote(
            nb.at[half],
            hb.at[half],
            h_ssem.at[half],
            h_rsem.at[half],
            seq=(rank + (1 if half == 0 else 15)) % 16,
        )

    for sub in range(2):
        kv_copy(0, 0, sub, False).start()
        kv_copy(1, 0, 1 - sub, False).start()
    for d in (1, 3, 2):
        q_copy(d).start()

    acc[...] = jnp.zeros_like(acc)
    total[...] = jnp.zeros_like(total)
    peak[...] = jnp.full_like(peak, NEG)
    ones = jnp.ones((SPAN, HD), BF)

    def block(d, qhalf, slot, half, diagonal):
        keys, values = kvb[slot, half, 0], kvb[slot, half, 1]
        scores = lax.dot_general(
            qb[d, qhalf], keys, (((1,), (1,)), ((), ())), preferred_element_type=F32
        )
        if diagonal:
            row = lax.broadcasted_iota(jnp.int32, (SPAN, SPAN), 0)
            col = lax.broadcasted_iota(jnp.int32, (SPAN, SPAN), 1)
            scores = jnp.where(col <= row, scores, NEG)
        old = peak[d, qhalf]
        new = jnp.maximum(old, jnp.max(scores, axis=1, keepdims=True))
        weights = jnp.exp2((scores - jnp.concatenate([new, new], axis=1)) * LOG2)
        factor = jnp.exp2((old - new) * LOG2)
        summed = lax.dot_general(
            weights.astype(BF),
            jnp.concatenate([values, ones], axis=1),
            (((1,), (0,)), ((), ())),
            preferred_element_type=F32,
        )
        acc[d, qhalf] = acc[d, qhalf] * factor + summed[:, :HD]
        total[d, qhalf] = total[d, qhalf] * factor + summed[:, HD:]
        peak[d, qhalf] = new

    def visit(d, slot, half):
        q_low = ((y + d) % 4) * 4 + zh
        k_low = y * 4 + (zh + slot) % 4
        if half == 0:
            block(d, 1, slot, 0, False)

            @pl.when(k_low < q_low)
            def _():
                block(d, 0, slot, 0, False)
        else:

            @pl.when(q_low < k_low)
            def _():
                block(d, 1, slot, 1, False)

    def visit_all(slot, half, start):
        def step(d, carry):
            visit(d, slot, half)
            return carry

        lax.fori_loop(start, 4, step, 0)

    def send_partial(half):
        def step(d, carry):
            norm = jnp.maximum(total[d, half], 1e-30)
            osend[d - 1, half] = (acc[d, half] / norm).astype(BF)
            lsend[d - 1, half, 0:2] = to_lanes(peak[d, half] * LOG2 + jnp.log2(norm))
            return carry

        lax.fori_loop(1, 4, step, 0)
        for d in (2, 1, 3):
            for copy in o_copies(d, half):
                copy.start()

    def combine(half):
        for d in (1, 2, 3):
            for copy in o_copies(d, half):
                copy.wait_recv()
        norm = jnp.maximum(total[0, half], 1e-30)
        logs = [peak[0, half] * LOG2 + jnp.log2(norm)]
        logs += [from_lanes(lrecv[s, half, 0:2]) for s in range(3)]
        top = functools.reduce(jnp.maximum, logs)
        shares = [jnp.exp2(log - top) for log in logs]
        mixed = shares[0] * (acc[0, half] / norm)
        for s in range(3):
            mixed = mixed + shares[s + 1] * orecv[s, half].astype(F32)
        gath[half, zl, x, core] = (mixed / functools.reduce(jnp.add, shares)).astype(BF)

    def send_x(half, k):
        for sub in range(2):
            x_copy(half, k, 0, sub, False).start()
            x_copy(half, k, 1, 1 - sub, False).start()
        p_copy(half, k, 0).start()

    def own_out(half):
        for k in (3, 2, 1):
            line_copy(half, k).start()
        send_x(half, 0)

    def line_in(half, k):
        line_arrival(half, k).wait_recv()
        send_x(half, k)

    def x_in(half, k):
        x_arrival(half, k, 3, 0).wait_recv()
        x_copy(half, k, 0, 0, True).start()
        x_arrival(half, k, 1, 1).wait_recv()
        x_copy(half, k, 1, 1, True).start()
        x_arrival(half, k, 3, 1).wait_recv()
        p_copy(half, k, 3).start()
        x_arrival(half, k, 1, 0).wait_recv()
        p_copy(half, k, 1).start()

    def x_far(half, k):
        x_arrival(half, k, 2, 0).wait_recv()
        x_arrival(half, k, 2, 1).wait_recv()
        p_copy(half, k, 2).start()

    def project(half, k):
        for d in range(4):
            p_arrival(half, k, d).wait_recv()
        rows = jnp.concatenate(
            [gath[half, lines[k], x_i, c] for x_i in range(4) for c in range(2)], axis=1
        )
        weights = w_ref[pl.ds(pl.multiple_of(lines[k] * 1024, 1024), 1024), :]
        part = jnp.dot(rows, weights, preferred_element_type=F32)
        if k == 0:
            resid[half] = in_order(inc_ref, half) + part
        else:
            resid[half] += part

    def stat_out(half):
        square = resid[half] * resid[half]
        stat[half, 0, 0:2] = jnp.concatenate(
            [jnp.sum(square[k : k + 128].T, axis=0, keepdims=True) for k in (0, 128)], axis=0
        )
        core_copy(half).start()

    def stat_mid(half):
        core_copy(half).wait_recv()
        stat[half, 1, 0:2] = stat[half, 0, 0:2] + stat_core[half, 0:2]
        for d in (2, 1, 3):
            sx_copy(half, d).start()

    def stat_late(half):
        for d in (1, 2, 3):
            sx_copy(half, d).wait_recv()
        stat[half, 2, 0:2] = stat[half, 1, 0:2] + (
            stat_x[half, 0, 0:2] + stat_x[half, 1, 0:2] + stat_x[half, 2, 0:2]
        )
        for k in (3, 2, 1):
            sz_copy(half, k).start()

    def normalize(half):
        for k in (1, 2, 3):
            sz_arrival(half, k).wait_recv()
        whole = stat[half, 2, 0:2]
        for k in (1, 2, 3):
            whole = whole + stat_z[half, lines[k], 0:2]
        scale = from_lanes(lax.rsqrt(whole / D + EPS))
        normed = (resid[half] * scale * gain_ref[...]).astype(BF)
        nb[half] = normed
        if half == 0:

            @pl.when(rank < 15)
            def _():
                h_copy(0).start()
        else:

            @pl.when(rank > 0)
            def _():
                h_copy(1).start()

        wide = normed.astype(F32)
        resid[half] += skip_ref[...] * wide
        for s in range(8):
            shift[half, s, SPAN + s : 2 * SPAN + s, :] = wide

    def lags(half, top, begin, end, start):
        def step(a, run):
            eight = taps[pl.ds(pl.multiple_of(a * 8, 8), 8), :]
            rows = pl.ds(pl.multiple_of(SPAN + top - a * 8, 8), TILE)
            for s in range(8):
                run = run + eight[s : s + 1] * shift[half, s, rows, :]
            return run

        return lax.fori_loop(begin, end, step, start)

    def conv_own(half):
        for top in range(TILE, SPAN, TILE):
            conv[half, top : top + TILE, :] = lags(
                half, top, 0, top // 8, jnp.zeros((TILE, HD), F32)
            )

    def conv_rest(half):
        edge = rank == (0 if half == 0 else 15)

        @pl.when(edge)
        def _():
            hb[half] = jnp.zeros((SPAN, HD), BF) if half == 0 else nb[0]

        @pl.when(jnp.logical_not(edge))
        def _():
            h_copy(half).wait_recv()

        before = hb[half].astype(F32)
        for s in range(8):
            shift[half, s, s : SPAN + s, :] = before
        for top in range(0, SPAN, TILE):
            begin = jnp.zeros((TILE, HD), F32) if top == 0 else conv[half, top : top + TILE, :]
            final[half, top : top + TILE, :] = resid[half, top : top + TILE, :] + lags(
                half, top, top // 8, FILT // 8, begin
            )

    block(0, 0, 0, 0, True)
    block(0, 1, 0, 0, False)
    block(0, 1, 0, 1, True)
    lag = lax.broadcasted_iota(jnp.int32, (FILT, HD), 0)
    turned = jnp.concatenate(
        [filt_ref[:, k : k + 128].astype(F32).T for k in (0, 128)], axis=0
    )
    taps[...] = jnp.where(lag < flen_ref[...], turned, 0.0)
    for d in (1, 2, 3):
        q_copy(d).wait_recv()
    visit_all(0, 0, 1)
    visit_all(0, 1, 1)

    kv_arrival(3, 0, 0).wait_recv()
    kv_copy(0, 0, 0, True).start()
    kv_arrival(1, 0, 1).wait_recv()
    kv_copy(1, 0, 1, True).start()
    for sub in range(2):
        kv_copy(0, 1, sub, False).start()
        kv_copy(1, 1, 1 - sub, False).start()
    kv_arrival(3, 0, 1).wait_recv()
    visit_all(3, 0, 0)
    kv_arrival(1, 0, 0).wait_recv()
    visit_all(1, 0, 0)
    kv_arrival(2, 0, 0).wait_recv()
    kv_arrival(2, 0, 1).wait_recv()
    visit_all(2, 0, 0)
    send_partial(0)

    kv_arrival(3, 1, 0).wait_recv()
    kv_copy(0, 1, 0, True).start()
    kv_arrival(1, 1, 1).wait_recv()
    kv_copy(1, 1, 1, True).start()
    combine(0)
    own_out(0)
    kv_arrival(3, 1, 1).wait_recv()
    visit_all(3, 1, 0)
    line_in(0, 1)
    x_in(0, 0)
    kv_arrival(1, 1, 0).wait_recv()
    visit_all(1, 1, 0)
    line_in(0, 2)
    x_in(0, 1)
    kv_arrival(2, 1, 0).wait_recv()
    kv_arrival(2, 1, 1).wait_recv()
    visit_all(2, 1, 0)
    send_partial(1)
    line_in(0, 3)
    x_far(0, 0)
    project(0, 0)
    x_in(0, 2)
    combine(1)
    own_out(1)
    x_far(0, 1)
    project(0, 1)
    x_in(0, 3)
    line_in(1, 1)
    x_far(0, 2)
    project(0, 2)
    x_in(1, 0)
    x_far(0, 3)
    line_in(1, 2)
    project(0, 3)
    stat_out(0)
    x_in(1, 1)
    line_in(1, 3)
    stat_mid(0)
    x_far(1, 0)
    project(1, 0)
    x_in(1, 2)
    stat_late(0)
    x_far(1, 1)
    project(1, 1)
    x_in(1, 3)
    x_far(1, 2)
    project(1, 2)
    normalize(0)
    x_far(1, 3)
    project(1, 3)
    stat_out(1)
    conv_own(0)
    stat_mid(1)
    conv_rest(0)
    stat_late(1)
    normalize(1)
    conv_own(1)
    conv_rest(1)
    low, high = final[0], final[1]
    out_ref[0:SPAN, :] = jnp.where(straight, low, high).astype(BF)
    out_ref[SPAN : 2 * SPAN, :] = jnp.where(straight, high, low).astype(BF)

    for half in range(2):
        for direction in range(2):
            for sub in range(2):
                kv_copy(direction, half, sub, False).wait_send()
            kv_copy(direction, half, direction, True).wait_send()
            for k in range(4):
                for sub in range(2):
                    x_copy(half, k, direction, sub, False).wait_send()
                x_copy(half, k, direction, direction, True).wait_send()
        for k in range(4):
            for d in range(4):
                p_copy(half, k, d).wait_send()
        core_copy(half).wait_send()
        for k in (1, 2, 3):
            for copy in o_copies(k, half):
                copy.wait_send()
            line_copy(half, k).wait_send()
            sx_copy(half, k).wait_send()
            sz_copy(half, k).wait_send()

        @pl.when(rank != (15 if half == 0 else 0))
        def _():
            h_copy(half).wait_send()

    for d in (1, 2, 3):
        q_copy(d).wait_send()


def on_device(
    incoming,
    queries,
    key_vecs,
    value_vecs,
    w_out,
    norm_gain,
    filters,
    filter_len,
    skip_gain,
    slot_map,
):
    dma = pltpu.SemaphoreType.DMA
    vmem = pl.BlockSpec(memory_space=pltpu.VMEM)
    return pl.pallas_call(
        layer_kernel,
        out_shape=jax.ShapeDtypeStruct(queries.shape, BF),
        in_specs=[pl.BlockSpec(memory_space=pltpu.SMEM)] + [vmem] * 9,
        out_specs=vmem,
        scratch_shapes=[
            pltpu.VMEM((4, 2, SPAN, HD), BF),
            pltpu.VMEM((4, 2, 2, SPAN, HD), BF),
            pltpu.VMEM((4, 2, SPAN, HD), F32),
            pltpu.VMEM((4, 2, SPAN, HD), F32),
            pltpu.VMEM((4, 2, SPAN, HD), F32),
            pltpu.VMEM((3, 2, SPAN, HD), BF),
            pltpu.VMEM((3, 2, 8, HD), F32),
            pltpu.VMEM((3, 2, SPAN, HD), BF),
            pltpu.VMEM((3, 2, 8, HD), F32),
            pltpu.VMEM((2, 4, 4, 2, SPAN, HD), BF),
            pltpu.VMEM((2, SPAN, HD), F32),
            pltpu.VMEM((FILT, HD), F32),
            pltpu.VMEM((2, 3, 8, HD), F32),
            pltpu.VMEM((2, 8, HD), F32),
            pltpu.VMEM((2, 3, 8, HD), F32),
            pltpu.VMEM((2, 4, 8, HD), F32),
            pltpu.VMEM((2, SPAN, HD), BF),
            pltpu.VMEM((2, SPAN, HD), BF),
            pltpu.VMEM((2, 8, 2 * SPAN + 8, HD), F32),
            pltpu.VMEM((2, SPAN, HD), F32),
            pltpu.VMEM((2, SPAN, HD), F32),
            dma((3,)),
            dma((3,)),
            dma((2, 2, 3)),
            dma((4, 2, 2)),
            dma((3, 2)),
            dma((3, 2)),
            dma((3, 2)),
            dma((3, 2)),
            dma((2, 3)),
            dma((2, 4)),
            dma((2, 4, 2, 3)),
            dma((2, 4, 4, 2)),
            dma((2, 4, 4)),
            dma((2, 4, 4)),
            dma((2, 7)),
            dma((2,)),
            dma((2, 3)),
            dma((2, 4)),
            dma((2,)),
            dma((2,)),
        ],
        compiler_params=pltpu.CompilerParams(collective_id=0, has_side_effects=True),
        name="layer",
    )(
        slot_map,
        queries,
        key_vecs,
        value_vecs,
        incoming,
        w_out,
        norm_gain.reshape(1, HD),
        filters,
        filter_len.reshape(1, HD),
        skip_gain.reshape(1, HD),
    )


def solution(mesh):
    placed = (
        P("seq", "mp"),
        P("seq", "mp"),
        P("seq", "mp"),
        P("seq", "mp"),
        P(None, "mp"),
        P("mp"),
        P("mp", None),
        P("mp"),
        P("mp"),
        P(),
    )
    return jax.shard_map(
        on_device, mesh=mesh, in_specs=placed, out_specs=P("seq", "mp"), check_vma=False
    )
```

```python
import functools
import math

import jax
import jax.numpy as jnp
from jax import lax
from jax.experimental import pallas as pl
from jax.experimental.pallas import tpu as pltpu
from jax.sharding import PartitionSpec as P

D = 4096
HD = 128
SPAN = 256
FILT = 256
EPS = 1e-05
NEG = -1e30
LOG2 = HD ** (-0.5) * math.log2(math.e)
BF = jnp.bfloat16
F32 = jnp.float32
TILE = 64


def remote(src, dst, send_sem, recv_sem, **where):
    return pltpu.make_async_remote_copy(
        src_ref=src,
        dst_ref=dst,
        send_sem=send_sem,
        recv_sem=recv_sem,
        device_id=where,
        device_id_type=pl.DeviceIdType.MESH,
    )


def greet(peers):
    barrier = pltpu.get_barrier_semaphore()
    for peer in peers:
        pl.semaphore_signal(
            barrier, inc=1, device_id=peer, device_id_type=pl.DeviceIdType.MESH
        )
    pl.semaphore_wait(barrier, len(peers))


def to_lanes(rep):
    return jnp.concatenate(
        [rep[k : k + 128].T[0:1] for k in range(0, rep.shape[0], 128)], axis=0
    )


def from_lanes(rows):
    return jnp.concatenate(
        [jnp.broadcast_to(rows[k : k + 1], (128, 128)).T for k in range(rows.shape[0])], axis=0
    )


def layer_kernel(
    slot_ref,
    q_ref,
    k_ref,
    v_ref,
    inc_ref,
    w_ref,
    gain_ref,
    filt_ref,
    flen_ref,
    skip_ref,
    out_ref,
    qb,
    kvb,
    acc,
    peak,
    total,
    osend,
    lsend,
    orecv,
    lrecv,
    gath,
    w_pair,
    sums,
    part_send,
    part_recv,
    resid,
    taps,
    stat,
    stat_x,
    stat_z,
    rb,
    hb,
    scales,
    hs,
    shift,
    conv,
    final,
    q_ssem,
    q_rsem,
    kv_ssem,
    kv_rsem,
    o_ssem,
    o_rsem,
    l_ssem,
    l_rsem,
    z_ssem,
    z_rsem,
    x_ssem,
    x_rsem,
    p_ssem,
    p_rsem,
    w_ssem,
    w_rsem,
    tx_ssem,
    tx_rsem,
    tz_ssem,
    tz_rsem,
    h_ssem,
    h_rsem,
    s_ssem,
    s_rsem,
):
    rank, head = lax.axis_index("seq"), lax.axis_index("mp")
    y, zh = rank // 4, rank % 4
    along_y = [((y + d) % 4) * 4 + zh for d in range(4)]
    along_z = [y * 4 + (zh + d) % 4 for d in range(4)]
    zl, x, core = head // 8, (head // 2) % 4, head % 2
    near = jnp.where(zl == 0, 1, zl - 1)
    far = jnp.where(zl < 2, 3, 0)
    lines = [zl, near, 6 - zl - near - far, far]
    xs = [(x + d) % 4 for d in range(4)]
    partner = head + 1 - 2 * core

    def mp_of(zl_i, x_i, core_i=core):
        return (zl_i * 4 + x_i) * 2 + core_i

    gap = slot_ref[2 * rank] - slot_ref[2 * rank + 1]
    straight = jnp.full((SPAN, HD), gap, jnp.int32) < 0

    def in_order(ref, half):
        one, two = ref[0:SPAN, :].astype(F32), ref[SPAN : 2 * SPAN, :].astype(F32)
        return jnp.where(straight, (one, two)[half], (two, one)[half])

    for half in range(2):
        qb[0, half] = in_order(q_ref, half).astype(BF)
        kvb[0, half, 0] = in_order(k_ref, half).astype(BF)
        kvb[0, half, 1] = in_order(v_ref, half).astype(BF)
    greet(
        [{"seq": along_y[d]} for d in (1, 2, 3)]
        + [{"seq": along_z[d]} for d in (1, 3)]
        + [{"seq": (rank + d) % 16} for d in (1, 15)]
        + [{"mp": partner}]
        + [{"mp": mp_of(zl, xs[d])} for d in (1, 2, 3)]
        + [{"mp": mp_of(zl, xs[d], 1 - core)} for d in (1, 2, 3)]
        + [{"mp": mp_of(lines[k], x)} for k in (1, 2, 3)]
    )

    def kv_copy(direction, half, sub, relay):
        source = 0 if not relay else (3 if direction == 0 else 1)
        target = 2 if relay else (3 if direction == 0 else 1)
        rows = pl.ds(sub * 128, 128)
        return remote(
            kvb.at[source, half, :, rows],
            kvb.at[target, half, :, rows],
            kv_ssem.at[direction, half, 2 if relay else sub],
            kv_rsem.at[target, half, sub],
            seq=along_z[1 if direction == 0 else 3],
        )

    def kv_arrival(slot, half, sub):
        view = kvb.at[slot, half, :, pl.ds(sub * 128, 128)]
        return remote(view, view, kv_ssem.at[0, half, sub], kv_rsem.at[slot, half, sub], seq=rank)

    def q_copy(d):
        return remote(qb.at[0], qb.at[4 - d], q_ssem.at[d - 1], q_rsem.at[3 - d], seq=along_y[d])

    def o_copies(d, half):
        return (
            remote(
                osend.at[d - 1, half],
                orecv.at[3 - d, half],
                o_ssem.at[d - 1, half],
                o_rsem.at[3 - d, half],
                seq=along_y[d],
            ),
            remote(
                lsend.at[d - 1, half],
                lrecv.at[3 - d, half],
                l_ssem.at[d - 1, half],
                l_rsem.at[3 - d, half],
                seq=along_y[d],
            ),
        )

    def line_copy(half, k):
        view = gath.at[half, zl, x]
        return remote(
            view, view, z_ssem.at[half, k - 1], z_rsem.at[half, zl], mp=mp_of(lines[k], x)
        )

    def line_arrival(half, k):
        view = gath.at[half, lines[k], x]
        return remote(view, view, z_ssem.at[half, k - 1], z_rsem.at[half, lines[k]], mp=head)

    def x_copy(half, k, direction, sub, relay):
        source = xs[(3 if direction == 0 else 1) if relay else 0]
        view = gath.at[half, lines[k], source, pl.ds(sub * 128, 128)]
        return remote(
            view,
            view,
            x_ssem.at[half, k, direction, 2 if relay else sub],
            x_rsem.at[half, k, source, sub],
            mp=mp_of(zl, xs[1 if direction == 0 else 3]),
        )

    def x_arrival(half, k, d, sub):
        view = gath.at[half, lines[k], xs[d], pl.ds(sub * 128, 128)]
        return remote(view, view, x_ssem.at[half, k, 0, sub], x_rsem.at[half, k, xs[d], sub], mp=head)

    w_copy = remote(w_ref.at[:, 1 - core], w_pair, w_ssem.at[0], w_rsem.at[0], mp=partner)

    def part_copy(half):
        return remote(
            part_send.at[half], part_recv.at[half], p_ssem.at[half], p_rsem.at[half], mp=partner
        )

    plane = [(d, c) for d in (2, 1, 3, 0) for c in (0, 1) if (d, c) != (0, 0)]

    def sx_copy(half, d, flip):
        return remote(
            stat.at[half, 0],
            stat_x.at[half, x * 2 + core],
            tx_ssem.at[half, d * 2 + flip],
            tx_rsem.at[half, x * 2 + core],
            mp=mp_of(zl, xs[d], core + flip - 2 * core * flip),
        )

    def sx_arrival(half, d, flip):
        spot = xs[d] * 2 + core + flip - 2 * core * flip
        view = stat_x.at[half, spot]
        return remote(view, view, tx_ssem.at[half, 0], tx_rsem.at[half, spot], mp=head)

    def sz_copy(half, k):
        return remote(
            stat.at[half, 1],
            stat_z.at[half, zl],
            tz_ssem.at[half, k],
            tz_rsem.at[half, zl],
            mp=mp_of(lines[k], x),
        )

    def sz_arrival(half, k):
        view = stat_z.at[half, lines[k]]
        return remote(view, view, tz_ssem.at[half, k], tz_rsem.at[half, lines[k]], mp=head)

    def h_copy(half):
        return remote(
            rb.at[half],
            hb.at[half],
            h_ssem.at[half],
            h_rsem.at[half],
            seq=(rank + (1 if half == 0 else 15)) % 16,
        )

    def s_copy(half):
        return remote(
            scales.at[half],
            hs.at[half],
            s_ssem.at[half],
            s_rsem.at[half],
            seq=(rank + (1 if half == 0 else 15)) % 16,
        )

    for sub in range(2):
        kv_copy(0, 0, sub, False).start()
        kv_copy(1, 0, 1 - sub, False).start()
    for d in (1, 3, 2):
        q_copy(d).start()

    acc[...] = jnp.zeros_like(acc)
    total[...] = jnp.zeros_like(total)
    peak[...] = jnp.full_like(peak, NEG)
    ones = jnp.ones((SPAN, HD), BF)

    def block(d, qhalf, slot, half, diagonal):
        keys, values = kvb[slot, half, 0], kvb[slot, half, 1]
        scores = lax.dot_general(
            qb[d, qhalf], keys, (((1,), (1,)), ((), ())), preferred_element_type=F32
        )
        if diagonal:
            row = lax.broadcasted_iota(jnp.int32, (SPAN, SPAN), 0)
            col = lax.broadcasted_iota(jnp.int32, (SPAN, SPAN), 1)
            scores = jnp.where(col <= row, scores, NEG)
        old = peak[d, qhalf]
        new = jnp.maximum(old, jnp.max(scores, axis=1, keepdims=True))
        weights = jnp.exp2((scores - jnp.concatenate([new, new], axis=1)) * LOG2)
        factor = jnp.exp2((old - new) * LOG2)
        summed = lax.dot_general(
            weights.astype(BF),
            jnp.concatenate([values, ones], axis=1),
            (((1,), (0,)), ((), ())),
            preferred_element_type=F32,
        )
        acc[d, qhalf] = acc[d, qhalf] * factor + summed[:, :HD]
        total[d, qhalf] = total[d, qhalf] * factor + summed[:, HD:]
        peak[d, qhalf] = new

    def visit(d, slot, half):
        q_low = ((y + d) % 4) * 4 + zh
        k_low = y * 4 + (zh + slot) % 4
        if half == 0:
            block(d, 1, slot, 0, False)

            @pl.when(k_low < q_low)
            def _():
                block(d, 0, slot, 0, False)
        else:

            @pl.when(q_low < k_low)
            def _():
                block(d, 1, slot, 1, False)

    def visit_all(slot, half, start):
        def step(d, carry):
            visit(d, slot, half)
            return carry

        lax.fori_loop(start, 4, step, 0)

    def send_partial(half):
        def step(d, carry):
            norm = jnp.maximum(total[d, half], 1e-30)
            osend[d - 1, half] = (acc[d, half] / norm).astype(BF)
            lsend[d - 1, half, 0:2] = to_lanes(peak[d, half] * LOG2 + jnp.log2(norm))
            return carry

        lax.fori_loop(1, 4, step, 0)
        for d in (2, 1, 3):
            for copy in o_copies(d, half):
                copy.start()

    def combine(half):
        for d in (1, 2, 3):
            for copy in o_copies(d, half):
                copy.wait_recv()
        norm = jnp.maximum(total[0, half], 1e-30)
        logs = [peak[0, half] * LOG2 + jnp.log2(norm)]
        logs += [from_lanes(lrecv[s, half, 0:2]) for s in range(3)]
        top = functools.reduce(jnp.maximum, logs)
        shares = [jnp.exp2(log - top) for log in logs]
        mixed = shares[0] * (acc[0, half] / norm)
        for s in range(3):
            mixed = mixed + shares[s + 1] * orecv[s, half].astype(F32)
        gath[half, zl, x] = (mixed / functools.reduce(jnp.add, shares)).astype(BF)

    def send_x(half, k):
        for sub in range(2):
            x_copy(half, k, 0, sub, False).start()
            x_copy(half, k, 1, 1 - sub, False).start()

    def own_out(half):
        for k in (1, 2, 3):
            line_copy(half, k).start()
        send_x(half, 0)

    def line_in(half, k):
        line_arrival(half, k).wait_recv()
        send_x(half, k)

    def x_in(half, k):
        x_arrival(half, k, 3, 0).wait_recv()
        x_copy(half, k, 0, 0, True).start()
        x_arrival(half, k, 1, 1).wait_recv()
        x_copy(half, k, 1, 1, True).start()

    def project(half, k):
        x_arrival(half, k, 3, 1).wait_recv()
        x_arrival(half, k, 1, 0).wait_recv()
        x_arrival(half, k, 2, 0).wait_recv()
        x_arrival(half, k, 2, 1).wait_recv()
        rows = jnp.concatenate([gath[half, lines[k], x_i] for x_i in range(4)], axis=1)
        weights = jnp.concatenate(
            [
                jnp.concatenate(
                    [w_ref[lines[k] * 4 + x_i, core], w_pair[lines[k] * 4 + x_i]], axis=1
                )
                for x_i in range(4)
            ],
            axis=0,
        )
        part = jnp.dot(rows, weights, preferred_element_type=F32)
        if k == 0:
            sums[half] = part
        elif k < 3:
            sums[half] += part
        else:
            both = sums[half] + part
            part_send[half] = both[:, HD:]
            part_copy(half).start()
            resid[half] = in_order(inc_ref, half) + both[:, :HD]

    def finish(half):
        part_copy(half).wait_recv()
        whole = resid[half] + part_recv[half]
        square = whole * whole
        stat[half, 0, 0:2] = jnp.concatenate(
            [jnp.sum(square[k : k + 128].T, axis=0, keepdims=True) for k in (0, 128)], axis=0
        )
        for d, flip in plane:
            sx_copy(half, d, flip).start()
        resid[half] = whole
        rb[half] = whole.astype(BF)

        @pl.when(rank != (15 if half == 0 else 0))
        def _():
            h_copy(half).start()

    def stat_late(half):
        for d, flip in plane:
            sx_arrival(half, d, flip).wait_recv()
        stat_x[half, x * 2 + core, 0:2] = stat[half, 0, 0:2]
        run = stat_x[half, 0, 0:2]
        for k in range(1, 8):
            run = run + stat_x[half, k, 0:2]
        stat[half, 1, 0:2] = run
        for k in (3, 2, 1):
            sz_copy(half, k).start()

    def normalize(half):
        for k in (1, 2, 3):
            sz_arrival(half, k).wait_recv()
        whole = stat[half, 1, 0:2]
        for k in (1, 2, 3):
            whole = whole + stat_z[half, lines[k], 0:2]
        lane_scale = lax.rsqrt(whole / D + EPS)
        scales[half, 0:2] = lane_scale

        @pl.when(rank != (15 if half == 0 else 0))
        def _():
            s_copy(half).start()

        scale = from_lanes(lane_scale)
        normed = (resid[half] * scale * gain_ref[...]).astype(BF)
        wide = normed.astype(F32)
        resid[half] += skip_ref[...] * wide
        for s in range(8):
            shift[half, s, SPAN + s : 2 * SPAN + s, :] = wide

    def lags(half, top, begin, end, start):
        def step(a, run):
            eight = taps[pl.ds(pl.multiple_of(a * 8, 8), 8), :]
            rows = pl.ds(pl.multiple_of(SPAN + top - a * 8, 8), TILE)
            for s in range(8):
                run = run + eight[s : s + 1] * shift[half, s, rows, :]
            return run

        return lax.fori_loop(begin, end, step, start)

    def conv_own(half):
        for top in range(TILE, SPAN, TILE):
            conv[half, top : top + TILE, :] = lags(
                half, top, 0, top // 8, jnp.zeros((TILE, HD), F32)
            )

    def conv_rest(half):
        edge = rank == (0 if half == 0 else 15)

        @pl.when(edge)
        def _():
            hb[half] = jnp.zeros((SPAN, HD), BF) if half == 0 else rb[0]
            hs[half, 0:2] = jnp.zeros((2, HD), F32) if half == 0 else scales[0, 0:2]

        @pl.when(jnp.logical_not(edge))
        def _():
            h_copy(half).wait_recv()
            s_copy(half).wait_recv()

        rows = hb[half].astype(F32) * from_lanes(hs[half, 0:2]) * gain_ref[...]
        before = rows.astype(BF).astype(F32)
        for s in range(8):
            shift[half, s, s : SPAN + s, :] = before
        for top in range(0, SPAN, TILE):
            begin = jnp.zeros((TILE, HD), F32) if top == 0 else conv[half, top : top + TILE, :]
            final[half, top : top + TILE, :] = resid[half, top : top + TILE, :] + lags(
                half, top, top // 8, FILT // 8, begin
            )

    def low_relay(half):
        kv_arrival(3, half, 0).wait_recv()
        kv_copy(0, half, 0, True).start()
        kv_arrival(1, half, 1).wait_recv()
        kv_copy(1, half, 1, True).start()

    def send_high(sub):
        kv_copy(0, 1, sub, False).start()
        kv_copy(1, 1, 1 - sub, False).start()

    w_copy.start()
    block(0, 0, 0, 0, True)
    block(0, 1, 0, 0, False)
    block(0, 1, 0, 1, True)
    lag = lax.broadcasted_iota(jnp.int32, (FILT, HD), 0)
    turned = jnp.concatenate(
        [filt_ref[:, k : k + 128].astype(F32).T for k in (0, 128)], axis=0
    )
    taps[...] = jnp.where(lag < flen_ref[...], turned, 0.0)
    for d in (1, 2, 3):
        q_copy(d).wait_recv()
    visit_all(0, 0, 1)
    low_relay(0)
    visit_all(0, 1, 1)
    kv_arrival(3, 0, 1).wait_recv()
    send_high(0)
    visit_all(3, 0, 0)
    kv_arrival(1, 0, 0).wait_recv()
    send_high(1)
    visit_all(1, 0, 0)
    kv_arrival(2, 0, 0).wait_recv()
    kv_arrival(2, 0, 1).wait_recv()
    visit_all(2, 0, 0)
    send_partial(0)
    low_relay(1)
    combine(0)
    own_out(0)
    w_copy.wait_recv()
    x_in(0, 0)
    kv_arrival(3, 1, 1).wait_recv()
    visit_all(3, 1, 0)
    line_in(0, 1)
    kv_arrival(1, 1, 0).wait_recv()
    visit_all(1, 1, 0)
    line_in(0, 2)
    x_in(0, 1)
    line_in(0, 3)
    kv_arrival(2, 1, 0).wait_recv()
    kv_arrival(2, 1, 1).wait_recv()
    visit_all(2, 1, 0)
    send_partial(1)
    project(0, 0)
    x_in(0, 2)
    project(0, 1)
    combine(1)
    own_out(1)
    x_in(0, 3)
    project(0, 2)
    line_in(1, 1)
    x_in(1, 0)
    line_in(1, 2)
    project(0, 3)
    line_in(1, 3)
    x_in(1, 1)
    finish(0)
    project(1, 0)
    x_in(1, 2)
    stat_late(0)
    project(1, 1)
    x_in(1, 3)
    normalize(0)
    project(1, 2)
    project(1, 3)
    conv_own(0)
    finish(1)
    conv_rest(0)
    stat_late(1)
    normalize(1)
    conv_own(1)
    conv_rest(1)
    low, high = final[0], final[1]
    out_ref[0:SPAN, :] = jnp.where(straight, low, high).astype(BF)
    out_ref[SPAN : 2 * SPAN, :] = jnp.where(straight, high, low).astype(BF)

    for half in range(2):
        for direction in range(2):
            for sub in range(2):
                kv_copy(direction, half, sub, False).wait_send()
            kv_copy(direction, half, direction, True).wait_send()
            for k in range(4):
                for sub in range(2):
                    x_copy(half, k, direction, sub, False).wait_send()
                x_copy(half, k, direction, direction, True).wait_send()
        part_copy(half).wait_send()
        for d, flip in plane:
            sx_copy(half, d, flip).wait_send()
        for k in (1, 2, 3):
            for copy in o_copies(k, half):
                copy.wait_send()
            line_copy(half, k).wait_send()
            sz_copy(half, k).wait_send()

        @pl.when(rank != (15 if half == 0 else 0))
        def _():
            h_copy(half).wait_send()
            s_copy(half).wait_send()

    w_copy.wait_send()
    for d in (1, 2, 3):
        q_copy(d).wait_send()


def on_device(
    incoming,
    queries,
    key_vecs,
    value_vecs,
    w_out,
    norm_gain,
    filters,
    filter_len,
    skip_gain,
    slot_map,
):
    dma = pltpu.SemaphoreType.DMA
    vmem = pl.BlockSpec(memory_space=pltpu.VMEM)
    return pl.pallas_call(
        layer_kernel,
        out_shape=jax.ShapeDtypeStruct(queries.shape, BF),
        in_specs=[pl.BlockSpec(memory_space=pltpu.SMEM)] + [vmem] * 9,
        out_specs=vmem,
        scratch_shapes=[
            pltpu.VMEM((4, 2, SPAN, HD), BF),
            pltpu.VMEM((4, 2, 2, SPAN, HD), BF),
            pltpu.VMEM((4, 2, SPAN, HD), F32),
            pltpu.VMEM((4, 2, SPAN, HD), F32),
            pltpu.VMEM((4, 2, SPAN, HD), F32),
            pltpu.VMEM((3, 2, SPAN, HD), BF),
            pltpu.VMEM((3, 2, 8, HD), F32),
            pltpu.VMEM((3, 2, SPAN, HD), BF),
            pltpu.VMEM((3, 2, 8, HD), F32),
            pltpu.VMEM((2, 4, 4, SPAN, HD), BF),
            pltpu.VMEM((16, HD, HD), BF),
            pltpu.VMEM((2, SPAN, 2 * HD), F32),
            pltpu.VMEM((2, SPAN, HD), F32),
            pltpu.VMEM((2, SPAN, HD), F32),
            pltpu.VMEM((2, SPAN, HD), F32),
            pltpu.VMEM((FILT, HD), F32),
            pltpu.VMEM((2, 2, 8, HD), F32),
            pltpu.VMEM((2, 8, 8, HD), F32),
            pltpu.VMEM((2, 4, 8, HD), F32),
            pltpu.VMEM((2, SPAN, HD), BF),
            pltpu.VMEM((2, SPAN, HD), BF),
            pltpu.VMEM((2, 8, HD), F32),
            pltpu.VMEM((2, 8, HD), F32),
            pltpu.VMEM((2, 8, 2 * SPAN + 8, HD), F32),
            pltpu.VMEM((2, SPAN, HD), F32),
            pltpu.VMEM((2, SPAN, HD), F32),
            dma((3,)),
            dma((3,)),
            dma((2, 2, 3)),
            dma((4, 2, 2)),
            dma((3, 2)),
            dma((3, 2)),
            dma((3, 2)),
            dma((3, 2)),
            dma((2, 3)),
            dma((2, 4)),
            dma((2, 4, 2, 3)),
            dma((2, 4, 4, 2)),
            dma((2,)),
            dma((2,)),
            dma((1,)),
            dma((1,)),
            dma((2, 8)),
            dma((2, 8)),
            dma((2, 4)),
            dma((2, 4)),
            dma((2,)),
            dma((2,)),
            dma((2,)),
            dma((2,)),
        ],
        compiler_params=pltpu.CompilerParams(collective_id=0, has_side_effects=True),
        name="layer",
    )(
        slot_map,
        queries,
        key_vecs,
        value_vecs,
        incoming,
        w_out.reshape(16, 2, HD, HD),
        norm_gain.reshape(1, HD),
        filters,
        filter_len.reshape(1, HD),
        skip_gain.reshape(1, HD),
    )


def solution(mesh):
    placed = (
        P("seq", "mp"),
        P("seq", "mp"),
        P("seq", "mp"),
        P("seq", "mp"),
        P(None, "mp"),
        P("mp"),
        P("mp", None),
        P("mp"),
        P("mp"),
        P(),
    )
    return jax.shard_map(
        on_device, mesh=mesh, in_specs=placed, out_specs=P("seq", "mp"), check_vma=False
    )
```

```python
import functools
import math

import jax
import jax.numpy as jnp
from jax import lax
from jax.experimental import pallas as pl
from jax.experimental.pallas import tpu as pltpu
from jax.sharding import PartitionSpec as P

D = 4096
HD = 128
SPAN = 256
FILT = 256
EPS = 1e-05
NEG = -1e30
LOG2 = HD ** (-0.5) * math.log2(math.e)
BF = jnp.bfloat16
F32 = jnp.float32
TILE = 64


def remote(src, dst, send_sem, recv_sem, **where):
    return pltpu.make_async_remote_copy(
        src_ref=src,
        dst_ref=dst,
        send_sem=send_sem,
        recv_sem=recv_sem,
        device_id=where,
        device_id_type=pl.DeviceIdType.MESH,
    )


def to_lanes(rep):
    return jnp.concatenate(
        [rep[k : k + 128].T[0:1] for k in range(0, rep.shape[0], 128)], axis=0
    )


def from_lanes(rows):
    return jnp.concatenate(
        [jnp.broadcast_to(rows[k : k + 1], (128, 128)).T for k in range(rows.shape[0])], axis=0
    )


def layer_kernel(
    slot_ref,
    q_hbm,
    k_hbm,
    v_hbm,
    w_hbm,
    inc_hbm,
    filt_hbm,
    gain_hbm,
    flen_hbm,
    skip_hbm,
    out_ref,
    q_ref,
    k_ref,
    v_ref,
    w_ref,
    inc_ref,
    filt_ref,
    gain_ref,
    flen_ref,
    skip_ref,
    qb,
    kvb,
    acc,
    peak,
    total,
    osend,
    lsend,
    orecv,
    lrecv,
    gath,
    w_pair,
    sums,
    part_send,
    part_recv,
    resid,
    taps,
    stat,
    stat_x,
    stat_z,
    rb,
    hb,
    scales,
    hs,
    shift,
    conv,
    final,
    q_ssem,
    q_rsem,
    kv_ssem,
    kv_rsem,
    o_ssem,
    o_rsem,
    l_ssem,
    l_rsem,
    z_ssem,
    z_rsem,
    x_ssem,
    x_rsem,
    p_ssem,
    p_rsem,
    w_ssem,
    w_rsem,
    tx_ssem,
    tx_rsem,
    tz_ssem,
    tz_rsem,
    h_ssem,
    h_rsem,
    s_ssem,
    s_rsem,
    in_sem,
):
    arrays = (q_hbm, k_hbm, v_hbm, w_hbm, inc_hbm, filt_hbm, gain_hbm, flen_hbm, skip_hbm)
    held = (q_ref, k_ref, v_ref, w_ref, inc_ref, filt_ref, gain_ref, flen_ref, skip_ref)
    rank, head = lax.axis_index("seq"), lax.axis_index("mp")
    y, zh = rank // 4, rank % 4
    along_y = [((y + d) % 4) * 4 + zh for d in range(4)]
    along_z = [y * 4 + (zh + d) % 4 for d in range(4)]
    zl, x, core = head // 8, (head // 2) % 4, head % 2
    near = jnp.where(zl == 0, 1, zl - 1)
    far = jnp.where(zl < 2, 3, 0)
    lines = [zl, near, 6 - zl - near - far, far]
    xs = [(x + d) % 4 for d in range(4)]
    partner = head + 1 - 2 * core

    def mp_of(zl_i, x_i, core_i=core):
        return (zl_i * 4 + x_i) * 2 + core_i

    peers = (
        [{"seq": along_y[d]} for d in (1, 2, 3)]
        + [{"seq": along_z[d]} for d in (1, 3)]
        + [{"seq": (rank + d) % 16} for d in (1, 15)]
        + [{"mp": partner}]
        + [{"mp": mp_of(zl, xs[d])} for d in (1, 2, 3)]
        + [{"mp": mp_of(zl, xs[d], 1 - core)} for d in (1, 2, 3)]
        + [{"mp": mp_of(lines[k], x)} for k in (1, 2, 3)]
    )
    barrier = pltpu.get_barrier_semaphore()
    for peer in peers:
        pl.semaphore_signal(
            barrier, inc=1, device_id=peer, device_id_type=pl.DeviceIdType.MESH
        )
    loads = [
        pltpu.make_async_copy(src, dst, in_sem.at[k])
        for k, (src, dst) in enumerate(zip(arrays, held))
    ]
    for load in loads:
        load.start()
    gap = slot_ref[2 * rank] - slot_ref[2 * rank + 1]
    straight = jnp.full((SPAN, HD), gap, jnp.int32) < 0

    def in_order(ref, half):
        one, two = ref[0:SPAN, :].astype(F32), ref[SPAN : 2 * SPAN, :].astype(F32)
        return jnp.where(straight, (one, two)[half], (two, one)[half])

    for load in loads[:3]:
        load.wait()
    for half in range(2):
        qb[0, half] = in_order(q_ref, half).astype(BF)
        kvb[0, half, 0] = in_order(k_ref, half).astype(BF)
        kvb[0, half, 1] = in_order(v_ref, half).astype(BF)
    for load in loads[3:]:
        load.wait()
    pl.semaphore_wait(barrier, len(peers))

    def kv_copy(direction, half, sub, relay):
        source = 0 if not relay else (3 if direction == 0 else 1)
        target = 2 if relay else (3 if direction == 0 else 1)
        rows = pl.ds(sub * 128, 128)
        return remote(
            kvb.at[source, half, :, rows],
            kvb.at[target, half, :, rows],
            kv_ssem.at[direction, half, 2 if relay else sub],
            kv_rsem.at[target, half, sub],
            seq=along_z[1 if direction == 0 else 3],
        )

    def kv_arrival(slot, half, sub):
        view = kvb.at[slot, half, :, pl.ds(sub * 128, 128)]
        return remote(view, view, kv_ssem.at[0, half, sub], kv_rsem.at[slot, half, sub], seq=rank)

    def q_copy(d):
        return remote(qb.at[0], qb.at[4 - d], q_ssem.at[d - 1], q_rsem.at[3 - d], seq=along_y[d])

    def o_copies(d, half):
        return (
            remote(
                osend.at[d - 1, half],
                orecv.at[3 - d, half],
                o_ssem.at[d - 1, half],
                o_rsem.at[3 - d, half],
                seq=along_y[d],
            ),
            remote(
                lsend.at[d - 1, half],
                lrecv.at[3 - d, half],
                l_ssem.at[d - 1, half],
                l_rsem.at[3 - d, half],
                seq=along_y[d],
            ),
        )

    def line_copy(half, k):
        view = gath.at[half, zl, x]
        return remote(
            view, view, z_ssem.at[half, k - 1], z_rsem.at[half, zl], mp=mp_of(lines[k], x)
        )

    def line_arrival(half, k):
        view = gath.at[half, lines[k], x]
        return remote(view, view, z_ssem.at[half, k - 1], z_rsem.at[half, lines[k]], mp=head)

    def x_copy(half, k, direction, sub, relay):
        source = xs[(3 if direction == 0 else 1) if relay else 0]
        view = gath.at[half, lines[k], source, pl.ds(sub * 128, 128)]
        return remote(
            view,
            view,
            x_ssem.at[half, k, direction, 2 if relay else sub],
            x_rsem.at[half, k, source, sub],
            mp=mp_of(zl, xs[1 if direction == 0 else 3]),
        )

    def x_arrival(half, k, d, sub):
        view = gath.at[half, lines[k], xs[d], pl.ds(sub * 128, 128)]
        return remote(view, view, x_ssem.at[half, k, 0, sub], x_rsem.at[half, k, xs[d], sub], mp=head)

    w_copy = remote(w_ref.at[:, 1 - core], w_pair, w_ssem.at[0], w_rsem.at[0], mp=partner)

    def part_copy(half):
        return remote(
            part_send.at[half], part_recv.at[half], p_ssem.at[half], p_rsem.at[half], mp=partner
        )

    plane = [(d, c) for d in (2, 1, 3, 0) for c in (0, 1) if (d, c) != (0, 0)]

    def sx_copy(half, d, flip):
        return remote(
            stat.at[half, 0],
            stat_x.at[half, x * 2 + core],
            tx_ssem.at[half, d * 2 + flip],
            tx_rsem.at[half, x * 2 + core],
            mp=mp_of(zl, xs[d], core + flip - 2 * core * flip),
        )

    def sx_arrival(half, d, flip):
        spot = xs[d] * 2 + core + flip - 2 * core * flip
        view = stat_x.at[half, spot]
        return remote(view, view, tx_ssem.at[half, 0], tx_rsem.at[half, spot], mp=head)

    def sz_copy(half, k):
        return remote(
            stat.at[half, 1],
            stat_z.at[half, zl],
            tz_ssem.at[half, k],
            tz_rsem.at[half, zl],
            mp=mp_of(lines[k], x),
        )

    def sz_arrival(half, k):
        view = stat_z.at[half, lines[k]]
        return remote(view, view, tz_ssem.at[half, k], tz_rsem.at[half, lines[k]], mp=head)

    def h_copy(half):
        return remote(
            rb.at[half],
            hb.at[half],
            h_ssem.at[half],
            h_rsem.at[half],
            seq=(rank + (1 if half == 0 else 15)) % 16,
        )

    def s_copy(half):
        return remote(
            scales.at[half],
            hs.at[half],
            s_ssem.at[half],
            s_rsem.at[half],
            seq=(rank + (1 if half == 0 else 15)) % 16,
        )

    for sub in range(2):
        kv_copy(0, 0, sub, False).start()
        kv_copy(1, 0, 1 - sub, False).start()
    for d in (1, 3, 2):
        q_copy(d).start()

    acc[...] = jnp.zeros_like(acc)
    total[...] = jnp.zeros_like(total)
    peak[...] = jnp.full_like(peak, NEG)
    ones = jnp.ones((SPAN, HD), BF)

    def block(d, qhalf, slot, half, diagonal):
        keys, values = kvb[slot, half, 0], kvb[slot, half, 1]
        scores = lax.dot_general(
            qb[d, qhalf], keys, (((1,), (1,)), ((), ())), preferred_element_type=F32
        )
        if diagonal:
            row = lax.broadcasted_iota(jnp.int32, (SPAN, SPAN), 0)
            col = lax.broadcasted_iota(jnp.int32, (SPAN, SPAN), 1)
            scores = jnp.where(col <= row, scores, NEG)
        old = peak[d, qhalf]
        new = jnp.maximum(old, jnp.max(scores, axis=1, keepdims=True))
        weights = jnp.exp2((scores - jnp.concatenate([new, new], axis=1)) * LOG2)
        factor = jnp.exp2((old - new) * LOG2)
        summed = lax.dot_general(
            weights.astype(BF),
            jnp.concatenate([values, ones], axis=1),
            (((1,), (0,)), ((), ())),
            preferred_element_type=F32,
        )
        acc[d, qhalf] = acc[d, qhalf] * factor + summed[:, :HD]
        total[d, qhalf] = total[d, qhalf] * factor + summed[:, HD:]
        peak[d, qhalf] = new

    def visit(d, slot, half):
        q_low = ((y + d) % 4) * 4 + zh
        k_low = y * 4 + (zh + slot) % 4
        if half == 0:
            block(d, 1, slot, 0, False)

            @pl.when(k_low < q_low)
            def _():
                block(d, 0, slot, 0, False)
        else:

            @pl.when(q_low < k_low)
            def _():
                block(d, 1, slot, 1, False)

    def visit_all(slot, half, start):
        def step(d, carry):
            visit(d, slot, half)
            return carry

        lax.fori_loop(start, 4, step, 0)

    def send_partial(half):
        def step(d, carry):
            norm = jnp.maximum(total[d, half], 1e-30)
            osend[d - 1, half] = (acc[d, half] / norm).astype(BF)
            lsend[d - 1, half, 0:2] = to_lanes(peak[d, half] * LOG2 + jnp.log2(norm))
            return carry

        lax.fori_loop(1, 4, step, 0)
        for d in (2, 1, 3):
            for copy in o_copies(d, half):
                copy.start()

    def combine(half):
        for d in (1, 2, 3):
            for copy in o_copies(d, half):
                copy.wait_recv()
        norm = jnp.maximum(total[0, half], 1e-30)
        logs = [peak[0, half] * LOG2 + jnp.log2(norm)]
        logs += [from_lanes(lrecv[s, half, 0:2]) for s in range(3)]
        top = functools.reduce(jnp.maximum, logs)
        shares = [jnp.exp2(log - top) for log in logs]
        mixed = shares[0] * (acc[0, half] / norm)
        for s in range(3):
            mixed = mixed + shares[s + 1] * orecv[s, half].astype(F32)
        gath[half, zl, x] = (mixed / functools.reduce(jnp.add, shares)).astype(BF)

    def send_x(half, k):
        for sub in range(2):
            x_copy(half, k, 0, sub, False).start()
            x_copy(half, k, 1, 1 - sub, False).start()

    def own_out(half):
        for k in (1, 2, 3):
            line_copy(half, k).start()
        send_x(half, 0)

    def line_in(half, k):
        line_arrival(half, k).wait_recv()
        send_x(half, k)

    def x_in(half, k):
        x_arrival(half, k, 3, 0).wait_recv()
        x_copy(half, k, 0, 0, True).start()
        x_arrival(half, k, 1, 1).wait_recv()
        x_copy(half, k, 1, 1, True).start()

    def project(half, k):
        x_arrival(half, k, 3, 1).wait_recv()
        x_arrival(half, k, 1, 0).wait_recv()
        x_arrival(half, k, 2, 0).wait_recv()
        x_arrival(half, k, 2, 1).wait_recv()
        rows = jnp.concatenate([gath[half, lines[k], x_i] for x_i in range(4)], axis=1)
        weights = jnp.concatenate(
            [
                jnp.concatenate(
                    [w_ref[lines[k] * 4 + x_i, core], w_pair[lines[k] * 4 + x_i]], axis=1
                )
                for x_i in range(4)
            ],
            axis=0,
        )
        part = jnp.dot(rows, weights, preferred_element_type=F32)
        if k == 0:
            sums[half] = part
        elif k < 3:
            sums[half] += part
        else:
            both = sums[half] + part
            part_send[half] = both[:, HD:]
            part_copy(half).start()
            resid[half] = in_order(inc_ref, half) + both[:, :HD]

    def finish(half):
        part_copy(half).wait_recv()
        whole = resid[half] + part_recv[half]
        square = whole * whole
        stat[half, 0, 0:2] = jnp.concatenate(
            [jnp.sum(square[k : k + 128].T, axis=0, keepdims=True) for k in (0, 128)], axis=0
        )
        for d, flip in plane:
            sx_copy(half, d, flip).start()
        resid[half] = whole
        rb[half] = whole.astype(BF)

        @pl.when(rank != (15 if half == 0 else 0))
        def _():
            h_copy(half).start()

    def stat_late(half):
        for d, flip in plane:
            sx_arrival(half, d, flip).wait_recv()
        stat_x[half, x * 2 + core, 0:2] = stat[half, 0, 0:2]
        run = stat_x[half, 0, 0:2]
        for k in range(1, 8):
            run = run + stat_x[half, k, 0:2]
        stat[half, 1, 0:2] = run
        for k in (3, 2, 1):
            sz_copy(half, k).start()

    def normalize(half):
        for k in (1, 2, 3):
            sz_arrival(half, k).wait_recv()
        whole = stat[half, 1, 0:2]
        for k in (1, 2, 3):
            whole = whole + stat_z[half, lines[k], 0:2]
        lane_scale = lax.rsqrt(whole / D + EPS)
        scales[half, 0:2] = lane_scale

        @pl.when(rank != (15 if half == 0 else 0))
        def _():
            s_copy(half).start()

        scale = from_lanes(lane_scale)
        normed = (resid[half] * scale * gain_ref[...]).astype(BF)
        wide = normed.astype(F32)
        resid[half] += skip_ref[...] * wide
        for s in range(8):
            shift[half, s, SPAN + s : 2 * SPAN + s, :] = wide

    def lags(half, top, begin, end, start):
        def step(a, run):
            eight = taps[pl.ds(pl.multiple_of(a * 8, 8), 8), :]
            rows = pl.ds(pl.multiple_of(SPAN + top - a * 8, 8), TILE)
            for s in range(8):
                run = run + eight[s : s + 1] * shift[half, s, rows, :]
            return run

        return lax.fori_loop(begin, end, step, start)

    def conv_own(half):
        for top in range(TILE, SPAN, TILE):
            conv[half, top : top + TILE, :] = lags(
                half, top, 0, top // 8, jnp.zeros((TILE, HD), F32)
            )

    def conv_rest(half):
        edge = rank == (0 if half == 0 else 15)

        @pl.when(edge)
        def _():
            hb[half] = jnp.zeros((SPAN, HD), BF) if half == 0 else rb[0]
            hs[half, 0:2] = jnp.zeros((2, HD), F32) if half == 0 else scales[0, 0:2]

        @pl.when(jnp.logical_not(edge))
        def _():
            h_copy(half).wait_recv()
            s_copy(half).wait_recv()

        rows = hb[half].astype(F32) * from_lanes(hs[half, 0:2]) * gain_ref[...]
        before = rows.astype(BF).astype(F32)
        for s in range(8):
            shift[half, s, s : SPAN + s, :] = before
        for top in range(0, SPAN, TILE):
            begin = jnp.zeros((TILE, HD), F32) if top == 0 else conv[half, top : top + TILE, :]
            final[half, top : top + TILE, :] = resid[half, top : top + TILE, :] + lags(
                half, top, top // 8, FILT // 8, begin
            )

    def low_relay(half):
        kv_arrival(3, half, 0).wait_recv()
        kv_copy(0, half, 0, True).start()
        kv_arrival(1, half, 1).wait_recv()
        kv_copy(1, half, 1, True).start()

    def send_high(sub):
        kv_copy(0, 1, sub, False).start()
        kv_copy(1, 1, 1 - sub, False).start()

    w_copy.start()
    block(0, 0, 0, 0, True)
    block(0, 1, 0, 0, False)
    block(0, 1, 0, 1, True)
    lag = lax.broadcasted_iota(jnp.int32, (FILT, HD), 0)
    turned = jnp.concatenate(
        [filt_ref[:, k : k + 128].astype(F32).T for k in (0, 128)], axis=0
    )
    taps[...] = jnp.where(lag < flen_ref[...], turned, 0.0)
    for d in (1, 2, 3):
        q_copy(d).wait_recv()
    visit_all(0, 0, 1)
    low_relay(0)
    visit_all(0, 1, 1)
    kv_arrival(3, 0, 1).wait_recv()
    visit_all(3, 0, 0)
    kv_arrival(1, 0, 0).wait_recv()
    send_high(0)
    visit_all(1, 0, 0)
    send_high(1)
    kv_arrival(2, 0, 0).wait_recv()
    kv_arrival(2, 0, 1).wait_recv()
    visit_all(2, 0, 1)
    send_partial(0)
    visit(0, 2, 0)
    low_relay(1)
    combine(0)
    own_out(0)
    kv_arrival(3, 1, 1).wait_recv()
    visit_all(3, 1, 0)
    kv_arrival(1, 1, 0).wait_recv()
    visit_all(1, 1, 0)
    x_in(0, 0)
    line_in(0, 1)
    kv_arrival(2, 1, 0).wait_recv()
    kv_arrival(2, 1, 1).wait_recv()
    visit_all(2, 1, 1)
    send_partial(1)
    visit(0, 2, 1)
    line_in(0, 2)
    x_in(0, 1)
    line_in(0, 3)
    w_copy.wait_recv()
    combine(1)
    own_out(1)
    project(0, 0)
    x_in(0, 2)
    project(0, 1)
    x_in(0, 3)
    line_in(1, 1)
    x_in(1, 0)
    line_in(1, 2)
    project(0, 2)
    line_in(1, 3)
    x_in(1, 1)
    project(0, 3)
    x_in(1, 2)
    finish(0)
    project(1, 0)
    x_in(1, 3)
    project(1, 1)
    project(1, 2)
    project(1, 3)
    stat_late(0)
    finish(1)
    stat_late(1)
    normalize(0)
    conv_own(0)
    normalize(1)
    conv_own(1)
    conv_rest(0)
    conv_rest(1)
    low, high = final[0], final[1]
    out_ref[0:SPAN, :] = jnp.where(straight, low, high).astype(BF)
    out_ref[SPAN : 2 * SPAN, :] = jnp.where(straight, high, low).astype(BF)

    for half in range(2):
        for direction in range(2):
            for sub in range(2):
                kv_copy(direction, half, sub, False).wait_send()
            kv_copy(direction, half, direction, True).wait_send()
            for k in range(4):
                for sub in range(2):
                    x_copy(half, k, direction, sub, False).wait_send()
                x_copy(half, k, direction, direction, True).wait_send()
        part_copy(half).wait_send()
        for d, flip in plane:
            sx_copy(half, d, flip).wait_send()
        for k in (1, 2, 3):
            for copy in o_copies(k, half):
                copy.wait_send()
            line_copy(half, k).wait_send()
            sz_copy(half, k).wait_send()

        @pl.when(rank != (15 if half == 0 else 0))
        def _():
            h_copy(half).wait_send()
            s_copy(half).wait_send()

    w_copy.wait_send()
    for d in (1, 2, 3):
        q_copy(d).wait_send()


def on_device(
    incoming,
    queries,
    key_vecs,
    value_vecs,
    w_out,
    norm_gain,
    filters,
    filter_len,
    skip_gain,
    slot_map,
):
    dma = pltpu.SemaphoreType.DMA
    vmem = pl.BlockSpec(memory_space=pltpu.VMEM)
    return pl.pallas_call(
        layer_kernel,
        out_shape=jax.ShapeDtypeStruct(queries.shape, BF),
        in_specs=[pl.BlockSpec(memory_space=pltpu.SMEM)] + [pl.BlockSpec(memory_space=pl.ANY)] * 9,
        out_specs=vmem,
        scratch_shapes=[
            pltpu.VMEM((2 * SPAN, HD), BF),
            pltpu.VMEM((2 * SPAN, HD), BF),
            pltpu.VMEM((2 * SPAN, HD), BF),
            pltpu.VMEM((16, 2, HD, HD), BF),
            pltpu.VMEM((2 * SPAN, HD), BF),
            pltpu.VMEM((HD, FILT), BF),
            pltpu.VMEM((1, HD), F32),
            pltpu.VMEM((1, HD), jnp.int32),
            pltpu.VMEM((1, HD), F32),
            pltpu.VMEM((4, 2, SPAN, HD), BF),
            pltpu.VMEM((4, 2, 2, SPAN, HD), BF),
            pltpu.VMEM((4, 2, SPAN, HD), F32),
            pltpu.VMEM((4, 2, SPAN, HD), F32),
            pltpu.VMEM((4, 2, SPAN, HD), F32),
            pltpu.VMEM((3, 2, SPAN, HD), BF),
            pltpu.VMEM((3, 2, 8, HD), F32),
            pltpu.VMEM((3, 2, SPAN, HD), BF),
            pltpu.VMEM((3, 2, 8, HD), F32),
            pltpu.VMEM((2, 4, 4, SPAN, HD), BF),
            pltpu.VMEM((16, HD, HD), BF),
            pltpu.VMEM((2, SPAN, 2 * HD), F32),
            pltpu.VMEM((2, SPAN, HD), F32),
            pltpu.VMEM((2, SPAN, HD), F32),
            pltpu.VMEM((2, SPAN, HD), F32),
            pltpu.VMEM((FILT, HD), F32),
            pltpu.VMEM((2, 2, 8, HD), F32),
            pltpu.VMEM((2, 8, 8, HD), F32),
            pltpu.VMEM((2, 4, 8, HD), F32),
            pltpu.VMEM((2, SPAN, HD), BF),
            pltpu.VMEM((2, SPAN, HD), BF),
            pltpu.VMEM((2, 8, HD), F32),
            pltpu.VMEM((2, 8, HD), F32),
            pltpu.VMEM((2, 8, 2 * SPAN + 8, HD), F32),
            pltpu.VMEM((2, SPAN, HD), F32),
            pltpu.VMEM((2, SPAN, HD), F32),
            dma((3,)),
            dma((3,)),
            dma((2, 2, 3)),
            dma((4, 2, 2)),
            dma((3, 2)),
            dma((3, 2)),
            dma((3, 2)),
            dma((3, 2)),
            dma((2, 3)),
            dma((2, 4)),
            dma((2, 4, 2, 3)),
            dma((2, 4, 4, 2)),
            dma((2,)),
            dma((2,)),
            dma((1,)),
            dma((1,)),
            dma((2, 8)),
            dma((2, 8)),
            dma((2, 4)),
            dma((2, 4)),
            dma((2,)),
            dma((2,)),
            dma((2,)),
            dma((2,)),
            dma((9,)),
        ],
        compiler_params=pltpu.CompilerParams(collective_id=0, has_side_effects=True),
        name="layer",
    )(
        slot_map,
        queries,
        key_vecs,
        value_vecs,
        w_out.reshape(16, 2, HD, HD),
        incoming,
        filters,
        norm_gain.reshape(1, HD),
        filter_len.reshape(1, HD),
        skip_gain.reshape(1, HD),
    )


def solution(mesh):
    placed = (
        P("seq", "mp"),
        P("seq", "mp"),
        P("seq", "mp"),
        P("seq", "mp"),
        P(None, "mp"),
        P("mp"),
        P("mp", None),
        P("mp"),
        P("mp"),
        P(),
    )
    return jax.shard_map(
        on_device, mesh=mesh, in_specs=placed, out_specs=P("seq", "mp"), check_vma=False
    )
```

```python
import functools
import math

import jax
import jax.numpy as jnp
from jax import lax
from jax.experimental import pallas as pl
from jax.experimental.pallas import tpu as pltpu
from jax.sharding import PartitionSpec as P

D = 4096
HD = 128
SPAN = 256
FILT = 256
EPS = 1e-05
NEG = -1e30
LOG2 = HD ** (-0.5) * math.log2(math.e)
BF = jnp.bfloat16
F32 = jnp.float32
TILE = 64


def remote(src, dst, send_sem, recv_sem, **where):
    return pltpu.make_async_remote_copy(
        src_ref=src,
        dst_ref=dst,
        send_sem=send_sem,
        recv_sem=recv_sem,
        device_id=where,
        device_id_type=pl.DeviceIdType.MESH,
    )


def to_lanes(rep):
    return jnp.concatenate(
        [rep[k : k + 128].T[0:1] for k in range(0, rep.shape[0], 128)], axis=0
    )


def from_lanes(rows):
    return jnp.concatenate(
        [jnp.broadcast_to(rows[k : k + 1], (128, 128)).T for k in range(rows.shape[0])], axis=0
    )


def layer_kernel(
    slot_ref,
    q_hbm,
    k_hbm,
    v_hbm,
    w_hbm,
    inc_hbm,
    filt_hbm,
    gain_hbm,
    flen_hbm,
    skip_hbm,
    out_ref,
    q_ref,
    k_ref,
    v_ref,
    w_ref,
    inc_ref,
    filt_ref,
    gain_ref,
    flen_ref,
    skip_ref,
    qb,
    kvb,
    acc,
    peak,
    total,
    osend,
    lsend,
    orecv,
    lrecv,
    gath,
    w_pair,
    sums,
    part_send,
    part_recv,
    resid,
    taps,
    stat,
    stat_all,
    rb,
    hb,
    scales,
    hs,
    shift,
    conv,
    final,
    q_ssem,
    q_rsem,
    kv_ssem,
    kv_rsem,
    o_ssem,
    o_rsem,
    l_ssem,
    l_rsem,
    z_ssem,
    z_rsem,
    x_ssem,
    x_rsem,
    p_ssem,
    p_rsem,
    w_ssem,
    w_rsem,
    t_ssem,
    t_rsem,
    h_ssem,
    h_rsem,
    s_ssem,
    s_rsem,
    in_sem,
):
    arrays = (q_hbm, k_hbm, v_hbm, w_hbm, inc_hbm, filt_hbm, gain_hbm, flen_hbm, skip_hbm)
    held = (q_ref, k_ref, v_ref, w_ref, inc_ref, filt_ref, gain_ref, flen_ref, skip_ref)
    rank, head = lax.axis_index("seq"), lax.axis_index("mp")
    y, zh = rank // 4, rank % 4
    along_y = [((y + d) % 4) * 4 + zh for d in range(4)]
    along_z = [y * 4 + (zh + d) % 4 for d in range(4)]
    zl, x, core = head // 8, (head // 2) % 4, head % 2
    near = jnp.where(zl == 0, 1, zl - 1)
    far = jnp.where(zl < 2, 3, 0)
    lines = [zl, near, 6 - zl - near - far, far]
    xs = [(x + d) % 4 for d in range(4)]
    partner = head + 1 - 2 * core

    def mp_of(zl_i, x_i, core_i=core):
        return (zl_i * 4 + x_i) * 2 + core_i

    peers = (
        [{"seq": along_y[d]} for d in (1, 2, 3)]
        + [{"seq": along_z[d]} for d in (1, 3)]
        + [{"seq": (rank + d) % 16} for d in (1, 15)]
    )
    barrier = pltpu.get_barrier_semaphore()
    for peer in peers:
        pl.semaphore_signal(
            barrier, inc=1, device_id=peer, device_id_type=pl.DeviceIdType.MESH
        )

    def greet(j, carry):
        pl.semaphore_signal(
            barrier, inc=1, device_id={"mp": (head + j) % 32}, device_id_type=pl.DeviceIdType.MESH
        )
        return carry

    lax.fori_loop(1, 32, greet, 0)
    loads = [
        pltpu.make_async_copy(src, dst, in_sem.at[k])
        for k, (src, dst) in enumerate(zip(arrays, held))
    ]
    for load in loads:
        load.start()
    gap = slot_ref[2 * rank] - slot_ref[2 * rank + 1]
    straight = jnp.full((SPAN, HD), gap, jnp.int32) < 0

    def in_order(ref, half):
        one, two = ref[0:SPAN, :].astype(F32), ref[SPAN : 2 * SPAN, :].astype(F32)
        return jnp.where(straight, (one, two)[half], (two, one)[half])

    for load in loads[:3]:
        load.wait()
    for half in range(2):
        qb[0, half] = in_order(q_ref, half).astype(BF)
        kvb[0, half, 0] = in_order(k_ref, half).astype(BF)
        kvb[0, half, 1] = in_order(v_ref, half).astype(BF)
    for load in loads[3:]:
        load.wait()
    pl.semaphore_wait(barrier, len(peers) + 31)

    def kv_copy(direction, half, sub, relay):
        source = 0 if not relay else (3 if direction == 0 else 1)
        target = 2 if relay else (3 if direction == 0 else 1)
        rows = pl.ds(sub * 128, 128)
        return remote(
            kvb.at[source, half, :, rows],
            kvb.at[target, half, :, rows],
            kv_ssem.at[direction, half, 2 if relay else sub],
            kv_rsem.at[target, half, sub],
            seq=along_z[1 if direction == 0 else 3],
        )

    def kv_arrival(slot, half, sub):
        view = kvb.at[slot, half, :, pl.ds(sub * 128, 128)]
        return remote(view, view, kv_ssem.at[0, half, sub], kv_rsem.at[slot, half, sub], seq=rank)

    def q_copy(d):
        return remote(qb.at[0], qb.at[4 - d], q_ssem.at[d - 1], q_rsem.at[3 - d], seq=along_y[d])

    def o_copies(d, half):
        return (
            remote(
                osend.at[d - 1, half],
                orecv.at[3 - d, half],
                o_ssem.at[d - 1, half],
                o_rsem.at[3 - d, half],
                seq=along_y[d],
            ),
            remote(
                lsend.at[d - 1, half],
                lrecv.at[3 - d, half],
                l_ssem.at[d - 1, half],
                l_rsem.at[3 - d, half],
                seq=along_y[d],
            ),
        )

    def line_copy(half, k):
        view = gath.at[half, zl, x]
        return remote(
            view, view, z_ssem.at[half, k - 1], z_rsem.at[half, zl], mp=mp_of(lines[k], x)
        )

    def line_arrival(half, k):
        view = gath.at[half, lines[k], x]
        return remote(view, view, z_ssem.at[half, k - 1], z_rsem.at[half, lines[k]], mp=head)

    def x_copy(half, k, direction, sub, relay):
        source = xs[(3 if direction == 0 else 1) if relay else 0]
        view = gath.at[half, lines[k], source, pl.ds(sub * 128, 128)]
        return remote(
            view,
            view,
            x_ssem.at[half, k, direction, 2 if relay else sub],
            x_rsem.at[half, k, source, sub],
            mp=mp_of(zl, xs[1 if direction == 0 else 3]),
        )

    def x_arrival(half, k, d, sub):
        view = gath.at[half, lines[k], xs[d], pl.ds(sub * 128, 128)]
        return remote(view, view, x_ssem.at[half, k, 0, sub], x_rsem.at[half, k, xs[d], sub], mp=head)

    w_copy = remote(w_ref.at[:, 1 - core], w_pair, w_ssem.at[0], w_rsem.at[0], mp=partner)

    def part_copy(half):
        return remote(
            part_send.at[half], part_recv.at[half], p_ssem.at[half], p_rsem.at[half], mp=partner
        )

    def stat_copy(half, j):
        return remote(
            stat.at[half],
            stat_all.at[half, head],
            t_ssem.at[half],
            t_rsem.at[half],
            mp=(head + j) % 32,
        )

    def stat_others(half):
        view = stat_all.at[half, pl.ds(0, 31)]
        return remote(view, view, t_ssem.at[half], t_rsem.at[half], mp=head)

    def h_copy(half, part):
        rows = pl.ds(128 - 128 * part, 128)
        return remote(
            rb.at[half, rows],
            hb.at[half, rows],
            h_ssem.at[half, part],
            h_rsem.at[half, part],
            seq=(rank + (1 if half == 0 else 15)) % 16,
        )

    def s_copy(half):
        return remote(
            scales.at[half],
            hs.at[half],
            s_ssem.at[half],
            s_rsem.at[half],
            seq=(rank + (1 if half == 0 else 15)) % 16,
        )

    for sub in range(2):
        kv_copy(0, 0, sub, False).start()
        kv_copy(1, 0, 1 - sub, False).start()
    for d in (1, 3, 2):
        q_copy(d).start()

    acc[...] = jnp.zeros_like(acc)
    total[...] = jnp.zeros_like(total)
    peak[...] = jnp.full_like(peak, NEG)
    ones = jnp.ones((SPAN, HD), BF)

    def block(d, qhalf, slot, half, diagonal):
        keys, values = kvb[slot, half, 0], kvb[slot, half, 1]
        scores = lax.dot_general(
            qb[d, qhalf], keys, (((1,), (1,)), ((), ())), preferred_element_type=F32
        )
        if diagonal:
            row = lax.broadcasted_iota(jnp.int32, (SPAN, SPAN), 0)
            col = lax.broadcasted_iota(jnp.int32, (SPAN, SPAN), 1)
            scores = jnp.where(col <= row, scores, NEG)
        old = peak[d, qhalf]
        new = jnp.maximum(old, jnp.max(scores, axis=1, keepdims=True))
        weights = jnp.exp2((scores - jnp.concatenate([new, new], axis=1)) * LOG2)
        factor = jnp.exp2((old - new) * LOG2)
        summed = lax.dot_general(
            weights.astype(BF),
            jnp.concatenate([values, ones], axis=1),
            (((1,), (0,)), ((), ())),
            preferred_element_type=F32,
        )
        acc[d, qhalf] = acc[d, qhalf] * factor + summed[:, :HD]
        total[d, qhalf] = total[d, qhalf] * factor + summed[:, HD:]
        peak[d, qhalf] = new

    def visit(d, slot, half):
        q_low = ((y + d) % 4) * 4 + zh
        k_low = y * 4 + (zh + slot) % 4
        if half == 0:
            block(d, 1, slot, 0, False)

            @pl.when(k_low < q_low)
            def _():
                block(d, 0, slot, 0, False)
        else:

            @pl.when(q_low < k_low)
            def _():
                block(d, 1, slot, 1, False)

    def visit_all(slot, half, start):
        def step(d, carry):
            visit(d, slot, half)
            return carry

        lax.fori_loop(start, 4, step, 0)

    def send_partial(half):
        def step(d, carry):
            norm = jnp.maximum(total[d, half], 1e-30)
            osend[d - 1, half] = (acc[d, half] / norm).astype(BF)
            lsend[d - 1, half, 0:2] = to_lanes(peak[d, half] * LOG2 + jnp.log2(norm))
            return carry

        lax.fori_loop(1, 4, step, 0)
        for d in (2, 1, 3):
            for copy in o_copies(d, half):
                copy.start()

    def combine(half):
        for d in (1, 2, 3):
            for copy in o_copies(d, half):
                copy.wait_recv()
        norm = jnp.maximum(total[0, half], 1e-30)
        logs = [peak[0, half] * LOG2 + jnp.log2(norm)]
        logs += [from_lanes(lrecv[s, half, 0:2]) for s in range(3)]
        top = functools.reduce(jnp.maximum, logs)
        shares = [jnp.exp2(log - top) for log in logs]
        mixed = shares[0] * (acc[0, half] / norm)
        for s in range(3):
            mixed = mixed + shares[s + 1] * orecv[s, half].astype(F32)
        gath[half, zl, x] = (mixed / functools.reduce(jnp.add, shares)).astype(BF)

    def send_x(half, k):
        for sub in range(2):
            x_copy(half, k, 0, sub, False).start()
            x_copy(half, k, 1, 1 - sub, False).start()

    def own_out(half):
        for k in (1, 2, 3):
            line_copy(half, k).start()
        send_x(half, 0)

    def line_in(half, k):
        line_arrival(half, k).wait_recv()
        send_x(half, k)

    def x_in(half, k):
        x_arrival(half, k, 3, 0).wait_recv()
        x_copy(half, k, 0, 0, True).start()
        x_arrival(half, k, 1, 1).wait_recv()
        x_copy(half, k, 1, 1, True).start()

    def project(half, k):
        x_arrival(half, k, 3, 1).wait_recv()
        x_arrival(half, k, 1, 0).wait_recv()
        x_arrival(half, k, 2, 0).wait_recv()
        x_arrival(half, k, 2, 1).wait_recv()
        rows = jnp.concatenate([gath[half, lines[k], x_i] for x_i in range(4)], axis=1)
        weights = jnp.concatenate(
            [
                jnp.concatenate(
                    [w_ref[lines[k] * 4 + x_i, core], w_pair[lines[k] * 4 + x_i]], axis=1
                )
                for x_i in range(4)
            ],
            axis=0,
        )
        part = jnp.dot(rows, weights, preferred_element_type=F32)
        if k == 0:
            sums[half] = part
        elif k < 3:
            sums[half] += part
        else:
            both = sums[half] + part
            part_send[half] = both[:, HD:]
            part_copy(half).start()
            resid[half] = in_order(inc_ref, half) + both[:, :HD]

    def finish(half):
        part_copy(half).wait_recv()
        whole = resid[half] + part_recv[half]
        square = whole * whole
        resid[half] = whole
        rb[half] = whole.astype(BF)
        stat[half] = jnp.concatenate(
            [jnp.sum(square[k : k + 128].T, axis=0, keepdims=True) for k in (0, 128)], axis=0
        )
        for j in range(31, 0, -1):
            stat_copy(half, j).start()

    def rows_out(half):
        @pl.when(rank != (15 if half == 0 else 0))
        def _():
            for part in range(2):
                h_copy(half, part).start()

    def normalize(half):
        stat_others(half).wait_recv()
        stat_all[half, head] = stat[half]
        whole = jnp.sum(stat_all[half], axis=0)
        lane_scale = lax.rsqrt(whole / D + EPS)
        scales[half, 0:2] = lane_scale

        @pl.when(rank != (15 if half == 0 else 0))
        def _():
            s_copy(half).start()

        scale = from_lanes(lane_scale)
        normed = (resid[half] * scale * gain_ref[...]).astype(BF)
        wide = normed.astype(F32)
        resid[half] += skip_ref[...] * wide
        for s in range(8):
            shift[half, s, SPAN + s : 2 * SPAN + s, :] = wide

    def lags(half, top, begin, end, start):
        def step(a, run):
            eight = taps[pl.ds(pl.multiple_of(a * 8, 8), 8), :]
            rows = pl.ds(pl.multiple_of(SPAN + top - a * 8, 8), TILE)
            for s in range(8):
                run = run + eight[s : s + 1] * shift[half, s, rows, :]
            return run

        return lax.fori_loop(begin, end, step, start)

    def conv_own(half):
        for top in range(TILE, SPAN, TILE):
            conv[half, top : top + TILE, :] = lags(
                half, top, 0, top // 8, jnp.zeros((TILE, HD), F32)
            )

    def conv_rest(half):
        edge = rank == (0 if half == 0 else 15)

        @pl.when(edge)
        def _():
            hb[half] = jnp.zeros((SPAN, HD), BF) if half == 0 else rb[0]
            hs[half, 0:2] = jnp.zeros((2, HD), F32) if half == 0 else scales[0, 0:2]

        def arrived(copy):
            @pl.when(jnp.logical_not(edge))
            def _():
                copy.wait_recv()

        arrived(s_copy(half))
        for part in range(2):
            at = 128 - 128 * part
            arrived(h_copy(half, part))
            scale = from_lanes(hs[half, 1 - part : 2 - part])
            rows = hb[half, at : at + 128, :].astype(F32) * scale * gain_ref[...]
            before = rows.astype(BF).astype(F32)
            for s in range(8):
                shift[half, s, at + s : at + s + 128, :] = before
            for top in range(0, SPAN, TILE):
                turn = min(FILT // 8, top // 8 + 15)
                if part == 0:
                    run = jnp.zeros((TILE, HD), F32) if top == 0 else conv[half, top : top + TILE, :]
                    run = lags(half, top, top // 8, turn, run)
                    if turn < FILT // 8:
                        conv[half, top : top + TILE, :] = run
                        continue
                elif turn < FILT // 8:
                    run = lags(half, top, turn, FILT // 8, conv[half, top : top + TILE, :])
                else:
                    continue
                final[half, top : top + TILE, :] = resid[half, top : top + TILE, :] + run

    def sent():
        for half in range(2):
            for direction in range(2):
                for sub in range(2):
                    kv_copy(direction, half, sub, False).wait_send()
                kv_copy(direction, half, direction, True).wait_send()
                for k in range(4):
                    for sub in range(2):
                        x_copy(half, k, direction, sub, False).wait_send()
                    x_copy(half, k, direction, direction, True).wait_send()
            part_copy(half).wait_send()
            stat_others(half).wait_send()
            for k in (1, 2, 3):
                for copy in o_copies(k, half):
                    copy.wait_send()
                line_copy(half, k).wait_send()

        w_copy.wait_send()
        for d in (1, 2, 3):
            q_copy(d).wait_send()

    def low_relay(half):
        kv_arrival(3, half, 0).wait_recv()
        kv_copy(0, half, 0, True).start()
        kv_arrival(1, half, 1).wait_recv()
        kv_copy(1, half, 1, True).start()

    def send_high(sub):
        kv_copy(0, 1, sub, False).start()
        kv_copy(1, 1, 1 - sub, False).start()

    w_copy.start()
    block(0, 0, 0, 0, True)
    block(0, 1, 0, 0, False)
    block(0, 1, 0, 1, True)
    lag = lax.broadcasted_iota(jnp.int32, (FILT, HD), 0)
    turned = jnp.concatenate(
        [filt_ref[:, k : k + 128].astype(F32).T for k in (0, 128)], axis=0
    )
    taps[...] = jnp.where(lag < flen_ref[...], turned, 0.0)
    for d in (1, 2, 3):
        q_copy(d).wait_recv()
    visit_all(0, 0, 1)
    low_relay(0)
    visit_all(0, 1, 1)
    kv_arrival(3, 0, 1).wait_recv()
    visit_all(3, 0, 0)
    kv_arrival(1, 0, 0).wait_recv()
    send_high(0)
    visit_all(1, 0, 0)
    send_high(1)
    kv_arrival(2, 0, 0).wait_recv()
    kv_arrival(2, 0, 1).wait_recv()
    visit_all(2, 0, 1)
    send_partial(0)
    visit(0, 2, 0)
    low_relay(1)
    combine(0)
    own_out(0)
    kv_arrival(3, 1, 1).wait_recv()
    visit_all(3, 1, 0)
    kv_arrival(1, 1, 0).wait_recv()
    visit_all(1, 1, 0)
    x_in(0, 0)
    line_in(0, 1)
    kv_arrival(2, 1, 0).wait_recv()
    kv_arrival(2, 1, 1).wait_recv()
    visit_all(2, 1, 1)
    send_partial(1)
    visit(0, 2, 1)
    line_in(0, 2)
    x_in(0, 1)
    line_in(0, 3)
    w_copy.wait_recv()
    combine(1)
    own_out(1)
    project(0, 0)
    x_in(0, 2)
    project(0, 1)
    x_in(0, 3)
    line_in(1, 1)
    x_in(1, 0)
    line_in(1, 2)
    project(0, 2)
    line_in(1, 3)
    x_in(1, 1)
    project(0, 3)
    x_in(1, 2)
    finish(0)
    rows_out(0)
    project(1, 0)
    x_in(1, 3)
    project(1, 1)
    project(1, 2)
    project(1, 3)
    finish(1)
    normalize(0)
    conv_own(0)
    rows_out(1)
    sent()
    normalize(1)
    conv_own(1)
    conv_rest(0)
    conv_rest(1)
    low, high = final[0], final[1]
    out_ref[0:SPAN, :] = jnp.where(straight, low, high).astype(BF)
    out_ref[SPAN : 2 * SPAN, :] = jnp.where(straight, high, low).astype(BF)

    for half in range(2):

        @pl.when(rank != (15 if half == 0 else 0))
        def _():
            h_copy(half, 0).wait_send()
            h_copy(half, 1).wait_send()
            s_copy(half).wait_send()


def on_device(
    incoming,
    queries,
    key_vecs,
    value_vecs,
    w_out,
    norm_gain,
    filters,
    filter_len,
    skip_gain,
    slot_map,
):
    dma = pltpu.SemaphoreType.DMA
    vmem = pl.BlockSpec(memory_space=pltpu.VMEM)
    return pl.pallas_call(
        layer_kernel,
        out_shape=jax.ShapeDtypeStruct(queries.shape, BF),
        in_specs=[pl.BlockSpec(memory_space=pltpu.SMEM)] + [pl.BlockSpec(memory_space=pl.ANY)] * 9,
        out_specs=vmem,
        scratch_shapes=[
            pltpu.VMEM((2 * SPAN, HD), BF),
            pltpu.VMEM((2 * SPAN, HD), BF),
            pltpu.VMEM((2 * SPAN, HD), BF),
            pltpu.VMEM((16, 2, HD, HD), BF),
            pltpu.VMEM((2 * SPAN, HD), BF),
            pltpu.VMEM((HD, FILT), BF),
            pltpu.VMEM((1, HD), F32),
            pltpu.VMEM((1, HD), jnp.int32),
            pltpu.VMEM((1, HD), F32),
            pltpu.VMEM((4, 2, SPAN, HD), BF),
            pltpu.VMEM((4, 2, 2, SPAN, HD), BF),
            pltpu.VMEM((4, 2, SPAN, HD), F32),
            pltpu.VMEM((4, 2, SPAN, HD), F32),
            pltpu.VMEM((4, 2, SPAN, HD), F32),
            pltpu.VMEM((3, 2, SPAN, HD), BF),
            pltpu.VMEM((3, 2, 8, HD), F32),
            pltpu.VMEM((3, 2, SPAN, HD), BF),
            pltpu.VMEM((3, 2, 8, HD), F32),
            pltpu.VMEM((2, 4, 4, SPAN, HD), BF),
            pltpu.VMEM((16, HD, HD), BF),
            pltpu.VMEM((2, SPAN, 2 * HD), F32),
            pltpu.VMEM((2, SPAN, HD), F32),
            pltpu.VMEM((2, SPAN, HD), F32),
            pltpu.VMEM((2, SPAN, HD), F32),
            pltpu.VMEM((FILT, HD), F32),
            pltpu.VMEM((2, 2, HD), F32),
            pltpu.VMEM((2, 32, 2, HD), F32),
            pltpu.VMEM((2, SPAN, HD), BF),
            pltpu.VMEM((2, SPAN, HD), BF),
            pltpu.VMEM((2, 8, HD), F32),
            pltpu.VMEM((2, 8, HD), F32),
            pltpu.VMEM((2, 8, 2 * SPAN + 8, HD), F32),
            pltpu.VMEM((2, SPAN, HD), F32),
            pltpu.VMEM((2, SPAN, HD), F32),
            dma((3,)),
            dma((3,)),
            dma((2, 2, 3)),
            dma((4, 2, 2)),
            dma((3, 2)),
            dma((3, 2)),
            dma((3, 2)),
            dma((3, 2)),
            dma((2, 3)),
            dma((2, 4)),
            dma((2, 4, 2, 3)),
            dma((2, 4, 4, 2)),
            dma((2,)),
            dma((2,)),
            dma((1,)),
            dma((1,)),
            dma((2,)),
            dma((2,)),
            dma((2, 2)),
            dma((2, 2)),
            dma((2,)),
            dma((2,)),
            dma((9,)),
        ],
        compiler_params=pltpu.CompilerParams(collective_id=0, has_side_effects=True),
        name="layer",
    )(
        slot_map,
        queries,
        key_vecs,
        value_vecs,
        w_out.reshape(16, 2, HD, HD),
        incoming,
        filters,
        norm_gain.reshape(1, HD),
        filter_len.reshape(1, HD),
        skip_gain.reshape(1, HD),
    )


def solution(mesh):
    placed = (
        P("seq", "mp"),
        P("seq", "mp"),
        P("seq", "mp"),
        P("seq", "mp"),
        P(None, "mp"),
        P("mp"),
        P("mp", None),
        P("mp"),
        P("mp"),
        P(),
    )
    return jax.shard_map(
        on_device, mesh=mesh, in_specs=placed, out_specs=P("seq", "mp"), check_vma=False
    )
```

```python
import functools
import math

import jax
import jax.numpy as jnp
from jax import lax
from jax.experimental import pallas as pl
from jax.experimental.pallas import tpu as pltpu
from jax.sharding import PartitionSpec as P

D = 4096
HD = 128
SPAN = 256
FILT = 256
EPS = 1e-05
NEG = -1e30
LOG2 = HD ** (-0.5) * math.log2(math.e)
BF = jnp.bfloat16
F32 = jnp.float32
TILE = 64


def remote(src, dst, send_sem, recv_sem, **where):
    return pltpu.make_async_remote_copy(
        src_ref=src,
        dst_ref=dst,
        send_sem=send_sem,
        recv_sem=recv_sem,
        device_id=where,
        device_id_type=pl.DeviceIdType.MESH,
    )


def to_lanes(rep):
    return jnp.concatenate(
        [rep[k : k + 128].T[0:1] for k in range(0, rep.shape[0], 128)], axis=0
    )


def from_lanes(rows):
    return jnp.concatenate(
        [jnp.broadcast_to(rows[k : k + 1], (128, 128)).T for k in range(rows.shape[0])], axis=0
    )


def layer_kernel(
    slot_ref,
    q_hbm,
    k_hbm,
    v_hbm,
    w_hbm,
    inc_hbm,
    filt_hbm,
    gain_hbm,
    flen_hbm,
    skip_hbm,
    out_ref,
    q_ref,
    k_ref,
    v_ref,
    w_ref,
    inc_ref,
    filt_ref,
    gain_ref,
    flen_ref,
    skip_ref,
    qb,
    kvb,
    acc,
    peak,
    total,
    osend,
    lsend,
    orecv,
    lrecv,
    gath,
    w_pair,
    sums,
    part_send,
    part_recv,
    resid,
    taps,
    stat,
    stat_all,
    rb,
    hb,
    scales,
    hs,
    shift,
    conv,
    final,
    q_ssem,
    q_rsem,
    kv_ssem,
    kv_rsem,
    o_ssem,
    o_rsem,
    l_ssem,
    l_rsem,
    z_ssem,
    z_rsem,
    x_ssem,
    x_rsem,
    p_ssem,
    p_rsem,
    w_ssem,
    w_rsem,
    t_ssem,
    t_rsem,
    h_ssem,
    h_rsem,
    s_ssem,
    s_rsem,
    in_sem,
):
    arrays = (q_hbm, k_hbm, v_hbm, w_hbm, inc_hbm, filt_hbm, gain_hbm, flen_hbm, skip_hbm)
    held = (q_ref, k_ref, v_ref, w_ref, inc_ref, filt_ref, gain_ref, flen_ref, skip_ref)
    rank, head = lax.axis_index("seq"), lax.axis_index("mp")
    y, zh = rank // 4, rank % 4
    along_y = [((y + d) % 4) * 4 + zh for d in range(4)]
    along_z = [y * 4 + (zh + d) % 4 for d in range(4)]
    zl, x, core = head // 8, (head // 2) % 4, head % 2
    near = jnp.where(zl == 0, 1, zl - 1)
    far = jnp.where(zl < 2, 3, 0)
    lines = [zl, near, 6 - zl - near - far, far]
    xs = [(x + d) % 4 for d in range(4)]
    partner = head + 1 - 2 * core

    def mp_of(zl_i, x_i, core_i=core):
        return (zl_i * 4 + x_i) * 2 + core_i

    peers = (
        [{"seq": along_y[d]} for d in (1, 2, 3)]
        + [{"seq": along_z[d]} for d in (1, 3)]
        + [{"seq": (rank + d) % 16} for d in (1, 15)]
    )
    barrier = pltpu.get_barrier_semaphore()
    for peer in peers:
        pl.semaphore_signal(
            barrier, inc=1, device_id=peer, device_id_type=pl.DeviceIdType.MESH
        )

    def greet(j, carry):
        pl.semaphore_signal(
            barrier, inc=1, device_id={"mp": (head + j) % 32}, device_id_type=pl.DeviceIdType.MESH
        )
        return carry

    lax.fori_loop(1, 32, greet, 0)
    loads = [
        pltpu.make_async_copy(src, dst, in_sem.at[k])
        for k, (src, dst) in enumerate(zip(arrays, held))
    ]
    for load in loads:
        load.start()
    gap = slot_ref[2 * rank] - slot_ref[2 * rank + 1]
    straight = jnp.full((SPAN, HD), gap, jnp.int32) < 0

    def in_order(ref, half):
        one, two = ref[0:SPAN, :].astype(F32), ref[SPAN : 2 * SPAN, :].astype(F32)
        return jnp.where(straight, (one, two)[half], (two, one)[half])

    for load in loads[:3]:
        load.wait()
    for half in range(2):
        qb[0, half] = in_order(q_ref, half).astype(BF)
        kvb[0, half, 0] = in_order(k_ref, half).astype(BF)
        kvb[0, half, 1] = in_order(v_ref, half).astype(BF)
    for load in loads[3:]:
        load.wait()
    pl.semaphore_wait(barrier, len(peers) + 31)

    def in_all(view, send_sem, recv_sem):
        return remote(view, view, send_sem, recv_sem, mp=head)

    def kv_copy(direction, half, sub, relay):
        source = 0 if not relay else (3 if direction == 0 else 1)
        target = 2 if relay else (3 if direction == 0 else 1)
        rows = pl.ds(sub * 128, 128)
        return remote(
            kvb.at[source, half, :, rows],
            kvb.at[target, half, :, rows],
            kv_ssem.at[0],
            kv_rsem.at[target - 1, half, sub],
            seq=along_z[1 if direction == 0 else 3],
        )

    def kv_arrival(slot, half, sub):
        view = kvb.at[slot, half, :, pl.ds(sub * 128, 128)]
        return remote(view, view, kv_ssem.at[0], kv_rsem.at[slot - 1, half, sub], seq=rank)

    def q_copy(d):
        return remote(qb.at[0], qb.at[4 - d], q_ssem.at[0], q_rsem.at[0], seq=along_y[d])

    def o_copies(d, half):
        return (
            remote(
                osend.at[d - 1, half],
                orecv.at[3 - d, half],
                o_ssem.at[0],
                o_rsem.at[half],
                seq=along_y[d],
            ),
            remote(
                lsend.at[d - 1, half],
                lrecv.at[3 - d, half],
                l_ssem.at[0],
                l_rsem.at[half],
                seq=along_y[d],
            ),
        )

    def line_copy(half, k):
        view = gath.at[half, zl, x]
        return remote(
            view, view, z_ssem.at[0], z_rsem.at[half, zl], mp=mp_of(lines[k], x)
        )

    def line_arrival(half, k):
        view = gath.at[half, lines[k], x]
        return remote(view, view, z_ssem.at[0], z_rsem.at[half, lines[k]], mp=head)

    def x_copy(half, k, direction, sub, relay):
        source = xs[(3 if direction == 0 else 1) if relay else 0]
        view = gath.at[half, lines[k], source, pl.ds(sub * 128, 128)]
        return remote(
            view,
            view,
            x_ssem.at[0],
            x_rsem.at[half, k, 1 + direction if not relay and sub == direction else 0],
            mp=mp_of(zl, xs[1 if direction == 0 else 3]),
        )

    def x_arrival(half, k, d, sub):
        view = gath.at[half, lines[k], xs[d], pl.ds(sub * 128, 128)]
        return remote(view, view, x_ssem.at[0], x_rsem.at[half, k, 1 + sub], mp=head)

    w_copy = remote(w_ref.at[:, 1 - core], w_pair, w_ssem.at[0], w_rsem.at[0], mp=partner)

    def part_copy(half):
        return remote(
            part_send.at[half], part_recv.at[half], p_ssem.at[half], p_rsem.at[half], mp=partner
        )

    def stat_copy(half, j):
        return remote(
            stat.at[half],
            stat_all.at[half, head],
            t_ssem.at[half],
            t_rsem.at[half],
            mp=(head + j) % 32,
        )

    def stat_others(half):
        view = stat_all.at[half, pl.ds(0, 31)]
        return remote(view, view, t_ssem.at[half], t_rsem.at[half], mp=head)

    def h_copy(half, part):
        rows = pl.ds(128 - 128 * part, 128)
        return remote(
            rb.at[half, rows],
            hb.at[half, rows],
            h_ssem.at[half, part],
            h_rsem.at[half, part],
            seq=(rank + (1 if half == 0 else 15)) % 16,
        )

    def s_copy(half):
        return remote(
            scales.at[half],
            hs.at[half],
            s_ssem.at[half],
            s_rsem.at[half],
            seq=(rank + (1 if half == 0 else 15)) % 16,
        )

    for sub in range(2):
        kv_copy(0, 0, sub, False).start()
        kv_copy(1, 0, 1 - sub, False).start()
    for d in (1, 3, 2):
        q_copy(d).start()

    acc[...] = jnp.zeros_like(acc)
    total[...] = jnp.zeros_like(total)
    peak[...] = jnp.full_like(peak, NEG)
    ones = jnp.ones((SPAN, HD), BF)

    def block(d, qhalf, slot, half, diagonal):
        keys, values = kvb[slot, half, 0], kvb[slot, half, 1]
        scores = lax.dot_general(
            qb[d, qhalf], keys, (((1,), (1,)), ((), ())), preferred_element_type=F32
        )
        if diagonal:
            row = lax.broadcasted_iota(jnp.int32, (SPAN, SPAN), 0)
            col = lax.broadcasted_iota(jnp.int32, (SPAN, SPAN), 1)
            scores = jnp.where(col <= row, scores, NEG)
        old = peak[d, qhalf]
        new = jnp.maximum(old, jnp.max(scores, axis=1, keepdims=True))
        weights = jnp.exp2((scores - jnp.concatenate([new, new], axis=1)) * LOG2)
        factor = jnp.exp2((old - new) * LOG2)
        summed = lax.dot_general(
            weights.astype(BF),
            jnp.concatenate([values, ones], axis=1),
            (((1,), (0,)), ((), ())),
            preferred_element_type=F32,
        )
        acc[d, qhalf] = acc[d, qhalf] * factor + summed[:, :HD]
        total[d, qhalf] = total[d, qhalf] * factor + summed[:, HD:]
        peak[d, qhalf] = new

    def visit(d, slot, half):
        q_low = ((y + d) % 4) * 4 + zh
        k_low = y * 4 + (zh + slot) % 4
        if half == 0:
            block(d, 1, slot, 0, False)

            @pl.when(k_low < q_low)
            def _():
                block(d, 0, slot, 0, False)
        else:

            @pl.when(q_low < k_low)
            def _():
                block(d, 1, slot, 1, False)

    def visit_all(slot, half, start):
        def step(d, carry):
            visit(d, slot, half)
            return carry

        lax.fori_loop(start, 4, step, 0)

    def send_partial(half):
        def step(d, carry):
            norm = jnp.maximum(total[d, half], 1e-30)
            osend[d - 1, half] = (acc[d, half] / norm).astype(BF)
            lsend[d - 1, half, 0:2] = to_lanes(peak[d, half] * LOG2 + jnp.log2(norm))
            return carry

        lax.fori_loop(1, 4, step, 0)
        for d in (2, 1, 3):
            for copy in o_copies(d, half):
                copy.start()

    def combine(half):
        in_all(orecv.at[:, half], o_ssem.at[0], o_rsem.at[half]).wait_recv()
        in_all(lrecv.at[:, half], l_ssem.at[0], l_rsem.at[half]).wait_recv()
        norm = jnp.maximum(total[0, half], 1e-30)
        logs = [peak[0, half] * LOG2 + jnp.log2(norm)]
        logs += [from_lanes(lrecv[s, half, 0:2]) for s in range(3)]
        top = functools.reduce(jnp.maximum, logs)
        shares = [jnp.exp2(log - top) for log in logs]
        mixed = shares[0] * (acc[0, half] / norm)
        for s in range(3):
            mixed = mixed + shares[s + 1] * orecv[s, half].astype(F32)
        gath[half, zl, x] = (mixed / functools.reduce(jnp.add, shares)).astype(BF)

    def send_x(half, k):
        for sub in range(2):
            x_copy(half, k, 0, sub, False).start()
            x_copy(half, k, 1, 1 - sub, False).start()

    def own_out(half):
        for k in (1, 2, 3):
            line_copy(half, k).start()
        send_x(half, 0)

    def line_in(half, k):
        line_arrival(half, k).wait_recv()
        send_x(half, k)

    def x_in(half, k):
        x_arrival(half, k, 3, 0).wait_recv()
        x_copy(half, k, 0, 0, True).start()
        x_arrival(half, k, 1, 1).wait_recv()
        x_copy(half, k, 1, 1, True).start()

    def project(half, k):
        in_all(gath.at[half, 0, pl.ds(0, 2)], x_ssem.at[0], x_rsem.at[half, k, 0]).wait_recv()
        rows = jnp.concatenate([gath[half, lines[k], x_i] for x_i in range(4)], axis=1)
        weights = jnp.concatenate(
            [
                jnp.concatenate(
                    [w_ref[lines[k] * 4 + x_i, core], w_pair[lines[k] * 4 + x_i]], axis=1
                )
                for x_i in range(4)
            ],
            axis=0,
        )
        part = jnp.dot(rows, weights, preferred_element_type=F32)
        if k == 0:
            sums[half] = part
        elif k < 3:
            sums[half] += part
        else:
            both = sums[half] + part
            part_send[half] = both[:, HD:]
            part_copy(half).start()
            resid[half] = in_order(inc_ref, half) + both[:, :HD]

    def finish(half):
        part_copy(half).wait_recv()
        whole = resid[half] + part_recv[half]
        square = whole * whole
        resid[half] = whole
        rb[half] = whole.astype(BF)
        stat[half] = jnp.concatenate(
            [jnp.sum(square[k : k + 128].T, axis=0, keepdims=True) for k in (0, 128)], axis=0
        )
        for j in range(31, 0, -1):
            stat_copy(half, j).start()

    def rows_out(half):
        @pl.when(rank != (15 if half == 0 else 0))
        def _():
            for part in range(2):
                h_copy(half, part).start()

    def normalize(half):
        stat_others(half).wait_recv()
        stat_all[half, head] = stat[half]
        whole = jnp.sum(stat_all[half], axis=0)
        lane_scale = lax.rsqrt(whole / D + EPS)
        scales[half, 0:2] = lane_scale

        @pl.when(rank != (15 if half == 0 else 0))
        def _():
            s_copy(half).start()

        scale = from_lanes(lane_scale)
        normed = (resid[half] * scale * gain_ref[...]).astype(BF)
        wide = normed.astype(F32)
        resid[half] += skip_ref[...] * wide
        for s in range(8):
            shift[half, s, SPAN + s : 2 * SPAN + s, :] = wide

    def lags(half, top, begin, end, start):
        def step(a, run):
            eight = taps[pl.ds(pl.multiple_of(a * 8, 8), 8), :]
            rows = pl.ds(pl.multiple_of(SPAN + top - a * 8, 8), TILE)
            for s in range(8):
                run = run + eight[s : s + 1] * shift[half, s, rows, :]
            return run

        return lax.fori_loop(begin, end, step, start)

    def conv_own(half):
        for top in range(TILE, SPAN, TILE):
            conv[half, top : top + TILE, :] = lags(
                half, top, 0, top // 8, jnp.zeros((TILE, HD), F32)
            )

    def conv_rest(half):
        edge = rank == (0 if half == 0 else 15)

        @pl.when(edge)
        def _():
            hb[half] = jnp.zeros((SPAN, HD), BF) if half == 0 else rb[0]
            hs[half, 0:2] = jnp.zeros((2, HD), F32) if half == 0 else scales[0, 0:2]

        def arrived(copy):
            @pl.when(jnp.logical_not(edge))
            def _():
                copy.wait_recv()

        arrived(s_copy(half))
        for part in range(2):
            at = 128 - 128 * part
            arrived(h_copy(half, part))
            scale = from_lanes(hs[half, 1 - part : 2 - part])
            rows = hb[half, at : at + 128, :].astype(F32) * scale * gain_ref[...]
            before = rows.astype(BF).astype(F32)
            for s in range(8):
                shift[half, s, at + s : at + s + 128, :] = before
            for top in range(0, SPAN, TILE):
                turn = min(FILT // 8, top // 8 + 15)
                if part == 0:
                    run = jnp.zeros((TILE, HD), F32) if top == 0 else conv[half, top : top + TILE, :]
                    run = lags(half, top, top // 8, turn, run)
                    if turn < FILT // 8:
                        conv[half, top : top + TILE, :] = run
                        continue
                elif turn < FILT // 8:
                    run = lags(half, top, turn, FILT // 8, conv[half, top : top + TILE, :])
                else:
                    continue
                final[half, top : top + TILE, :] = resid[half, top : top + TILE, :] + run

    def sent():
        in_all(kvb.at[pl.ds(0, 3)], kv_ssem.at[0], kv_rsem.at[0, 0, 0]).wait_send()
        in_all(qb.at[pl.ds(1, 3)], q_ssem.at[0], q_rsem.at[0]).wait_send()
        in_all(osend, o_ssem.at[0], o_rsem.at[0]).wait_send()
        in_all(lsend, l_ssem.at[0], l_rsem.at[0]).wait_send()
        in_all(gath.at[:, pl.ds(0, 3), 0], z_ssem.at[0], z_rsem.at[0, 0]).wait_send()
        in_all(gath.at[:, pl.ds(0, 3)], x_ssem.at[0], x_rsem.at[0, 0, 0]).wait_send()
        for half in range(2):
            part_copy(half).wait_send()
            stat_others(half).wait_send()
        w_copy.wait_send()

    def low_relay(half):
        kv_arrival(3, half, 0).wait_recv()
        kv_copy(0, half, 0, True).start()
        kv_arrival(1, half, 1).wait_recv()
        kv_copy(1, half, 1, True).start()

    def send_high(sub):
        kv_copy(0, 1, sub, False).start()
        kv_copy(1, 1, 1 - sub, False).start()

    w_copy.start()
    block(0, 0, 0, 0, True)
    block(0, 1, 0, 0, False)
    block(0, 1, 0, 1, True)
    lag = lax.broadcasted_iota(jnp.int32, (FILT, HD), 0)
    turned = jnp.concatenate(
        [filt_ref[:, k : k + 128].astype(F32).T for k in (0, 128)], axis=0
    )
    taps[...] = jnp.where(lag < flen_ref[...], turned, 0.0)
    in_all(qb.at[pl.ds(1, 3)], q_ssem.at[0], q_rsem.at[0]).wait_recv()
    visit_all(0, 0, 1)
    low_relay(0)
    visit_all(0, 1, 1)
    kv_arrival(3, 0, 1).wait_recv()
    visit_all(3, 0, 0)
    kv_arrival(1, 0, 0).wait_recv()
    send_high(0)
    visit_all(1, 0, 0)
    send_high(1)
    kv_arrival(2, 0, 0).wait_recv()
    kv_arrival(2, 0, 1).wait_recv()
    visit_all(2, 0, 1)
    send_partial(0)
    visit(0, 2, 0)
    low_relay(1)
    combine(0)
    own_out(0)
    kv_arrival(3, 1, 1).wait_recv()
    visit_all(3, 1, 0)
    kv_arrival(1, 1, 0).wait_recv()
    visit_all(1, 1, 0)
    x_in(0, 0)
    line_in(0, 1)
    kv_arrival(2, 1, 0).wait_recv()
    kv_arrival(2, 1, 1).wait_recv()
    visit_all(2, 1, 1)
    send_partial(1)
    visit(0, 2, 1)
    line_in(0, 2)
    x_in(0, 1)
    line_in(0, 3)
    w_copy.wait_recv()
    combine(1)
    own_out(1)
    project(0, 0)
    x_in(0, 2)
    project(0, 1)
    x_in(0, 3)
    line_in(1, 1)
    x_in(1, 0)
    line_in(1, 2)
    project(0, 2)
    line_in(1, 3)
    x_in(1, 1)
    project(0, 3)
    x_in(1, 2)
    finish(0)
    rows_out(0)
    project(1, 0)
    x_in(1, 3)
    project(1, 1)
    project(1, 2)
    project(1, 3)
    finish(1)
    normalize(0)
    conv_own(0)
    rows_out(1)
    sent()
    normalize(1)
    conv_own(1)
    conv_rest(0)
    conv_rest(1)
    low, high = final[0], final[1]
    out_ref[0:SPAN, :] = jnp.where(straight, low, high).astype(BF)
    out_ref[SPAN : 2 * SPAN, :] = jnp.where(straight, high, low).astype(BF)

    for half in range(2):

        @pl.when(rank != (15 if half == 0 else 0))
        def _():
            h_copy(half, 0).wait_send()
            h_copy(half, 1).wait_send()
            s_copy(half).wait_send()


def on_device(
    incoming,
    queries,
    key_vecs,
    value_vecs,
    w_out,
    norm_gain,
    filters,
    filter_len,
    skip_gain,
    slot_map,
):
    dma = pltpu.SemaphoreType.DMA
    vmem = pl.BlockSpec(memory_space=pltpu.VMEM)
    return pl.pallas_call(
        layer_kernel,
        out_shape=jax.ShapeDtypeStruct(queries.shape, BF),
        in_specs=[pl.BlockSpec(memory_space=pltpu.SMEM)] + [pl.BlockSpec(memory_space=pl.ANY)] * 9,
        out_specs=vmem,
        scratch_shapes=[
            pltpu.VMEM((2 * SPAN, HD), BF),
            pltpu.VMEM((2 * SPAN, HD), BF),
            pltpu.VMEM((2 * SPAN, HD), BF),
            pltpu.VMEM((16, 2, HD, HD), BF),
            pltpu.VMEM((2 * SPAN, HD), BF),
            pltpu.VMEM((HD, FILT), BF),
            pltpu.VMEM((1, HD), F32),
            pltpu.VMEM((1, HD), jnp.int32),
            pltpu.VMEM((1, HD), F32),
            pltpu.VMEM((4, 2, SPAN, HD), BF),
            pltpu.VMEM((4, 2, 2, SPAN, HD), BF),
            pltpu.VMEM((4, 2, SPAN, HD), F32),
            pltpu.VMEM((4, 2, SPAN, HD), F32),
            pltpu.VMEM((4, 2, SPAN, HD), F32),
            pltpu.VMEM((3, 2, SPAN, HD), BF),
            pltpu.VMEM((3, 2, 8, HD), F32),
            pltpu.VMEM((3, 2, SPAN, HD), BF),
            pltpu.VMEM((3, 2, 8, HD), F32),
            pltpu.VMEM((2, 4, 4, SPAN, HD), BF),
            pltpu.VMEM((16, HD, HD), BF),
            pltpu.VMEM((2, SPAN, 2 * HD), F32),
            pltpu.VMEM((2, SPAN, HD), F32),
            pltpu.VMEM((2, SPAN, HD), F32),
            pltpu.VMEM((2, SPAN, HD), F32),
            pltpu.VMEM((FILT, HD), F32),
            pltpu.VMEM((2, 2, HD), F32),
            pltpu.VMEM((2, 32, 2, HD), F32),
            pltpu.VMEM((2, SPAN, HD), BF),
            pltpu.VMEM((2, SPAN, HD), BF),
            pltpu.VMEM((2, 8, HD), F32),
            pltpu.VMEM((2, 8, HD), F32),
            pltpu.VMEM((2, 8, 2 * SPAN + 8, HD), F32),
            pltpu.VMEM((2, SPAN, HD), F32),
            pltpu.VMEM((2, SPAN, HD), F32),
            dma((1,)),
            dma((1,)),
            dma((1,)),
            dma((3, 2, 2)),
            dma((1,)),
            dma((2,)),
            dma((1,)),
            dma((2,)),
            dma((1,)),
            dma((2, 4)),
            dma((1,)),
            dma((2, 4, 3)),
            dma((2,)),
            dma((2,)),
            dma((1,)),
            dma((1,)),
            dma((2,)),
            dma((2,)),
            dma((2, 2)),
            dma((2, 2)),
            dma((2,)),
            dma((2,)),
            dma((9,)),
        ],
        compiler_params=pltpu.CompilerParams(collective_id=0, has_side_effects=True),
        name="layer",
    )(
        slot_map,
        queries,
        key_vecs,
        value_vecs,
        w_out.reshape(16, 2, HD, HD),
        incoming,
        filters,
        norm_gain.reshape(1, HD),
        filter_len.reshape(1, HD),
        skip_gain.reshape(1, HD),
    )


def solution(mesh):
    placed = (
        P("seq", "mp"),
        P("seq", "mp"),
        P("seq", "mp"),
        P("seq", "mp"),
        P(None, "mp"),
        P("mp"),
        P("mp", None),
        P("mp"),
        P("mp"),
        P(),
    )
    return jax.shard_map(
        on_device, mesh=mesh, in_specs=placed, out_specs=P("seq", "mp"), check_vma=False
    )
```

```python
import functools
import math

import jax
import jax.numpy as jnp
from jax import lax
from jax.experimental import pallas as pl
from jax.experimental.pallas import tpu as pltpu
from jax.sharding import PartitionSpec as P

D = 4096
HD = 128
SPAN = 256
FILT = 256
EPS = 1e-05
NEG = -1e30
LOG2 = HD ** (-0.5) * math.log2(math.e)
BF = jnp.bfloat16
F32 = jnp.float32
TILE = 64


def remote(src, dst, send_sem, recv_sem, **where):
    return pltpu.make_async_remote_copy(
        src_ref=src,
        dst_ref=dst,
        send_sem=send_sem,
        recv_sem=recv_sem,
        device_id=where,
        device_id_type=pl.DeviceIdType.MESH,
    )


def to_lanes(rep):
    return jnp.concatenate(
        [rep[k : k + 128].T[0:1] for k in range(0, rep.shape[0], 128)], axis=0
    )


def from_lanes(rows):
    return jnp.concatenate(
        [jnp.broadcast_to(rows[k : k + 1], (128, 128)).T for k in range(rows.shape[0])], axis=0
    )


def layer_kernel(
    slot_hbm,
    q_hbm,
    k_hbm,
    v_hbm,
    w_hbm,
    inc_hbm,
    filt_hbm,
    gain_hbm,
    flen_hbm,
    skip_hbm,
    out_ref,
    slot_ref,
    q_ref,
    k_ref,
    v_ref,
    w_ref,
    inc_ref,
    filt_ref,
    gain_ref,
    flen_ref,
    skip_ref,
    qb,
    kvb,
    acc,
    peak,
    total,
    osend,
    lsend,
    orecv,
    lrecv,
    gath,
    w_pair,
    sums,
    part_send,
    part_recv,
    resid,
    taps,
    stat,
    stat_all,
    rb,
    hb,
    scales,
    hs,
    shift,
    conv,
    final,
    q_ssem,
    q_rsem,
    kv_ssem,
    kv_rsem,
    o_ssem,
    o_rsem,
    l_ssem,
    l_rsem,
    z_ssem,
    z_rsem,
    x_ssem,
    x_rsem,
    p_ssem,
    p_rsem,
    w_ssem,
    w_rsem,
    t_ssem,
    t_rsem,
    h_ssem,
    h_rsem,
    s_ssem,
    s_rsem,
    in_sem,
):
    arrays = (
        slot_hbm, q_hbm, k_hbm, v_hbm, w_hbm, inc_hbm, filt_hbm, gain_hbm, flen_hbm, skip_hbm
    )
    held = (
        slot_ref, q_ref, k_ref, v_ref, w_ref, inc_ref, filt_ref, gain_ref, flen_ref, skip_ref
    )
    rank, head = lax.axis_index("seq"), lax.axis_index("mp")
    y, zh = rank // 4, rank % 4
    along_y = [((y + d) % 4) * 4 + zh for d in range(4)]
    along_z = [y * 4 + (zh + d) % 4 for d in range(4)]
    zl, x, core = head // 8, (head // 2) % 4, head % 2
    near = jnp.where(zl == 0, 1, zl - 1)
    far = jnp.where(zl < 2, 3, 0)
    lines = [zl, near, 6 - zl - near - far, far]
    xs = [(x + d) % 4 for d in range(4)]
    partner = head + 1 - 2 * core

    def mp_of(zl_i, x_i, core_i=core):
        return (zl_i * 4 + x_i) * 2 + core_i

    peers = (
        [{"seq": along_y[d]} for d in (1, 2, 3)]
        + [{"seq": along_z[d]} for d in (1, 3)]
        + [{"seq": (rank + d) % 16} for d in (1, 15)]
    )
    barrier = pltpu.get_barrier_semaphore()
    for peer in peers:
        pl.semaphore_signal(
            barrier, inc=1, device_id=peer, device_id_type=pl.DeviceIdType.MESH
        )

    def greet(j, carry):
        pl.semaphore_signal(
            barrier, inc=1, device_id={"mp": (head + j) % 32}, device_id_type=pl.DeviceIdType.MESH
        )
        return carry

    lax.fori_loop(1, 32, greet, 0)
    loads = [
        pltpu.make_async_copy(src, dst, in_sem.at[k])
        for k, (src, dst) in enumerate(zip(arrays, held))
    ]
    for load in loads:
        load.start()
    loads[0].wait()
    gap = slot_ref[2 * rank] - slot_ref[2 * rank + 1]
    straight = jnp.full((SPAN, HD), gap, jnp.int32) < 0

    def in_order(ref, half):
        one, two = ref[0:SPAN, :].astype(F32), ref[SPAN : 2 * SPAN, :].astype(F32)
        return jnp.where(straight, (one, two)[half], (two, one)[half])

    for load in loads[1:4]:
        load.wait()
    for half in range(2):
        qb[0, half] = in_order(q_ref, half).astype(BF)
        kvb[0, half, 0] = in_order(k_ref, half).astype(BF)
        kvb[0, half, 1] = in_order(v_ref, half).astype(BF)
    for load in loads[4:]:
        load.wait()
    pl.semaphore_wait(barrier, len(peers) + 31)

    def in_all(view, send_sem, recv_sem):
        return remote(view, view, send_sem, recv_sem, mp=head)

    def kv_copy(direction, half, sub, relay):
        source = 0 if not relay else (3 if direction == 0 else 1)
        target = 2 if relay else (3 if direction == 0 else 1)
        rows = pl.ds(sub * 128, 128)
        return remote(
            kvb.at[source, half, :, rows],
            kvb.at[target, half, :, rows],
            kv_ssem.at[0],
            kv_rsem.at[target - 1, half, sub],
            seq=along_z[1 if direction == 0 else 3],
        )

    def kv_arrival(slot, half, sub):
        view = kvb.at[slot, half, :, pl.ds(sub * 128, 128)]
        return remote(view, view, kv_ssem.at[0], kv_rsem.at[slot - 1, half, sub], seq=rank)

    def q_copy(d):
        return remote(qb.at[0], qb.at[4 - d], q_ssem.at[0], q_rsem.at[0], seq=along_y[d])

    def o_copies(d, half):
        return (
            remote(
                osend.at[d - 1, half],
                orecv.at[3 - d, half],
                o_ssem.at[0],
                o_rsem.at[half],
                seq=along_y[d],
            ),
            remote(
                lsend.at[d - 1, half],
                lrecv.at[3 - d, half],
                l_ssem.at[0],
                l_rsem.at[half],
                seq=along_y[d],
            ),
        )

    def line_copy(half, k):
        view = gath.at[half, zl, x]
        return remote(
            view, view, z_ssem.at[0], z_rsem.at[half, zl], mp=mp_of(lines[k], x)
        )

    def line_arrival(half, k):
        view = gath.at[half, lines[k], x]
        return remote(view, view, z_ssem.at[0], z_rsem.at[half, lines[k]], mp=head)

    def x_copy(half, k, direction, sub, relay):
        source = xs[(3 if direction == 0 else 1) if relay else 0]
        view = gath.at[half, lines[k], source, pl.ds(sub * 128, 128)]
        return remote(
            view,
            view,
            x_ssem.at[0],
            x_rsem.at[half, k, 1 + direction if not relay and sub == direction else 0],
            mp=mp_of(zl, xs[1 if direction == 0 else 3]),
        )

    def x_arrival(half, k, d, sub):
        view = gath.at[half, lines[k], xs[d], pl.ds(sub * 128, 128)]
        return remote(view, view, x_ssem.at[0], x_rsem.at[half, k, 1 + sub], mp=head)

    w_copy = remote(w_ref.at[:, 1 - core], w_pair, w_ssem.at[0], w_rsem.at[0], mp=partner)

    def part_copy(half):
        return remote(
            part_send.at[half], part_recv.at[half], p_ssem.at[half], p_rsem.at[half], mp=partner
        )

    def stat_copy(half, j):
        return remote(
            stat.at[half],
            stat_all.at[half, head],
            t_ssem.at[half],
            t_rsem.at[half],
            mp=(head + j) % 32,
        )

    def stat_others(half):
        view = stat_all.at[half, pl.ds(0, 31)]
        return remote(view, view, t_ssem.at[half], t_rsem.at[half], mp=head)

    def h_copy(half, part):
        rows = pl.ds(128 - 128 * part, 128)
        return remote(
            rb.at[half, rows],
            hb.at[half, rows],
            h_ssem.at[half, part],
            h_rsem.at[half, part],
            seq=(rank + (1 if half == 0 else 15)) % 16,
        )

    def s_copy(half):
        return remote(
            scales.at[half],
            hs.at[half],
            s_ssem.at[half],
            s_rsem.at[half],
            seq=(rank + (1 if half == 0 else 15)) % 16,
        )

    for sub in range(2):
        kv_copy(0, 0, sub, False).start()
        kv_copy(1, 0, 1 - sub, False).start()
    for d in (1, 3, 2):
        q_copy(d).start()

    acc[...] = jnp.zeros_like(acc)
    total[...] = jnp.zeros_like(total)
    peak[...] = jnp.full_like(peak, NEG)
    ones = jnp.ones((SPAN, HD), BF)

    def block(d, qhalf, slot, half, diagonal, count=1):
        rows = count * SPAN
        some = pl.ds(d, count)
        keys, values = kvb[slot, half, 0], kvb[slot, half, 1]
        scores = lax.dot_general(
            qb[some, qhalf].reshape(rows, HD),
            keys,
            (((1,), (1,)), ((), ())),
            preferred_element_type=F32,
        )
        if diagonal:
            row = lax.broadcasted_iota(jnp.int32, (SPAN, SPAN), 0)
            col = lax.broadcasted_iota(jnp.int32, (SPAN, SPAN), 1)
            scores = jnp.where(col <= row, scores, NEG)
        old = peak[some, qhalf].reshape(rows, HD)
        new = jnp.maximum(old, jnp.max(scores, axis=1, keepdims=True))
        weights = jnp.exp2((scores - jnp.concatenate([new, new], axis=1)) * LOG2)
        factor = jnp.exp2((old - new) * LOG2)
        summed = lax.dot_general(
            weights.astype(BF),
            jnp.concatenate([values, ones], axis=1),
            (((1,), (0,)), ((), ())),
            preferred_element_type=F32,
        )
        shape = (count, SPAN, HD)
        acc[some, qhalf] = (acc[some, qhalf].reshape(rows, HD) * factor + summed[:, :HD]).reshape(shape)
        total[some, qhalf] = (
            total[some, qhalf].reshape(rows, HD) * factor + summed[:, HD:]
        ).reshape(shape)
        peak[some, qhalf] = new.reshape(shape)

    def visit(d, slot, half):
        q_low = ((y + d) % 4) * 4 + zh
        k_low = y * 4 + (zh + slot) % 4
        if half == 0:

            @pl.when(k_low < q_low)
            def _():
                block(d, 0, slot, 0, False)
        else:

            @pl.when(q_low < k_low)
            def _():
                block(d, 1, slot, 1, False)

    def visit_all(slot, half, start):
        def step(d, carry):
            visit(d, slot, half)
            return carry

        if half == 0:
            if start == 0:
                block(0, 1, slot, 0, False)
            block(1, 1, slot, 0, False)
            block(2, 1, slot, 0, False, 2)
            lax.fori_loop(start, 4, step, 0)
        else:
            @pl.when(y >= 2)
            def _():
                block(2, 1, slot, 1, False, 2)

            lax.fori_loop(start, jnp.where(y >= 2, 2, 4), step, 0)

    def send_partial(half):
        def step(d, carry):
            norm = jnp.maximum(total[d, half], 1e-30)
            osend[d - 1, half] = (acc[d, half] / norm).astype(BF)
            lsend[d - 1, half, 0:2] = to_lanes(peak[d, half] * LOG2 + jnp.log2(norm))
            return carry

        lax.fori_loop(1, 4, step, 0)
        for d in (2, 1, 3):
            for copy in o_copies(d, half):
                copy.start()

    def combine(half):
        in_all(orecv.at[:, half], o_ssem.at[0], o_rsem.at[half]).wait_recv()
        in_all(lrecv.at[:, half], l_ssem.at[0], l_rsem.at[half]).wait_recv()
        norm = jnp.maximum(total[0, half], 1e-30)
        logs = [peak[0, half] * LOG2 + jnp.log2(norm)]
        logs += [from_lanes(lrecv[s, half, 0:2]) for s in range(3)]
        top = functools.reduce(jnp.maximum, logs)
        shares = [jnp.exp2(log - top) for log in logs]
        mixed = shares[0] * (acc[0, half] / norm)
        for s in range(3):
            mixed = mixed + shares[s + 1] * orecv[s, half].astype(F32)
        gath[half, zl, x] = (mixed / functools.reduce(jnp.add, shares)).astype(BF)

    def send_x(half, k):
        for sub in range(2):
            x_copy(half, k, 0, sub, False).start()
            x_copy(half, k, 1, 1 - sub, False).start()

    def own_out(half):
        for k in (1, 2, 3):
            line_copy(half, k).start()
        send_x(half, 0)

    def line_in(half, k):
        line_arrival(half, k).wait_recv()
        send_x(half, k)

    def x_in(half, k):
        x_arrival(half, k, 3, 0).wait_recv()
        x_copy(half, k, 0, 0, True).start()
        x_arrival(half, k, 1, 1).wait_recv()
        x_copy(half, k, 1, 1, True).start()

    def project(half, k):
        in_all(gath.at[half, 0, pl.ds(0, 2)], x_ssem.at[0], x_rsem.at[half, k, 0]).wait_recv()
        rows = jnp.concatenate([gath[half, lines[k], x_i] for x_i in range(4)], axis=1)
        weights = jnp.concatenate(
            [
                jnp.concatenate(
                    [w_ref[lines[k] * 4 + x_i, core], w_pair[lines[k] * 4 + x_i]], axis=1
                )
                for x_i in range(4)
            ],
            axis=0,
        )
        part = jnp.dot(rows, weights, preferred_element_type=F32)
        if k == 0:
            sums[half] = part
        elif k < 3:
            sums[half] += part
        else:
            both = sums[half] + part
            part_send[half] = both[:, HD:]
            part_copy(half).start()
            resid[half] = in_order(inc_ref, half) + both[:, :HD]

    def finish(half):
        part_copy(half).wait_recv()
        whole = resid[half] + part_recv[half]
        square = whole * whole
        resid[half] = whole
        rb[half] = whole.astype(BF)
        stat[half] = jnp.concatenate(
            [jnp.sum(square[k : k + 128].T, axis=0, keepdims=True) for k in (0, 128)], axis=0
        )
        for j in range(31, 0, -1):
            stat_copy(half, j).start()

    def rows_out(half):
        @pl.when(rank != (15 if half == 0 else 0))
        def _():
            for part in range(2):
                h_copy(half, part).start()

    def normalize(half):
        stat_others(half).wait_recv()
        stat_all[half, head] = stat[half]
        whole = jnp.sum(stat_all[half], axis=0)
        lane_scale = lax.rsqrt(whole / D + EPS)
        scales[half, 0:2] = lane_scale

        @pl.when(rank != (15 if half == 0 else 0))
        def _():
            s_copy(half).start()

        scale = from_lanes(lane_scale)
        normed = (resid[half] * scale * gain_ref[...]).astype(BF)
        wide = normed.astype(F32)
        resid[half] += skip_ref[...] * wide
        for s in range(8):
            shift[half, s, SPAN + s : 2 * SPAN + s, :] = wide

    def lags(half, top, begin, end, start):
        def step(a, run):
            eight = taps[pl.ds(pl.multiple_of(a * 8, 8), 8), :]
            rows = pl.ds(pl.multiple_of(SPAN + top - a * 8, 8), TILE)
            for s in range(8):
                run = run + eight[s : s + 1] * shift[half, s, rows, :]
            return run

        return lax.fori_loop(begin, end, step, start)

    def conv_own(half):
        for top in range(TILE, SPAN, TILE):
            conv[half, top : top + TILE, :] = lags(
                half, top, 0, top // 8, jnp.zeros((TILE, HD), F32)
            )

    def conv_rest(half):
        edge = rank == (0 if half == 0 else 15)

        @pl.when(edge)
        def _():
            hb[half] = jnp.zeros((SPAN, HD), BF) if half == 0 else rb[0]
            hs[half, 0:2] = jnp.zeros((2, HD), F32) if half == 0 else scales[0, 0:2]

        def arrived(copy):
            @pl.when(jnp.logical_not(edge))
            def _():
                copy.wait_recv()

        arrived(s_copy(half))
        for part in range(2):
            at = 128 - 128 * part
            arrived(h_copy(half, part))
            scale = from_lanes(hs[half, 1 - part : 2 - part])
            rows = hb[half, at : at + 128, :].astype(F32) * scale * gain_ref[...]
            before = rows.astype(BF).astype(F32)
            for s in range(8):
                shift[half, s, at + s : at + s + 128, :] = before
            for top in range(0, SPAN, TILE):
                turn = min(FILT // 8, top // 8 + 15)
                if part == 0:
                    run = jnp.zeros((TILE, HD), F32) if top == 0 else conv[half, top : top + TILE, :]
                    run = lags(half, top, top // 8, turn, run)
                    if turn < FILT // 8:
                        conv[half, top : top + TILE, :] = run
                        continue
                elif turn < FILT // 8:
                    run = lags(half, top, turn, FILT // 8, conv[half, top : top + TILE, :])
                else:
                    continue
                final[half, top : top + TILE, :] = resid[half, top : top + TILE, :] + run

    def sent():
        in_all(kvb.at[pl.ds(0, 3)], kv_ssem.at[0], kv_rsem.at[0, 0, 0]).wait_send()
        in_all(qb.at[pl.ds(1, 3)], q_ssem.at[0], q_rsem.at[0]).wait_send()
        in_all(osend, o_ssem.at[0], o_rsem.at[0]).wait_send()
        in_all(lsend, l_ssem.at[0], l_rsem.at[0]).wait_send()
        in_all(gath.at[:, pl.ds(0, 3), 0], z_ssem.at[0], z_rsem.at[0, 0]).wait_send()
        in_all(gath.at[:, pl.ds(0, 3)], x_ssem.at[0], x_rsem.at[0, 0, 0]).wait_send()
        for half in range(2):
            part_copy(half).wait_send()
            stat_others(half).wait_send()
        w_copy.wait_send()

    def low_relay(half):
        kv_arrival(3, half, 0).wait_recv()
        kv_copy(0, half, 0, True).start()
        kv_arrival(1, half, 1).wait_recv()
        kv_copy(1, half, 1, True).start()

    def send_high(sub):
        kv_copy(0, 1, sub, False).start()
        kv_copy(1, 1, 1 - sub, False).start()

    w_copy.start()
    block(0, 0, 0, 0, True)
    block(0, 1, 0, 0, False)
    block(0, 1, 0, 1, True)
    lag = lax.broadcasted_iota(jnp.int32, (FILT, HD), 0)
    turned = jnp.concatenate(
        [filt_ref[:, k : k + 128].astype(F32).T for k in (0, 128)], axis=0
    )
    taps[...] = jnp.where(lag < flen_ref[...], turned, 0.0)
    in_all(qb.at[pl.ds(1, 3)], q_ssem.at[0], q_rsem.at[0]).wait_recv()
    visit_all(0, 0, 1)
    low_relay(0)
    visit_all(0, 1, 1)
    kv_arrival(3, 0, 1).wait_recv()
    visit_all(3, 0, 0)
    kv_arrival(1, 0, 0).wait_recv()
    send_high(0)
    visit_all(1, 0, 0)
    send_high(1)
    kv_arrival(2, 0, 0).wait_recv()
    kv_arrival(2, 0, 1).wait_recv()
    visit_all(2, 0, 1)
    send_partial(0)
    block(0, 1, 2, 0, False)
    visit(0, 2, 0)
    low_relay(1)
    combine(0)
    own_out(0)
    kv_arrival(3, 1, 1).wait_recv()
    visit_all(3, 1, 0)
    kv_arrival(1, 1, 0).wait_recv()
    visit_all(1, 1, 0)
    x_in(0, 0)
    line_in(0, 1)
    kv_arrival(2, 1, 0).wait_recv()
    kv_arrival(2, 1, 1).wait_recv()
    visit_all(2, 1, 1)
    send_partial(1)
    visit(0, 2, 1)
    line_in(0, 2)
    x_in(0, 1)
    line_in(0, 3)
    w_copy.wait_recv()
    combine(1)
    own_out(1)
    project(0, 0)
    x_in(0, 2)
    project(0, 1)
    x_in(0, 3)
    line_in(1, 1)
    x_in(1, 0)
    line_in(1, 2)
    project(0, 2)
    line_in(1, 3)
    x_in(1, 1)
    project(0, 3)
    x_in(1, 2)
    finish(0)
    rows_out(0)
    project(1, 0)
    x_in(1, 3)
    project(1, 1)
    project(1, 2)
    project(1, 3)
    finish(1)
    normalize(0)
    conv_own(0)
    rows_out(1)
    sent()
    normalize(1)
    conv_own(1)
    conv_rest(0)
    conv_rest(1)
    low, high = final[0], final[1]
    out_ref[0:SPAN, :] = jnp.where(straight, low, high).astype(BF)
    out_ref[SPAN : 2 * SPAN, :] = jnp.where(straight, high, low).astype(BF)

    for half in range(2):

        @pl.when(rank != (15 if half == 0 else 0))
        def _():
            h_copy(half, 0).wait_send()
            h_copy(half, 1).wait_send()
            s_copy(half).wait_send()


def on_device(
    incoming,
    queries,
    key_vecs,
    value_vecs,
    w_out,
    norm_gain,
    filters,
    filter_len,
    skip_gain,
    slot_map,
):
    dma = pltpu.SemaphoreType.DMA
    vmem = pl.BlockSpec(memory_space=pltpu.VMEM)
    return pl.pallas_call(
        layer_kernel,
        out_shape=jax.ShapeDtypeStruct(queries.shape, BF),
        in_specs=[pl.BlockSpec(memory_space=pl.ANY)] * 10,
        out_specs=vmem,
        scratch_shapes=[
            pltpu.SMEM((32,), jnp.int32),
            pltpu.VMEM((2 * SPAN, HD), BF),
            pltpu.VMEM((2 * SPAN, HD), BF),
            pltpu.VMEM((2 * SPAN, HD), BF),
            pltpu.VMEM((16, 2, HD, HD), BF),
            pltpu.VMEM((2 * SPAN, HD), BF),
            pltpu.VMEM((HD, FILT), BF),
            pltpu.VMEM((1, HD), F32),
            pltpu.VMEM((1, HD), jnp.int32),
            pltpu.VMEM((1, HD), F32),
            pltpu.VMEM((4, 2, SPAN, HD), BF),
            pltpu.VMEM((4, 2, 2, SPAN, HD), BF),
            pltpu.VMEM((4, 2, SPAN, HD), F32),
            pltpu.VMEM((4, 2, SPAN, HD), F32),
            pltpu.VMEM((4, 2, SPAN, HD), F32),
            pltpu.VMEM((3, 2, SPAN, HD), BF),
            pltpu.VMEM((3, 2, 8, HD), F32),
            pltpu.VMEM((3, 2, SPAN, HD), BF),
            pltpu.VMEM((3, 2, 8, HD), F32),
            pltpu.VMEM((2, 4, 4, SPAN, HD), BF),
            pltpu.VMEM((16, HD, HD), BF),
            pltpu.VMEM((2, SPAN, 2 * HD), F32),
            pltpu.VMEM((2, SPAN, HD), F32),
            pltpu.VMEM((2, SPAN, HD), F32),
            pltpu.VMEM((2, SPAN, HD), F32),
            pltpu.VMEM((FILT, HD), F32),
            pltpu.VMEM((2, 2, HD), F32),
            pltpu.VMEM((2, 32, 2, HD), F32),
            pltpu.VMEM((2, SPAN, HD), BF),
            pltpu.VMEM((2, SPAN, HD), BF),
            pltpu.VMEM((2, 8, HD), F32),
            pltpu.VMEM((2, 8, HD), F32),
            pltpu.VMEM((2, 8, 2 * SPAN + 8, HD), F32),
            pltpu.VMEM((2, SPAN, HD), F32),
            pltpu.VMEM((2, SPAN, HD), F32),
            dma((1,)),
            dma((1,)),
            dma((1,)),
            dma((3, 2, 2)),
            dma((1,)),
            dma((2,)),
            dma((1,)),
            dma((2,)),
            dma((1,)),
            dma((2, 4)),
            dma((1,)),
            dma((2, 4, 3)),
            dma((2,)),
            dma((2,)),
            dma((1,)),
            dma((1,)),
            dma((2,)),
            dma((2,)),
            dma((2, 2)),
            dma((2, 2)),
            dma((2,)),
            dma((2,)),
            dma((10,)),
        ],
        compiler_params=pltpu.CompilerParams(collective_id=0, has_side_effects=True),
        name="layer",
    )(
        slot_map,
        queries,
        key_vecs,
        value_vecs,
        w_out.reshape(16, 2, HD, HD),
        incoming,
        filters,
        norm_gain.reshape(1, HD),
        filter_len.reshape(1, HD),
        skip_gain.reshape(1, HD),
    )


def solution(mesh):
    placed = (
        P("seq", "mp"),
        P("seq", "mp"),
        P("seq", "mp"),
        P("seq", "mp"),
        P(None, "mp"),
        P("mp"),
        P("mp", None),
        P("mp"),
        P("mp"),
        P(),
    )
    return jax.shard_map(
        on_device, mesh=mesh, in_specs=placed, out_specs=P("seq", "mp"), check_vma=False
    )
```

```python
import functools
import math

import jax
import jax.numpy as jnp
from jax import lax
from jax.experimental import pallas as pl
from jax.experimental.pallas import tpu as pltpu
from jax.sharding import PartitionSpec as P

D = 4096
HD = 128
SPAN = 256
FILT = 256
EPS = 1e-05
NEG = -1e30
LOG2 = HD ** (-0.5) * math.log2(math.e)
BF = jnp.bfloat16
F32 = jnp.float32
TILE = 64


def remote(src, dst, send_sem, recv_sem, **where):
    return pltpu.make_async_remote_copy(
        src_ref=src,
        dst_ref=dst,
        send_sem=send_sem,
        recv_sem=recv_sem,
        device_id=where,
        device_id_type=pl.DeviceIdType.MESH,
    )


def to_lanes(rep):
    return jnp.concatenate(
        [rep[k : k + 128].T[0:1] for k in range(0, rep.shape[0], 128)], axis=0
    )


def from_lanes(rows):
    return jnp.concatenate(
        [jnp.broadcast_to(rows[k : k + 1], (128, 128)).T for k in range(rows.shape[0])], axis=0
    )


def layer_kernel(
    slot_hbm,
    q_hbm,
    k_hbm,
    v_hbm,
    w_hbm,
    inc_hbm,
    filt_hbm,
    gain_hbm,
    flen_hbm,
    skip_hbm,
    out_ref,
    slot_ref,
    q_ref,
    k_ref,
    v_ref,
    w_ref,
    inc_ref,
    filt_ref,
    gain_ref,
    flen_ref,
    skip_ref,
    qb,
    kvb,
    acc,
    peak,
    total,
    osend,
    lsend,
    orecv,
    lrecv,
    gath,
    w_pair,
    sums,
    part_send,
    part_recv,
    resid,
    taps,
    stat,
    stat_all,
    rb,
    hb,
    scales,
    hs,
    shift,
    conv,
    final,
    q_ssem,
    q_rsem,
    kv_ssem,
    kv_rsem,
    o_ssem,
    o_rsem,
    l_ssem,
    l_rsem,
    z_ssem,
    z_rsem,
    x_ssem,
    x_rsem,
    p_ssem,
    p_rsem,
    w_ssem,
    w_rsem,
    t_ssem,
    t_rsem,
    h_ssem,
    h_rsem,
    s_ssem,
    s_rsem,
    in_sem,
):
    arrays = (
        slot_hbm, q_hbm, k_hbm, v_hbm, w_hbm, inc_hbm, filt_hbm, gain_hbm, flen_hbm, skip_hbm
    )
    held = (
        slot_ref, q_ref, k_ref, v_ref, w_ref, inc_ref, filt_ref, gain_ref, flen_ref, skip_ref
    )
    rank, head = lax.axis_index("seq"), lax.axis_index("mp")
    y, zh = rank // 4, rank % 4
    along_y = [((y + d) % 4) * 4 + zh for d in range(4)]
    along_z = [y * 4 + (zh + d) % 4 for d in range(4)]
    zl, x, core = head // 8, (head // 2) % 4, head % 2
    near = jnp.where(zl == 0, 1, zl - 1)
    far = jnp.where(zl < 2, 3, 0)
    lines = [zl, near, 6 - zl - near - far, far]
    xs = [(x + d) % 4 for d in range(4)]
    partner = head + 1 - 2 * core

    def mp_of(zl_i, x_i, core_i=core):
        return (zl_i * 4 + x_i) * 2 + core_i

    peers = (
        [{"seq": along_y[d]} for d in (1, 2, 3)]
        + [{"seq": along_z[d]} for d in (1, 3)]
        + [{"seq": (rank + d) % 16} for d in (1, 15)]
    )
    barrier = pltpu.get_barrier_semaphore()
    for peer in peers:
        pl.semaphore_signal(
            barrier, inc=1, device_id=peer, device_id_type=pl.DeviceIdType.MESH
        )

    def greet(j, carry):
        pl.semaphore_signal(
            barrier, inc=1, device_id={"mp": (head + j) % 32}, device_id_type=pl.DeviceIdType.MESH
        )
        return carry

    lax.fori_loop(1, 32, greet, 0)
    loads = [
        pltpu.make_async_copy(src, dst, in_sem.at[k])
        for k, (src, dst) in enumerate(zip(arrays, held))
    ]
    for load in loads:
        load.start()
    loads[0].wait()
    gap = slot_ref[2 * rank] - slot_ref[2 * rank + 1]
    straight = jnp.full((SPAN, HD), gap, jnp.int32) < 0

    def in_order(ref, half):
        one, two = ref[0:SPAN, :].astype(F32), ref[SPAN : 2 * SPAN, :].astype(F32)
        return jnp.where(straight, (one, two)[half], (two, one)[half])

    for load in loads[1:4]:
        load.wait()
    for half in range(2):
        qb[0, half] = in_order(q_ref, half).astype(BF)
        kvb[0, half, 0] = in_order(k_ref, half).astype(BF)
        kvb[0, half, 1] = in_order(v_ref, half).astype(BF)
    for load in loads[4:]:
        load.wait()
    pl.semaphore_wait(barrier, len(peers) + 31)

    def in_all(view, send_sem, recv_sem):
        return remote(view, view, send_sem, recv_sem, mp=head)

    def kv_copy(direction, half, sub, relay):
        source = 0 if not relay else (3 if direction == 0 else 1)
        target = 2 if relay else (3 if direction == 0 else 1)
        rows = pl.ds(sub * 128, 128)
        return remote(
            kvb.at[source, half, :, rows],
            kvb.at[target, half, :, rows],
            kv_ssem.at[0],
            kv_rsem.at[target - 1, half, sub],
            seq=along_z[1 if direction == 0 else 3],
        )

    def kv_arrival(slot, half, sub):
        view = kvb.at[slot, half, :, pl.ds(sub * 128, 128)]
        return remote(view, view, kv_ssem.at[0], kv_rsem.at[slot - 1, half, sub], seq=rank)

    def q_copy(d):
        return remote(qb.at[0], qb.at[4 - d], q_ssem.at[0], q_rsem.at[0], seq=along_y[d])

    def o_copies(d, half):
        return (
            remote(
                osend.at[d - 1, half],
                orecv.at[3 - d, half],
                o_ssem.at[0],
                o_rsem.at[half],
                seq=along_y[d],
            ),
            remote(
                lsend.at[d - 1, half],
                lrecv.at[3 - d, half],
                l_ssem.at[0],
                l_rsem.at[half],
                seq=along_y[d],
            ),
        )

    def line_copy(half, k):
        view = gath.at[half, zl, x]
        return remote(
            view, view, z_ssem.at[0], z_rsem.at[half, zl], mp=mp_of(lines[k], x)
        )

    def line_arrival(half, k):
        view = gath.at[half, lines[k], x]
        return remote(view, view, z_ssem.at[0], z_rsem.at[half, lines[k]], mp=head)

    def x_copy(half, k, direction, sub, relay):
        source = xs[(3 if direction == 0 else 1) if relay else 0]
        view = gath.at[half, lines[k], source, pl.ds(sub * 128, 128)]
        return remote(
            view,
            view,
            x_ssem.at[0],
            x_rsem.at[half, k, 1 + direction if not relay and sub == direction else 0],
            mp=mp_of(zl, xs[1 if direction == 0 else 3]),
        )

    def x_arrival(half, k, d, sub):
        view = gath.at[half, lines[k], xs[d], pl.ds(sub * 128, 128)]
        return remote(view, view, x_ssem.at[0], x_rsem.at[half, k, 1 + sub], mp=head)

    w_copy = remote(w_ref.at[:, 1 - core], w_pair, w_ssem.at[0], w_rsem.at[0], mp=partner)

    def part_copy(half):
        return remote(
            part_send.at[half], part_recv.at[half], p_ssem.at[half], p_rsem.at[half], mp=partner
        )

    def stat_copy(half, j):
        return remote(
            stat.at[half],
            stat_all.at[half, head],
            t_ssem.at[half],
            t_rsem.at[half],
            mp=(head + j) % 32,
        )

    def stat_others(half):
        view = stat_all.at[half, pl.ds(0, 31)]
        return remote(view, view, t_ssem.at[half], t_rsem.at[half], mp=head)

    def h_copy(half, part):
        rows = pl.ds(128 - 128 * part, 128)
        return remote(
            rb.at[half, rows],
            hb.at[half, rows],
            h_ssem.at[half, part],
            h_rsem.at[half, part],
            seq=(rank + (1 if half == 0 else 15)) % 16,
        )

    def s_copy(half):
        return remote(
            scales.at[half],
            hs.at[half],
            s_ssem.at[half],
            s_rsem.at[half],
            seq=(rank + (1 if half == 0 else 15)) % 16,
        )

    for sub in range(2):
        kv_copy(0, 0, sub, False).start()
        kv_copy(1, 0, 1 - sub, False).start()
    for d in (1, 3, 2):
        q_copy(d).start()

    acc[...] = jnp.zeros_like(acc)
    total[...] = jnp.zeros_like(total)
    peak[...] = jnp.full_like(peak, NEG)
    ones = jnp.ones((SPAN, HD), BF)

    def block(d, qhalf, slot, half, diagonal, count=1):
        rows = count * SPAN
        some = pl.ds(d, count)
        keys, values = kvb[slot, half, 0], kvb[slot, half, 1]
        scores = lax.dot_general(
            qb[some, qhalf].reshape(rows, HD),
            keys,
            (((1,), (1,)), ((), ())),
            preferred_element_type=F32,
        )
        if diagonal:
            row = lax.broadcasted_iota(jnp.int32, (SPAN, SPAN), 0)
            col = lax.broadcasted_iota(jnp.int32, (SPAN, SPAN), 1)
            scores = jnp.where(col <= row, scores, NEG)
        old = peak[some, qhalf].reshape(rows, HD)
        new = jnp.maximum(old, jnp.max(scores, axis=1, keepdims=True))
        weights = jnp.exp2((scores - jnp.concatenate([new, new], axis=1)) * LOG2)
        factor = jnp.exp2((old - new) * LOG2)
        summed = lax.dot_general(
            weights.astype(BF),
            jnp.concatenate([values, ones], axis=1),
            (((1,), (0,)), ((), ())),
            preferred_element_type=F32,
        )
        shape = (count, SPAN, HD)
        acc[some, qhalf] = (acc[some, qhalf].reshape(rows, HD) * factor + summed[:, :HD]).reshape(shape)
        total[some, qhalf] = (
            total[some, qhalf].reshape(rows, HD) * factor + summed[:, HD:]
        ).reshape(shape)
        peak[some, qhalf] = new.reshape(shape)

    def visit(d, slot, half):
        q_low = ((y + d) % 4) * 4 + zh
        k_low = y * 4 + (zh + slot) % 4
        if half == 0:

            @pl.when(k_low < q_low)
            def _():
                block(d, 0, slot, 0, False)
        else:

            @pl.when(q_low < k_low)
            def _():
                block(d, 1, slot, 1, False)

    def visit_all(slot, half, start):
        def step(d, carry):
            visit(d, slot, half)
            return carry

        if half == 0:
            if start == 0:
                block(0, 1, slot, 0, False)
            block(1, 1, slot, 0, False)
            block(2, 1, slot, 0, False, 2)
            lax.fori_loop(start, 4, step, 0)
        else:
            @pl.when(y >= 2)
            def _():
                block(2, 1, slot, 1, False, 2)

            lax.fori_loop(start, jnp.where(y >= 2, 2, 4), step, 0)

    def send_partial(half):
        def step(d, carry):
            norm = jnp.maximum(total[d, half], 1e-30)
            osend[d - 1, half] = (acc[d, half] / norm).astype(BF)
            lsend[d - 1, half, 0:2] = to_lanes(peak[d, half] * LOG2 + jnp.log2(norm))
            return carry

        lax.fori_loop(1, 4, step, 0)
        for d in (2, 1, 3):
            for copy in o_copies(d, half):
                copy.start()

    def combine(half):
        in_all(orecv.at[:, half], o_ssem.at[0], o_rsem.at[half]).wait_recv()
        in_all(lrecv.at[:, half], l_ssem.at[0], l_rsem.at[half]).wait_recv()
        norm = jnp.maximum(total[0, half], 1e-30)
        logs = [peak[0, half] * LOG2 + jnp.log2(norm)]
        logs += [from_lanes(lrecv[s, half, 0:2]) for s in range(3)]
        top = functools.reduce(jnp.maximum, logs)
        shares = [jnp.exp2(log - top) for log in logs]
        mixed = shares[0] * (acc[0, half] / norm)
        for s in range(3):
            mixed = mixed + shares[s + 1] * orecv[s, half].astype(F32)
        gath[half, zl, x] = (mixed / functools.reduce(jnp.add, shares)).astype(BF)

    def send_x(half, k):
        for sub in range(2):
            x_copy(half, k, 0, sub, False).start()
            x_copy(half, k, 1, 1 - sub, False).start()

    def own_out(half):
        for k in (1, 2, 3):
            line_copy(half, k).start()
        send_x(half, 0)

    def line_in(half, k):
        line_arrival(half, k).wait_recv()
        send_x(half, k)

    def x_in(half, k):
        x_arrival(half, k, 3, 0).wait_recv()
        x_copy(half, k, 0, 0, True).start()
        x_arrival(half, k, 1, 1).wait_recv()
        x_copy(half, k, 1, 1, True).start()

    def project(half, k):
        in_all(gath.at[half, 0, pl.ds(0, 2)], x_ssem.at[0], x_rsem.at[half, k, 0]).wait_recv()
        rows = jnp.concatenate([gath[half, lines[k], x_i] for x_i in range(4)], axis=1)
        weights = jnp.concatenate(
            [
                jnp.concatenate(
                    [w_ref[lines[k] * 4 + x_i, core], w_pair[lines[k] * 4 + x_i]], axis=1
                )
                for x_i in range(4)
            ],
            axis=0,
        )
        part = jnp.dot(rows, weights, preferred_element_type=F32)
        if k == 0:
            sums[half] = part
        elif k < 3:
            sums[half] += part
        else:
            both = sums[half] + part
            part_send[half] = both[:, HD:]
            part_copy(half).start()
            resid[half] = in_order(inc_ref, half) + both[:, :HD]

    def finish(half):
        part_copy(half).wait_recv()
        whole = resid[half] + part_recv[half]
        square = whole * whole
        resid[half] = whole
        rb[half] = whole.astype(BF)
        stat[half] = jnp.concatenate(
            [jnp.sum(square[k : k + 128].T, axis=0, keepdims=True) for k in (0, 128)], axis=0
        )
        for j in range(31, 0, -1):
            stat_copy(half, j).start()

    def rows_out(half):
        @pl.when(rank != (15 if half == 0 else 0))
        def _():
            for part in range(2):
                h_copy(half, part).start()

    def normalize(half):
        stat_others(half).wait_recv()
        stat_all[half, head] = stat[half]
        whole = jnp.sum(stat_all[half], axis=0)
        lane_scale = lax.rsqrt(whole / D + EPS)
        scales[half, 0:2] = lane_scale

        @pl.when(rank != (15 if half == 0 else 0))
        def _():
            s_copy(half).start()

        scale = from_lanes(lane_scale)
        normed = (resid[half] * scale * gain_ref[...]).astype(BF)
        wide = normed.astype(F32)
        resid[half] += skip_ref[...] * wide
        for s in range(8):
            shift[half, s, SPAN + s : 2 * SPAN + s, :] = wide

    def lags(half, top, begin, end, start):
        def step(a, run):
            eight = taps[pl.ds(pl.multiple_of(a * 8, 8), 8), :]
            rows = pl.ds(pl.multiple_of(SPAN + top - a * 8, 8), TILE)
            for s in range(8):
                run = run + eight[s : s + 1] * shift[half, s, rows, :]
            return run

        return lax.fori_loop(begin, end, step, start)

    def conv_own(half):
        for top in range(TILE, SPAN, TILE):
            conv[half, top : top + TILE, :] = lags(
                half, top, 0, top // 8, jnp.zeros((TILE, HD), F32)
            )

    def conv_rest(half):
        edge = rank == (0 if half == 0 else 15)

        @pl.when(edge)
        def _():
            hb[half] = jnp.zeros((SPAN, HD), BF) if half == 0 else rb[0]
            hs[half, 0:2] = jnp.zeros((2, HD), F32) if half == 0 else scales[0, 0:2]

        def arrived(copy):
            @pl.when(jnp.logical_not(edge))
            def _():
                copy.wait_recv()

        arrived(s_copy(half))
        for part in range(2):
            at = 128 - 128 * part
            arrived(h_copy(half, part))
            scale = from_lanes(hs[half, 1 - part : 2 - part])
            rows = hb[half, at : at + 128, :].astype(F32) * scale * gain_ref[...]
            before = rows.astype(BF).astype(F32)
            for s in range(8):
                shift[half, s, at + s : at + s + 128, :] = before
            for top in range(0, SPAN, TILE):
                turn = min(FILT // 8, top // 8 + 15)
                if part == 0:
                    run = jnp.zeros((TILE, HD), F32) if top == 0 else conv[half, top : top + TILE, :]
                    run = lags(half, top, top // 8, turn, run)
                    if turn < FILT // 8:
                        conv[half, top : top + TILE, :] = run
                        continue
                elif turn < FILT // 8:
                    run = lags(half, top, turn, FILT // 8, conv[half, top : top + TILE, :])
                else:
                    continue
                final[half, top : top + TILE, :] = resid[half, top : top + TILE, :] + run

    def sent():
        in_all(kvb.at[pl.ds(0, 3)], kv_ssem.at[0], kv_rsem.at[0, 0, 0]).wait_send()
        in_all(qb.at[pl.ds(1, 3)], q_ssem.at[0], q_rsem.at[0]).wait_send()
        in_all(osend, o_ssem.at[0], o_rsem.at[0]).wait_send()
        in_all(lsend, l_ssem.at[0], l_rsem.at[0]).wait_send()
        in_all(gath.at[:, pl.ds(0, 3), 0], z_ssem.at[0], z_rsem.at[0, 0]).wait_send()
        in_all(gath.at[:, pl.ds(0, 3)], x_ssem.at[0], x_rsem.at[0, 0, 0]).wait_send()
        for half in range(2):
            part_copy(half).wait_send()
            stat_others(half).wait_send()
        w_copy.wait_send()

    def low_relay(half):
        kv_arrival(3, half, 0).wait_recv()
        kv_copy(0, half, 0, True).start()
        kv_arrival(1, half, 1).wait_recv()
        kv_copy(1, half, 1, True).start()

    def send_high(sub):
        kv_copy(0, 1, sub, False).start()
        kv_copy(1, 1, 1 - sub, False).start()

    w_copy.start()
    block(0, 0, 0, 0, True)
    block(0, 1, 0, 0, False)
    block(0, 1, 0, 1, True)
    lag = lax.broadcasted_iota(jnp.int32, (FILT, HD), 0)
    turned = jnp.concatenate(
        [filt_ref[:, k : k + 128].astype(F32).T for k in (0, 128)], axis=0
    )
    taps[...] = jnp.where(lag < flen_ref[...], turned, 0.0)
    in_all(qb.at[pl.ds(1, 3)], q_ssem.at[0], q_rsem.at[0]).wait_recv()
    visit_all(0, 0, 1)
    low_relay(0)
    visit_all(0, 1, 1)
    kv_arrival(3, 0, 1).wait_recv()
    visit_all(3, 0, 0)
    kv_arrival(1, 0, 0).wait_recv()
    send_high(0)
    visit_all(1, 0, 0)
    send_high(1)
    kv_arrival(2, 0, 0).wait_recv()
    kv_arrival(2, 0, 1).wait_recv()
    visit_all(2, 0, 1)
    send_partial(0)
    block(0, 1, 2, 0, False)
    visit(0, 2, 0)
    low_relay(1)
    combine(0)
    own_out(0)
    kv_arrival(3, 1, 1).wait_recv()
    visit_all(3, 1, 0)
    kv_arrival(1, 1, 0).wait_recv()
    visit_all(1, 1, 0)
    x_in(0, 0)
    line_in(0, 1)
    kv_arrival(2, 1, 0).wait_recv()
    kv_arrival(2, 1, 1).wait_recv()
    visit_all(2, 1, 1)
    send_partial(1)
    visit(0, 2, 1)
    line_in(0, 2)
    x_in(0, 1)
    line_in(0, 3)
    w_copy.wait_recv()
    combine(1)
    own_out(1)
    project(0, 0)
    x_in(0, 2)
    project(0, 1)
    x_in(0, 3)
    line_in(1, 1)
    x_in(1, 0)
    line_in(1, 2)
    project(0, 2)
    line_in(1, 3)
    x_in(1, 1)
    project(0, 3)
    x_in(1, 2)
    finish(0)
    rows_out(0)
    project(1, 0)
    x_in(1, 3)
    project(1, 1)
    project(1, 2)
    project(1, 3)
    finish(1)
    normalize(0)
    conv_own(0)
    rows_out(1)
    sent()
    normalize(1)
    conv_own(1)
    conv_rest(0)
    conv_rest(1)
    low, high = final[0], final[1]
    out_ref[0:SPAN, :] = jnp.where(straight, low, high)
    out_ref[SPAN : 2 * SPAN, :] = jnp.where(straight, high, low)

    for half in range(2):

        @pl.when(rank != (15 if half == 0 else 0))
        def _():
            h_copy(half, 0).wait_send()
            h_copy(half, 1).wait_send()
            s_copy(half).wait_send()


def on_device(
    incoming,
    queries,
    key_vecs,
    value_vecs,
    w_out,
    norm_gain,
    filters,
    filter_len,
    skip_gain,
    slot_map,
):
    dma = pltpu.SemaphoreType.DMA
    vmem = pl.BlockSpec(memory_space=pltpu.VMEM)
    return pl.pallas_call(
        layer_kernel,
        out_shape=pltpu.VMEM(queries.shape, F32),
        in_specs=[pl.BlockSpec(memory_space=pl.ANY)] * 10,
        out_specs=vmem,
        scratch_shapes=[
            pltpu.SMEM((32,), jnp.int32),
            pltpu.VMEM((2 * SPAN, HD), BF),
            pltpu.VMEM((2 * SPAN, HD), BF),
            pltpu.VMEM((2 * SPAN, HD), BF),
            pltpu.VMEM((16, 2, HD, HD), BF),
            pltpu.VMEM((2 * SPAN, HD), BF),
            pltpu.VMEM((HD, FILT), BF),
            pltpu.VMEM((1, HD), F32),
            pltpu.VMEM((1, HD), jnp.int32),
            pltpu.VMEM((1, HD), F32),
            pltpu.VMEM((4, 2, SPAN, HD), BF),
            pltpu.VMEM((4, 2, 2, SPAN, HD), BF),
            pltpu.VMEM((4, 2, SPAN, HD), F32),
            pltpu.VMEM((4, 2, SPAN, HD), F32),
            pltpu.VMEM((4, 2, SPAN, HD), F32),
            pltpu.VMEM((3, 2, SPAN, HD), BF),
            pltpu.VMEM((3, 2, 8, HD), F32),
            pltpu.VMEM((3, 2, SPAN, HD), BF),
            pltpu.VMEM((3, 2, 8, HD), F32),
            pltpu.VMEM((2, 4, 4, SPAN, HD), BF),
            pltpu.VMEM((16, HD, HD), BF),
            pltpu.VMEM((2, SPAN, 2 * HD), F32),
            pltpu.VMEM((2, SPAN, HD), F32),
            pltpu.VMEM((2, SPAN, HD), F32),
            pltpu.VMEM((2, SPAN, HD), F32),
            pltpu.VMEM((FILT, HD), F32),
            pltpu.VMEM((2, 2, HD), F32),
            pltpu.VMEM((2, 32, 2, HD), F32),
            pltpu.VMEM((2, SPAN, HD), BF),
            pltpu.VMEM((2, SPAN, HD), BF),
            pltpu.VMEM((2, 8, HD), F32),
            pltpu.VMEM((2, 8, HD), F32),
            pltpu.VMEM((2, 8, 2 * SPAN + 8, HD), F32),
            pltpu.VMEM((2, SPAN, HD), F32),
            pltpu.VMEM((2, SPAN, HD), F32),
            dma((1,)),
            dma((1,)),
            dma((1,)),
            dma((3, 2, 2)),
            dma((1,)),
            dma((2,)),
            dma((1,)),
            dma((2,)),
            dma((1,)),
            dma((2, 4)),
            dma((1,)),
            dma((2, 4, 3)),
            dma((2,)),
            dma((2,)),
            dma((1,)),
            dma((1,)),
            dma((2,)),
            dma((2,)),
            dma((2, 2)),
            dma((2, 2)),
            dma((2,)),
            dma((2,)),
            dma((10,)),
        ],
        compiler_params=pltpu.CompilerParams(collective_id=0, has_side_effects=True),
        name="layer",
    )(
        slot_map,
        queries,
        key_vecs,
        value_vecs,
        w_out.reshape(16, 2, HD, HD),
        incoming,
        filters,
        norm_gain.reshape(1, HD),
        filter_len.reshape(1, HD),
        skip_gain.reshape(1, HD),
    ).astype(BF)


def solution(mesh):
    placed = (
        P("seq", "mp"),
        P("seq", "mp"),
        P("seq", "mp"),
        P("seq", "mp"),
        P(None, "mp"),
        P("mp"),
        P("mp", None),
        P("mp"),
        P("mp"),
        P(),
    )
    return jax.shard_map(
        on_device, mesh=mesh, in_specs=placed, out_specs=P("seq", "mp"), check_vma=False
    )
```

```python
import functools
import math

import jax
import jax.numpy as jnp
from jax import lax
from jax.experimental import pallas as pl
from jax.experimental.pallas import tpu as pltpu
from jax.sharding import PartitionSpec as P

D = 4096
HD = 128
SPAN = 256
FILT = 256
EPS = 1e-05
NEG = -1e30
LOG2 = HD ** (-0.5) * math.log2(math.e)
BF = jnp.bfloat16
F32 = jnp.float32
TILE = 64


def remote(src, dst, send_sem, recv_sem, **where):
    return pltpu.make_async_remote_copy(
        src_ref=src,
        dst_ref=dst,
        send_sem=send_sem,
        recv_sem=recv_sem,
        device_id=where,
        device_id_type=pl.DeviceIdType.MESH,
    )


def to_lanes(rep):
    return jnp.concatenate(
        [rep[k : k + 128].T[0:1] for k in range(0, rep.shape[0], 128)], axis=0
    )


def from_lanes(rows):
    return jnp.concatenate(
        [jnp.broadcast_to(rows[k : k + 1], (128, 128)).T for k in range(rows.shape[0])], axis=0
    )


def layer_kernel(
    slot_hbm,
    q_hbm,
    k_hbm,
    v_hbm,
    w_hbm,
    inc_hbm,
    filt_hbm,
    gain_hbm,
    flen_hbm,
    skip_hbm,
    out_ref,
    slot_ref,
    q_ref,
    k_ref,
    v_ref,
    w_ref,
    inc_ref,
    filt_ref,
    gain_ref,
    flen_ref,
    skip_ref,
    qb,
    kvb,
    acc,
    peak,
    total,
    osend,
    lsend,
    orecv,
    lrecv,
    gath,
    w_pair,
    sums,
    part_send,
    part_recv,
    resid,
    taps,
    stat,
    stat_all,
    rb,
    hb,
    scales,
    hs,
    shift,
    conv,
    final,
    q_ssem,
    q_rsem,
    kv_ssem,
    kv_rsem,
    o_ssem,
    o_rsem,
    l_ssem,
    l_rsem,
    z_ssem,
    z_rsem,
    x_ssem,
    x_rsem,
    p_ssem,
    p_rsem,
    w_ssem,
    w_rsem,
    t_ssem,
    t_rsem,
    h_ssem,
    h_rsem,
    s_ssem,
    s_rsem,
    in_sem,
):
    arrays = (
        slot_hbm, q_hbm, k_hbm, v_hbm, w_hbm, inc_hbm, filt_hbm, gain_hbm, flen_hbm, skip_hbm
    )
    held = (
        slot_ref, q_ref, k_ref, v_ref, w_ref, inc_ref, filt_ref, gain_ref, flen_ref, skip_ref
    )
    rank, head = lax.axis_index("seq"), lax.axis_index("mp")
    y, zh = rank // 4, rank % 4
    along_y = [((y + d) % 4) * 4 + zh for d in range(4)]
    along_z = [y * 4 + (zh + d) % 4 for d in range(4)]
    zl, x, core = head // 8, (head // 2) % 4, head % 2
    near = jnp.where(zl == 0, 1, zl - 1)
    far = jnp.where(zl < 2, 3, 0)
    lines = [zl, near, 6 - zl - near - far, far]
    xs = [(x + d) % 4 for d in range(4)]
    partner = head + 1 - 2 * core

    def mp_of(zl_i, x_i, core_i=core):
        return (zl_i * 4 + x_i) * 2 + core_i

    peers = (
        [{"seq": along_y[d]} for d in (1, 2, 3)]
        + [{"seq": along_z[d]} for d in (1, 3)]
        + [{"seq": (rank + d) % 16} for d in (1, 15)]
    )
    barrier = pltpu.get_barrier_semaphore()
    for peer in peers:
        pl.semaphore_signal(
            barrier, inc=1, device_id=peer, device_id_type=pl.DeviceIdType.MESH
        )

    def greet(j, carry):
        pl.semaphore_signal(
            barrier, inc=1, device_id={"mp": (head + j) % 32}, device_id_type=pl.DeviceIdType.MESH
        )
        return carry

    lax.fori_loop(1, 32, greet, 0)
    loads = [
        pltpu.make_async_copy(src, dst, in_sem.at[k])
        for k, (src, dst) in enumerate(zip(arrays, held))
    ]
    for load in loads:
        load.start()
    loads[0].wait()
    gap = slot_ref[2 * rank] - slot_ref[2 * rank + 1]
    straight = jnp.full((SPAN, HD), gap, jnp.int32) < 0

    def in_order(ref, half):
        one, two = ref[0:SPAN, :].astype(F32), ref[SPAN : 2 * SPAN, :].astype(F32)
        return jnp.where(straight, (one, two)[half], (two, one)[half])

    for load in loads[1:4]:
        load.wait()
    for half in range(2):
        qb[0, half] = in_order(q_ref, half).astype(BF)
        kvb[0, half, 0] = in_order(k_ref, half).astype(BF)
        kvb[0, half, 1] = in_order(v_ref, half).astype(BF)
    for load in loads[4:]:
        load.wait()
    pl.semaphore_wait(barrier, len(peers) + 31)

    def in_all(view, send_sem, recv_sem):
        return remote(view, view, send_sem, recv_sem, mp=head)

    def kv_copy(direction, half, sub, relay):
        source = 0 if not relay else (3 if direction == 0 else 1)
        target = 2 if relay else (3 if direction == 0 else 1)
        rows = pl.ds(sub * 128, 128)
        return remote(
            kvb.at[source, half, :, rows],
            kvb.at[target, half, :, rows],
            kv_ssem.at[0],
            kv_rsem.at[target - 1, half, sub],
            seq=along_z[1 if direction == 0 else 3],
        )

    def kv_arrival(slot, half, sub):
        view = kvb.at[slot, half, :, pl.ds(sub * 128, 128)]
        return remote(view, view, kv_ssem.at[0], kv_rsem.at[slot - 1, half, sub], seq=rank)

    def q_copy(d):
        return remote(qb.at[0], qb.at[4 - d], q_ssem.at[0], q_rsem.at[0], seq=along_y[d])

    def o_copies(d, half):
        return (
            remote(
                osend.at[d - 1, half],
                orecv.at[3 - d, half],
                o_ssem.at[0],
                o_rsem.at[half],
                seq=along_y[d],
            ),
            remote(
                lsend.at[d - 1, half],
                lrecv.at[3 - d, half],
                l_ssem.at[0],
                l_rsem.at[half],
                seq=along_y[d],
            ),
        )

    def line_copy(half, k):
        view = gath.at[half, zl, x]
        return remote(
            view, view, z_ssem.at[0], z_rsem.at[half, zl], mp=mp_of(lines[k], x)
        )

    def line_arrival(half, k):
        view = gath.at[half, lines[k], x]
        return remote(view, view, z_ssem.at[0], z_rsem.at[half, lines[k]], mp=head)

    def x_copy(half, k, direction, sub, relay):
        source = xs[(3 if direction == 0 else 1) if relay else 0]
        view = gath.at[half, lines[k], source, pl.ds(sub * 128, 128)]
        return remote(
            view,
            view,
            x_ssem.at[0],
            x_rsem.at[half, k, 1 + direction if not relay and sub == direction else 0],
            mp=mp_of(zl, xs[1 if direction == 0 else 3]),
        )

    def x_arrival(half, k, d, sub):
        view = gath.at[half, lines[k], xs[d], pl.ds(sub * 128, 128)]
        return remote(view, view, x_ssem.at[0], x_rsem.at[half, k, 1 + sub], mp=head)

    w_copy = remote(w_ref.at[:, 1 - core], w_pair, w_ssem.at[0], w_rsem.at[0], mp=partner)

    def part_copy(half):
        return remote(
            part_send.at[half], part_recv.at[half], p_ssem.at[half], p_rsem.at[half], mp=partner
        )

    def stat_copy(half, j):
        return remote(
            stat.at[half],
            stat_all.at[half, head],
            t_ssem.at[half],
            t_rsem.at[half],
            mp=(head + j) % 32,
        )

    def stat_others(half):
        view = stat_all.at[half, pl.ds(0, 31)]
        return remote(view, view, t_ssem.at[half], t_rsem.at[half], mp=head)

    def h_copy(half, part):
        rows = pl.ds(128 - 128 * part, 128)
        return remote(
            rb.at[half, rows],
            hb.at[half, rows],
            h_ssem.at[half, part],
            h_rsem.at[half, part],
            seq=(rank + (1 if half == 0 else 15)) % 16,
        )

    def s_copy(half):
        return remote(
            scales.at[half],
            hs.at[half],
            s_ssem.at[half],
            s_rsem.at[half],
            seq=(rank + (1 if half == 0 else 15)) % 16,
        )

    for sub in range(2):
        kv_copy(0, 0, sub, False).start()
        kv_copy(1, 0, 1 - sub, False).start()
    for d in (1, 3, 2):
        q_copy(d).start()

    acc[...] = jnp.zeros_like(acc)
    total[...] = jnp.zeros_like(total)
    peak[...] = jnp.full_like(peak, NEG)
    ones = jnp.ones((SPAN, HD), BF)

    def block(d, qhalf, slot, half, diagonal, count=1):
        rows = count * SPAN
        some = pl.ds(d, count)
        keys, values = kvb[slot, half, 0], kvb[slot, half, 1]
        scores = lax.dot_general(
            qb[some, qhalf].reshape(rows, HD),
            keys,
            (((1,), (1,)), ((), ())),
            preferred_element_type=F32,
        )
        if diagonal:
            row = lax.broadcasted_iota(jnp.int32, (SPAN, SPAN), 0)
            col = lax.broadcasted_iota(jnp.int32, (SPAN, SPAN), 1)
            scores = jnp.where(col <= row, scores, NEG)
        old = peak[some, qhalf].reshape(rows, HD)
        new = jnp.maximum(old, jnp.max(scores, axis=1, keepdims=True))
        weights = jnp.exp2((scores - jnp.concatenate([new, new], axis=1)) * LOG2)
        factor = jnp.exp2((old - new) * LOG2)
        summed = lax.dot_general(
            weights.astype(BF),
            jnp.concatenate([values, ones], axis=1),
            (((1,), (0,)), ((), ())),
            preferred_element_type=F32,
        )
        shape = (count, SPAN, HD)
        acc[some, qhalf] = (acc[some, qhalf].reshape(rows, HD) * factor + summed[:, :HD]).reshape(shape)
        total[some, qhalf] = (
            total[some, qhalf].reshape(rows, HD) * factor + summed[:, HD:]
        ).reshape(shape)
        peak[some, qhalf] = new.reshape(shape)

    def visit(d, slot, half):
        q_low = ((y + d) % 4) * 4 + zh
        k_low = y * 4 + (zh + slot) % 4
        if half == 0:

            @pl.when(k_low < q_low)
            def _():
                block(d, 0, slot, 0, False)
        else:

            @pl.when(q_low < k_low)
            def _():
                block(d, 1, slot, 1, False)

    def visit_all(slot, half, start):
        def step(d, carry):
            visit(d, slot, half)
            return carry

        if half == 0:
            if start == 0:
                block(0, 1, slot, 0, False)
            block(1, 1, slot, 0, False)
            block(2, 1, slot, 0, False, 2)
            lax.fori_loop(start, 4, step, 0)
        else:
            @pl.when(y >= 2)
            def _():
                block(2, 1, slot, 1, False, 2)

            lax.fori_loop(start, jnp.where(y >= 2, 2, 4), step, 0)

    def send_partial(half):
        for d in (2, 1, 3):
            norm = jnp.maximum(total[d, half], 1e-30)
            osend[d - 1, half] = (acc[d, half] / norm).astype(BF)
            lsend[d - 1, half, 0:2] = to_lanes(peak[d, half] * LOG2 + jnp.log2(norm))
        for d in (2, 1, 3):
            for copy in o_copies(d, half):
                copy.start()

    def combine(half):
        in_all(orecv.at[:, half], o_ssem.at[0], o_rsem.at[half]).wait_recv()
        in_all(lrecv.at[:, half], l_ssem.at[0], l_rsem.at[half]).wait_recv()
        norm = jnp.maximum(total[0, half], 1e-30)
        logs = [peak[0, half] * LOG2 + jnp.log2(norm)]
        logs += [from_lanes(lrecv[s, half, 0:2]) for s in range(3)]
        top = functools.reduce(jnp.maximum, logs)
        shares = [jnp.exp2(log - top) for log in logs]
        mixed = shares[0] * (acc[0, half] / norm)
        for s in range(3):
            mixed = mixed + shares[s + 1] * orecv[s, half].astype(F32)
        gath[half, zl, x] = (mixed / functools.reduce(jnp.add, shares)).astype(BF)

    def send_x(half, k):
        for sub in range(2):
            x_copy(half, k, 0, sub, False).start()
            x_copy(half, k, 1, 1 - sub, False).start()

    def own_out(half):
        for k in (1, 2, 3):
            line_copy(half, k).start()
        send_x(half, 0)

    def line_in(half, k):
        line_arrival(half, k).wait_recv()
        send_x(half, k)

    def x_in(half, k):
        x_arrival(half, k, 3, 0).wait_recv()
        x_copy(half, k, 0, 0, True).start()
        x_arrival(half, k, 1, 1).wait_recv()
        x_copy(half, k, 1, 1, True).start()

    def project(half, k):
        in_all(gath.at[half, 0, pl.ds(0, 2)], x_ssem.at[0], x_rsem.at[half, k, 0]).wait_recv()
        rows = jnp.concatenate([gath[half, lines[k], x_i] for x_i in range(4)], axis=1)
        weights = jnp.concatenate(
            [
                jnp.concatenate(
                    [w_ref[lines[k] * 4 + x_i, core], w_pair[lines[k] * 4 + x_i]], axis=1
                )
                for x_i in range(4)
            ],
            axis=0,
        )
        part = jnp.dot(rows, weights, preferred_element_type=F32)
        if k == 0:
            sums[half] = part
        elif k < 3:
            sums[half] += part
        else:
            both = sums[half] + part
            part_send[half] = both[:, HD:]
            part_copy(half).start()
            resid[half] = in_order(inc_ref, half) + both[:, :HD]

    def finish(half):
        part_copy(half).wait_recv()
        whole = resid[half] + part_recv[half]
        square = whole * whole
        resid[half] = whole
        rb[half] = whole.astype(BF)
        stat[half] = jnp.concatenate(
            [jnp.sum(square[k : k + 128].T, axis=0, keepdims=True) for k in (0, 128)], axis=0
        )
        for j in range(31, 0, -1):
            stat_copy(half, j).start()

    def rows_out(half):
        @pl.when(rank != (15 if half == 0 else 0))
        def _():
            for part in range(2):
                h_copy(half, part).start()

    def normalize(half):
        stat_others(half).wait_recv()
        stat_all[half, head] = stat[half]
        whole = jnp.sum(stat_all[half], axis=0)
        lane_scale = lax.rsqrt(whole / D + EPS)
        scales[half, 0:2] = lane_scale

        @pl.when(rank != (15 if half == 0 else 0))
        def _():
            s_copy(half).start()

        scale = from_lanes(lane_scale)
        normed = (resid[half] * scale * gain_ref[...]).astype(BF)
        wide = normed.astype(F32)
        resid[half] += skip_ref[...] * wide
        for s in range(8):
            shift[half, s, SPAN + s : 2 * SPAN + s, :] = wide

    def lags(half, top, begin, end, start):
        def step(a, run):
            eight = taps[pl.ds(pl.multiple_of(a * 8, 8), 8), :]
            rows = pl.ds(pl.multiple_of(SPAN + top - a * 8, 8), TILE)
            for s in range(8):
                run = run + eight[s : s + 1] * shift[half, s, rows, :]
            return run

        return lax.fori_loop(begin, end, step, start)

    def conv_own(half):
        for top in range(TILE, SPAN, TILE):
            conv[half, top : top + TILE, :] = lags(
                half, top, 0, top // 8, jnp.zeros((TILE, HD), F32)
            )

    def conv_rest(half):
        edge = rank == (0 if half == 0 else 15)

        @pl.when(edge)
        def _():
            hb[half] = jnp.zeros((SPAN, HD), BF) if half == 0 else rb[0]
            hs[half, 0:2] = jnp.zeros((2, HD), F32) if half == 0 else scales[0, 0:2]

        def arrived(copy):
            @pl.when(jnp.logical_not(edge))
            def _():
                copy.wait_recv()

        arrived(s_copy(half))
        for part in range(2):
            at = 128 - 128 * part
            arrived(h_copy(half, part))
            scale = from_lanes(hs[half, 1 - part : 2 - part])
            rows = hb[half, at : at + 128, :].astype(F32) * scale * gain_ref[...]
            before = rows.astype(BF).astype(F32)
            for s in range(8):
                shift[half, s, at + s : at + s + 128, :] = before
            for top in range(0, SPAN, TILE):
                turn = min(FILT // 8, top // 8 + 15)
                if part == 0:
                    run = jnp.zeros((TILE, HD), F32) if top == 0 else conv[half, top : top + TILE, :]
                    run = lags(half, top, top // 8, turn, run)
                    if turn < FILT // 8:
                        conv[half, top : top + TILE, :] = run
                        continue
                elif turn < FILT // 8:
                    run = lags(half, top, turn, FILT // 8, conv[half, top : top + TILE, :])
                else:
                    continue
                final[half, top : top + TILE, :] = resid[half, top : top + TILE, :] + run

    def sent():
        in_all(kvb.at[pl.ds(0, 3)], kv_ssem.at[0], kv_rsem.at[0, 0, 0]).wait_send()
        in_all(qb.at[pl.ds(1, 3)], q_ssem.at[0], q_rsem.at[0]).wait_send()
        in_all(osend, o_ssem.at[0], o_rsem.at[0]).wait_send()
        in_all(lsend, l_ssem.at[0], l_rsem.at[0]).wait_send()
        in_all(gath.at[:, pl.ds(0, 3), 0], z_ssem.at[0], z_rsem.at[0, 0]).wait_send()
        in_all(gath.at[:, pl.ds(0, 3)], x_ssem.at[0], x_rsem.at[0, 0, 0]).wait_send()
        for half in range(2):
            part_copy(half).wait_send()
            stat_others(half).wait_send()
        w_copy.wait_send()

    def low_relay(half):
        kv_arrival(3, half, 0).wait_recv()
        kv_copy(0, half, 0, True).start()
        kv_arrival(1, half, 1).wait_recv()
        kv_copy(1, half, 1, True).start()

    def send_high(sub):
        kv_copy(0, 1, sub, False).start()
        kv_copy(1, 1, 1 - sub, False).start()

    w_copy.start()
    block(0, 0, 0, 0, True)
    block(0, 1, 0, 0, False)
    block(0, 1, 0, 1, True)
    lag = lax.broadcasted_iota(jnp.int32, (FILT, HD), 0)
    turned = jnp.concatenate(
        [filt_ref[:, k : k + 128].astype(F32).T for k in (0, 128)], axis=0
    )
    taps[...] = jnp.where(lag < flen_ref[...], turned, 0.0)
    in_all(qb.at[pl.ds(1, 3)], q_ssem.at[0], q_rsem.at[0]).wait_recv()
    visit_all(0, 0, 1)
    low_relay(0)
    visit_all(0, 1, 1)
    kv_arrival(3, 0, 1).wait_recv()
    visit_all(3, 0, 0)
    kv_arrival(1, 0, 0).wait_recv()
    send_high(0)
    visit_all(1, 0, 0)
    send_high(1)
    kv_arrival(2, 0, 0).wait_recv()
    kv_arrival(2, 0, 1).wait_recv()
    visit_all(2, 0, 1)
    send_partial(0)
    block(0, 1, 2, 0, False)
    visit(0, 2, 0)
    low_relay(1)
    combine(0)
    own_out(0)
    kv_arrival(3, 1, 1).wait_recv()
    visit_all(3, 1, 0)
    kv_arrival(1, 1, 0).wait_recv()
    visit_all(1, 1, 0)
    x_in(0, 0)
    line_in(0, 1)
    kv_arrival(2, 1, 0).wait_recv()
    kv_arrival(2, 1, 1).wait_recv()
    visit_all(2, 1, 1)
    send_partial(1)
    visit(0, 2, 1)
    line_in(0, 2)
    x_in(0, 1)
    line_in(0, 3)
    w_copy.wait_recv()
    combine(1)
    own_out(1)
    project(0, 0)
    x_in(0, 2)
    project(0, 1)
    x_in(0, 3)
    line_in(1, 1)
    x_in(1, 0)
    line_in(1, 2)
    project(0, 2)
    line_in(1, 3)
    x_in(1, 1)
    project(0, 3)
    x_in(1, 2)
    finish(0)
    rows_out(0)
    project(1, 0)
    x_in(1, 3)
    project(1, 1)
    project(1, 2)
    project(1, 3)
    finish(1)
    normalize(0)
    conv_own(0)
    rows_out(1)
    sent()
    normalize(1)
    conv_own(1)
    conv_rest(0)
    conv_rest(1)
    low, high = final[0], final[1]
    out_ref[0:SPAN, :] = jnp.where(straight, low, high)
    out_ref[SPAN : 2 * SPAN, :] = jnp.where(straight, high, low)

    for half in range(2):

        @pl.when(rank != (15 if half == 0 else 0))
        def _():
            h_copy(half, 0).wait_send()
            h_copy(half, 1).wait_send()
            s_copy(half).wait_send()


def on_device(
    incoming,
    queries,
    key_vecs,
    value_vecs,
    w_out,
    norm_gain,
    filters,
    filter_len,
    skip_gain,
    slot_map,
):
    dma = pltpu.SemaphoreType.DMA
    vmem = pl.BlockSpec(memory_space=pltpu.VMEM)
    return pl.pallas_call(
        layer_kernel,
        out_shape=pltpu.VMEM(queries.shape, F32),
        in_specs=[pl.BlockSpec(memory_space=pl.ANY)] * 10,
        out_specs=vmem,
        scratch_shapes=[
            pltpu.SMEM((32,), jnp.int32),
            pltpu.VMEM((2 * SPAN, HD), BF),
            pltpu.VMEM((2 * SPAN, HD), BF),
            pltpu.VMEM((2 * SPAN, HD), BF),
            pltpu.VMEM((16, 2, HD, HD), BF),
            pltpu.VMEM((2 * SPAN, HD), BF),
            pltpu.VMEM((HD, FILT), BF),
            pltpu.VMEM((1, HD), F32),
            pltpu.VMEM((1, HD), jnp.int32),
            pltpu.VMEM((1, HD), F32),
            pltpu.VMEM((4, 2, SPAN, HD), BF),
            pltpu.VMEM((4, 2, 2, SPAN, HD), BF),
            pltpu.VMEM((4, 2, SPAN, HD), F32),
            pltpu.VMEM((4, 2, SPAN, HD), F32),
            pltpu.VMEM((4, 2, SPAN, HD), F32),
            pltpu.VMEM((3, 2, SPAN, HD), BF),
            pltpu.VMEM((3, 2, 8, HD), F32),
            pltpu.VMEM((3, 2, SPAN, HD), BF),
            pltpu.VMEM((3, 2, 8, HD), F32),
            pltpu.VMEM((2, 4, 4, SPAN, HD), BF),
            pltpu.VMEM((16, HD, HD), BF),
            pltpu.VMEM((2, SPAN, 2 * HD), F32),
            pltpu.VMEM((2, SPAN, HD), F32),
            pltpu.VMEM((2, SPAN, HD), F32),
            pltpu.VMEM((2, SPAN, HD), F32),
            pltpu.VMEM((FILT, HD), F32),
            pltpu.VMEM((2, 2, HD), F32),
            pltpu.VMEM((2, 32, 2, HD), F32),
            pltpu.VMEM((2, SPAN, HD), BF),
            pltpu.VMEM((2, SPAN, HD), BF),
            pltpu.VMEM((2, 8, HD), F32),
            pltpu.VMEM((2, 8, HD), F32),
            pltpu.VMEM((2, 8, 2 * SPAN + 8, HD), F32),
            pltpu.VMEM((2, SPAN, HD), F32),
            pltpu.VMEM((2, SPAN, HD), F32),
            dma((1,)),
            dma((1,)),
            dma((1,)),
            dma((3, 2, 2)),
            dma((1,)),
            dma((2,)),
            dma((1,)),
            dma((2,)),
            dma((1,)),
            dma((2, 4)),
            dma((1,)),
            dma((2, 4, 3)),
            dma((2,)),
            dma((2,)),
            dma((1,)),
            dma((1,)),
            dma((2,)),
            dma((2,)),
            dma((2, 2)),
            dma((2, 2)),
            dma((2,)),
            dma((2,)),
            dma((10,)),
        ],
        compiler_params=pltpu.CompilerParams(collective_id=0, has_side_effects=True),
        name="layer",
    )(
        slot_map,
        queries,
        key_vecs,
        value_vecs,
        w_out.reshape(16, 2, HD, HD),
        incoming,
        filters,
        norm_gain.reshape(1, HD),
        filter_len.reshape(1, HD),
        skip_gain.reshape(1, HD),
    ).astype(BF)


def solution(mesh):
    placed = (
        P("seq", "mp"),
        P("seq", "mp"),
        P("seq", "mp"),
        P("seq", "mp"),
        P(None, "mp"),
        P("mp"),
        P("mp", None),
        P("mp"),
        P("mp"),
        P(),
    )
    return jax.shard_map(
        on_device, mesh=mesh, in_specs=placed, out_specs=P("seq", "mp"), check_vma=False
    )
```
